128 devices in a mesh: dp: 8 (over z_hi, y), tensor: 16 (over x, z_lo, core).
Axes of the slice: x: 4, y: 4, z: 4 (z_hi: 2, z_lo: 2; z = z_hi * 2 + z_lo), core: 2. Of those that a mesh axis runs over, the one named last changes fastest.
Arguments:
- noisy: bfloat16 [64, 256, 1152], P('dp', None, 'tensor'), may hold values from -6 to 6
- labels: int32 [64], P('dp'), may hold values from 0 to 999
- tsteps: int32 [64], P('dp'), may hold values from 0 to 999
- guide_index: int32 [64], P('dp'), may hold values from 0 to 31
- class_table: bfloat16 [1001, 1152], replicated, may hold values from -6 to 6
- time_table: bfloat16 [1000, 1152], replicated, may hold values from -6 to 6
- guide_table: bfloat16 [32, 1152], replicated, may hold values from -6 to 6
- guide_weights: float32 [32], replicated, may hold values from 0.5 to 4
- teacher_qkv: bfloat16 [1152, 3456], P(None, 'tensor'), may hold values from -0.1875 to 0.1875
- teacher_out: bfloat16 [1152, 1152], P('tensor'), may hold values from -0.1875 to 0.1875
- teacher_ada: bfloat16 [3, 1152, 1152], P(None, None, 'tensor'), may hold values from -0.1875 to 0.1875
- student_qkv: bfloat16 [1152, 3456], P(None, 'tensor'), may hold values from -0.1875 to 0.1875
- student_out: bfloat16 [1152, 1152], P('tensor'), may hold values from -0.1875 to 0.1875
- student_ada: bfloat16 [3, 1152, 1152], P(None, None, 'tensor'), may hold values from -0.1875 to 0.1875
Outputs:
- grad_qkv: float32 [1152, 3456], P('dp', 'tensor')
- grad_out: float32 [1152, 1152], P('tensor', 'dp')
- grad_ada: float32 [3, 1152, 1152], P(None, 'dp', 'tensor')
The draws below stay inside these ranges and needn't reach their ends.
All inputs are finite; a program needn't handle non-finite values.
Results may differ from the reference program's by a relative error of at most 0.034.
Values may be sent and summed in bfloat16 or wider, within the bound.
A program may use at most 128 MiB of HBM per device.

```python
import math
import jax
import jax.numpy as jnp
from jax import lax

D = 1152
HEADS = 16
HD = 72
CLASSES = 1000
L = 256
TSTEPS = 1000
GUIDES = 32
BATCH = 64
N_TENSOR = 16


def touch_ends(values, key, smallest, high):
    longest = values.shape.index(max(values.shape))
    spots = []
    for shift in (0, 1):
        where = [jax.random.randint(jax.random.fold_in(key, axis), (), 0, length) for axis, length in enumerate(values.shape)]
        where[longest] = (where[longest] + shift) % values.shape[longest]
        spots.append(tuple(where))
    return values.at[spots[0]].set(smallest).at[spots[1]].set(high)


def block_scale(stream_key, shape, pieces, low, largest):
    gain = 1.0
    for position, parts in pieces:
        steps = jax.random.uniform(jax.random.fold_in(jax.random.fold_in(stream_key, 6), position), (parts,), jnp.float32, low / len(pieces), largest / len(pieces))
        gain = gain * jnp.repeat(jnp.exp(steps), shape[position] // parts).reshape((-1,) + (1,) * (len(shape) - 1 - position))
    return gain


def normal_values(rng, dims, scale, limit, cuts=(), dtype=jnp.bfloat16):
    result = scale * jax.random.normal(rng, dims, jnp.float32)
    if cuts:
        result = result * block_scale(rng, dims, cuts, -0.22, 0.18)
    return jnp.clip(result, -limit, limit).astype(dtype)


def setup_inputs(seed: int = 0) -> dict:
    key_list = jax.random.split(jax.random.key(seed), 15)
    noisy = normal_values(key_list[0], (BATCH, L, D), 1.0, 6.0, ((0, 8), (2, 16)))
    labels = touch_ends(jax.random.randint(key_list[1], (BATCH,), 0, CLASSES), jax.random.fold_in(key_list[1], 1), 0, CLASSES - 1).astype(jnp.int32)
    tsteps = touch_ends(jax.random.randint(key_list[2], (BATCH,), 0, TSTEPS), jax.random.fold_in(key_list[2], 1), 0, TSTEPS - 1).astype(jnp.int32)
    guide_index = touch_ends(jax.random.randint(key_list[3], (BATCH,), 0, GUIDES), jax.random.fold_in(key_list[3], 1), 0, GUIDES - 1).astype(jnp.int32)
    class_table = normal_values(key_list[4], (CLASSES + 1, D), 1.0, 6.0)
    time_table = normal_values(key_list[5], (TSTEPS, D), 1.0, 6.0)
    guide_table = normal_values(key_list[6], (GUIDES, D), 1.0, 6.0)
    guide_weights = jnp.clip(jax.random.uniform(key_list[7], (GUIDES,), jnp.float32, 0.5, 4.0), 0.5, 4.0)
    teacher_qkv = normal_values(key_list[8], (D, 3 * D), D ** -0.5, 0.1875, ((1, 16),))
    teacher_out = normal_values(key_list[9], (D, D), D ** -0.5, 0.1875, ((0, 16),))
    teacher_ada = normal_values(key_list[10], (3, D, D), D ** -0.5, 0.1875, ((2, 16),))
    student_qkv = normal_values(key_list[11], (D, 3 * D), D ** -0.5, 0.1875, ((1, 16),))
    student_out = normal_values(key_list[12], (D, D), D ** -0.5, 0.1875, ((0, 16),))
    student_ada = normal_values(key_list[13], (3, D, D), D ** -0.5, 0.1875, ((2, 16),))
    return dict(noisy=noisy, labels=labels, tsteps=tsteps, guide_index=guide_index, class_table=class_table, time_table=time_table, guide_table=guide_table, guide_weights=guide_weights, teacher_qkv=teacher_qkv, teacher_out=teacher_out, teacher_ada=teacher_ada, student_qkv=student_qkv, student_out=student_out, student_ada=student_ada)


norm_eps = 1e-06

def round_trip(value):
    return lax.optimization_barrier(value.astype(jnp.bfloat16)).astype(jnp.float32)

def block_sum(left_rows, right_rows, block_count):
    inner_width = left_rows.shape[1] // block_count

    def add_block(block_idx, running):
        offset = (block_idx * inner_width).astype(jnp.int32)
        left_block = lax.dynamic_slice_in_dim(left_rows, offset, inner_width, 1)
        right_block = lax.dynamic_slice_in_dim(right_rows, offset, inner_width, 0)
        partial_value = jnp.dot(left_block, right_block, preferred_element_type=jnp.float32)
        return running + round_trip(partial_value)
    initial = jnp.zeros((left_rows.shape[0], right_rows.shape[1]), jnp.float32)
    return lax.fori_loop(0, block_count, add_block, initial)

def sample_probs(sample_qkv):
    queries = sample_qkv[:, :, 0].astype(jnp.float32)
    key_rows = sample_qkv[:, :, 1].astype(jnp.float32)
    scores = jnp.einsum('lhe,mhe->hlm', queries, key_rows) * (1.0 / math.sqrt(HD))
    exponent = jnp.exp(scores - lax.optimization_barrier(jnp.max(scores, axis=-1, keepdims=True)))
    return exponent / lax.optimization_barrier(jnp.sum(exponent, axis=-1, keepdims=True))

def attend_one(sample_qkv):
    attn_prob = sample_probs(sample_qkv)
    values = sample_qkv[:, :, 2].astype(jnp.float32)
    attn_mixed = jnp.einsum('hlm,mhe->lhe', round_trip(attn_prob), values)
    return attn_mixed.astype(jnp.bfloat16)

def attend_back(sample_pair):
    sample_qkv, grad_low = sample_pair
    attn_prob = sample_probs(sample_qkv)
    prob_low = round_trip(attn_prob)
    queries = sample_qkv[:, :, 0].astype(jnp.float32)
    key_rows = sample_qkv[:, :, 1].astype(jnp.float32)
    values = sample_qkv[:, :, 2].astype(jnp.float32)
    grad_mixed = grad_low.astype(jnp.float32)
    grad_probs = jnp.einsum('lhe,mhe->hlm', grad_mixed, values)
    row_delta = lax.optimization_barrier(jnp.sum(attn_prob * grad_probs, axis=-1, keepdims=True))
    grad_scores = round_trip(attn_prob * (grad_probs - row_delta) * (1.0 / math.sqrt(HD)))
    grad_query = jnp.einsum('hlm,mhe->lhe', grad_scores, key_rows)
    grad_keys = jnp.einsum('hlm,lhe->mhe', grad_scores, queries)
    grad_values = jnp.einsum('hlm,lhe->mhe', prob_low, grad_mixed)
    return jnp.stack([grad_query, grad_keys, grad_values], axis=2).astype(jnp.bfloat16)

def forward(normed, embed_act, qkv_weight, out_weight, ada_weight):
    batch_size = normed.shape[0]
    modulation = jnp.einsum('bd,kde->bke', embed_act.astype(jnp.float32), ada_weight.astype(jnp.float32))
    modulated = (normed.astype(jnp.float32) * (1.0 + modulation[:, 1][:, None]) + modulation[:, 0][:, None]).astype(jnp.bfloat16)
    qkv_sums = jnp.dot(modulated.reshape(-1, D), qkv_weight, preferred_element_type=jnp.float32)
    heads_qkv = qkv_sums.astype(jnp.bfloat16).reshape(batch_size, L, HEADS, 3, HD)
    attn_mixed = lax.map(attend_one, heads_qkv).reshape(-1, D)
    projected = block_sum(attn_mixed, out_weight, N_TENSOR).reshape(batch_size, L, D)
    branch = modulation[:, 2][:, None] * projected
    return (branch, modulated, heads_qkv, attn_mixed, projected, modulation)

def reference(noisy, labels, tsteps, guide_index, class_table, time_table, guide_table, guide_weights, teacher_qkv, teacher_out, teacher_ada, student_qkv, student_out, student_ada):
    batch_size = noisy.shape[0]
    signal = noisy.astype(jnp.float32)
    row_mean = lax.optimization_barrier(jnp.sum(signal, axis=2, keepdims=True)) / D
    row_var = lax.optimization_barrier(jnp.sum(signal * signal, axis=2, keepdims=True)) / D - row_mean * row_mean
    normed = ((signal - row_mean) * lax.rsqrt(row_var + norm_eps)).astype(jnp.bfloat16)
    time_embed = time_table[tsteps].astype(jnp.float32)
    cond_embed = class_table[labels].astype(jnp.float32) + time_embed
    null_embed = class_table[CLASSES].astype(jnp.float32)[None, :] + time_embed
    student_embed = cond_embed + guide_table[guide_index].astype(jnp.float32)
    cond_act = jax.nn.silu(cond_embed).astype(jnp.bfloat16)
    null_act = jax.nn.silu(null_embed).astype(jnp.bfloat16)
    student_act = jax.nn.silu(student_embed).astype(jnp.bfloat16)
    cond_result = forward(normed, cond_act, teacher_qkv, teacher_out, teacher_ada)
    null_result = forward(normed, null_act, teacher_qkv, teacher_out, teacher_ada)
    cond_update = round_trip(cond_result[0])
    null_update = round_trip(null_result[0])
    strength = guide_weights[guide_index][:, None, None]
    target = signal + ((1.0 + strength) * cond_update - strength * null_update)
    branch, modulated, heads_qkv, attn_mixed, projected, modulation = forward(normed, student_act, student_qkv, student_out, student_ada)
    cotangent = (signal + branch - target) * (1.0 / math.sqrt(batch_size * L))
    grad_gate = lax.optimization_barrier(jnp.sum(cotangent * projected, axis=1))
    grad_proj = (cotangent * modulation[:, 2][:, None]).astype(jnp.bfloat16).reshape(-1, D)
    grad_out = jnp.dot(attn_mixed.T, grad_proj, preferred_element_type=jnp.float32)
    grad_mixed = jnp.dot(grad_proj, student_out.T, preferred_element_type=jnp.float32)
    grad_low = grad_mixed.astype(jnp.bfloat16).reshape(batch_size, L, HEADS, HD)
    grad_qkv_act = lax.map(attend_back, (heads_qkv, grad_low)).reshape(-1, 3 * D)
    grad_qkv = jnp.dot(modulated.reshape(-1, D).T, grad_qkv_act, preferred_element_type=jnp.float32)
    grad_input = block_sum(grad_qkv_act, student_qkv.T, N_TENSOR).reshape(batch_size, L, D)
    grad_shift = lax.optimization_barrier(jnp.sum(grad_input, axis=1))
    grad_scale = lax.optimization_barrier(jnp.sum(grad_input * normed.astype(jnp.float32), axis=1))
    grad_modulation = jnp.stack([grad_shift, grad_scale, grad_gate], axis=1)
    grad_ada = jnp.einsum('bd,bke->kde', student_act.astype(jnp.float32), grad_modulation, precision=lax.Precision.HIGHEST)
    return (grad_qkv, grad_out, grad_ada)
```

```python
import math

import jax
import jax.numpy as jnp
from jax import lax
from jax.sharding import PartitionSpec as P

HD = 72


norm_eps = 1e-06


def in_order(pieces, dim):
    shape = list(pieces.shape[1:])
    shape[dim] *= pieces.shape[0]
    return jnp.moveaxis(pieces, 0, dim).reshape(shape)


def sent_to_all(shard, axis):
    copies = jnp.broadcast_to(shard, (lax.axis_size(axis), *shard.shape))
    return lax.all_to_all(copies, axis, split_axis=0, concat_axis=0, tiled=True)


def collect(shard, axis, dim):
    return in_order(sent_to_all(shard, axis), dim)


def taken_together(shard, axis):
    return sent_to_all(shard, axis).sum(axis=0)


def in_one(arrays, axis):
    vector, at, outs = (jnp.concatenate([a.reshape(-1) for a in arrays]), 0, [])
    running = taken_together(vector, axis)
    for a in arrays:
        outs.append(running[at : at + a.size].reshape(a.shape))
        at += a.size
    return tuple(outs)


def in_blocks(shard, dim, devices):
    shape = shard.shape
    pieces = shard.reshape(*shape[:dim], devices, shape[dim] // devices, *shape[dim + 1 :])
    return jnp.moveaxis(pieces, dim, 0)


def sum_together(arrays, axis, dims):
    devices = lax.axis_size(axis)
    pieces = [in_blocks(a, dim, devices) for a, dim in zip(arrays, dims)]
    lines = jnp.concatenate([b.reshape(devices, -1) for b in pieces], axis=1)
    span = max(16, -(-lines.shape[1] // 1024) * 8)
    lines = jnp.pad(lines, ((0, 0), (0, span * 128 - lines.shape[1]))).reshape(-1, 128)
    vector, at, outs = (lax.psum_scatter(lines, axis, tiled=True).reshape(-1), 0, [])
    for b in pieces:
        part = b[0]
        outs.append(vector[at : at + part.size].reshape(part.shape))
        at += part.size
    return tuple(outs)


def lookup_rows(indices, table_rows):
    one_hot = (
        indices[:, None] == jnp.arange(table_rows.shape[0], dtype=jnp.int32)[None, :]
    ).astype(table_rows.dtype)
    return jnp.dot(one_hot, table_rows, preferred_element_type=jnp.float32)


def attend(qkv_sums, heads_here):
    batch_rows, seq_len = (qkv_sums.shape[0], qkv_sums.shape[1])
    heads_qkv = qkv_sums.astype(jnp.bfloat16).reshape(batch_rows, seq_len, heads_here, 3, HD)
    queries, key_rows, values = (
        heads_qkv[:, :, :, 0],
        heads_qkv[:, :, :, 1],
        heads_qkv[:, :, :, 2],
    )
    scores = jnp.einsum(
        "blhe,bmhe->bhlm", queries, key_rows, preferred_element_type=jnp.float32
    ) * (1.0 / math.sqrt(HD))
    exponent = jnp.exp(scores - jnp.max(scores, axis=-1, keepdims=True))
    attn_prob = exponent / jnp.sum(exponent, axis=-1, keepdims=True)
    prob_low = attn_prob.astype(jnp.bfloat16)
    attn_mixed = jnp.einsum("bhlm,bmhe->blhe", prob_low, values, preferred_element_type=jnp.float32)
    attn_mixed = attn_mixed.astype(jnp.bfloat16).reshape(batch_rows, seq_len, heads_here * HD)
    return (heads_qkv, attn_prob, prob_low, attn_mixed)


def attend_grad(heads_qkv, attn_prob, prob_low, grad_low):
    batch_rows, seq_len = (heads_qkv.shape[0], heads_qkv.shape[1])
    queries, key_rows, values = (
        heads_qkv[:, :, :, 0],
        heads_qkv[:, :, :, 1],
        heads_qkv[:, :, :, 2],
    )
    grad_probs = jnp.einsum("blhe,bmhe->bhlm", grad_low, values, preferred_element_type=jnp.float32)
    row_delta = jnp.sum(attn_prob * grad_probs, axis=-1, keepdims=True)
    grad_scores = (attn_prob * (grad_probs - row_delta) * (1.0 / math.sqrt(HD))).astype(
        jnp.bfloat16
    )
    grad_query = jnp.einsum(
        "bhlm,bmhe->blhe", grad_scores, key_rows, preferred_element_type=jnp.float32
    )
    grad_keys = jnp.einsum(
        "bhlm,blhe->bmhe", grad_scores, queries, preferred_element_type=jnp.float32
    )
    grad_values = jnp.einsum(
        "bhlm,blhe->bmhe", prob_low, grad_low, preferred_element_type=jnp.float32
    )
    grad_qkv_act = jnp.stack([grad_query, grad_keys, grad_values], axis=3).astype(jnp.bfloat16)
    return grad_qkv_act.reshape(batch_rows, seq_len, -1)


def forward(normed, wide_mod, qkv_weight, heads_here):
    full_rows = (
        normed.astype(jnp.float32) * (1.0 + wide_mod[:, 1][:, None]) + wide_mod[:, 0][:, None]
    ).astype(jnp.bfloat16)
    qkv_sums = jnp.einsum("bld,df->blf", full_rows, qkv_weight, preferred_element_type=jnp.float32)
    return attend(qkv_sums, heads_here)


def local(
    noisy,
    labels,
    tsteps,
    guide_index,
    class_table,
    time_table,
    guide_table,
    guide_weights,
    teacher_qkv,
    teacher_out,
    teacher_ada,
    student_qkv,
    student_out,
    student_ada,
):
    samples, seq_len, width_part = noisy.shape
    model_width = width_part * lax.axis_size("tensor")
    dp = lax.axis_size("dp")
    batch_size = samples * dp
    heads_here = student_out.shape[0] // HD
    wide = lax.all_gather(noisy, "tensor", axis=2, tiled=True)
    null_class = class_table.shape[0] - 1
    time_embed = lookup_rows(tsteps, time_table)
    cond_embed = lookup_rows(labels, class_table) + time_embed
    null_embed = class_table[null_class].astype(jnp.float32)[None, :] + time_embed
    guide_hot = guide_index[:, None] == jnp.arange(guide_table.shape[0], dtype=jnp.int32)[None, :]
    student_embed = cond_embed + jnp.dot(
        guide_hot.astype(jnp.bfloat16), guide_table, preferred_element_type=jnp.float32
    )
    strength = jnp.sum(jnp.where(guide_hot, guide_weights[None, :], 0.0), axis=1)
    cond_act = jax.nn.silu(cond_embed).astype(jnp.bfloat16)
    null_act = jax.nn.silu(null_embed).astype(jnp.bfloat16)
    student_act = jax.nn.silu(student_embed).astype(jnp.bfloat16)
    teacher_act = jnp.concatenate([cond_act, null_act], axis=0)
    mod_t = jnp.einsum("bd,kde->bke", teacher_act, teacher_ada, preferred_element_type=jnp.float32)
    mod_s = jnp.einsum("bd,kde->bke", student_act, student_ada, preferred_element_type=jnp.float32)
    wide_mod = collect(jnp.concatenate([mod_t, mod_s], axis=0), "tensor", 2)
    cond_mod, null_mod, student_mod = (
        wide_mod[:samples],
        wide_mod[samples : 2 * samples],
        wide_mod[2 * samples :],
    )
    scale_norm = 1.0 / math.sqrt(batch_size * seq_len)
    signal = wide.astype(jnp.float32)
    row_mean = jnp.sum(signal, axis=2) / model_width
    row_var = jnp.sum(signal * signal, axis=2) / model_width - row_mean * row_mean
    normed = ((signal - row_mean[:, :, None]) * lax.rsqrt(row_var + norm_eps)[:, :, None]).astype(
        jnp.bfloat16
    )
    teacher_mixed = forward(
        jnp.concatenate([normed, normed], axis=0), wide_mod[: 2 * samples], teacher_qkv, heads_here
    )[3]
    heads_qkv, attn_prob, prob_low, attn_mixed = forward(
        normed, student_mod, student_qkv, heads_here
    )
    teacher_part = jnp.einsum(
        "blf,fd->bld", teacher_mixed, teacher_out, preferred_element_type=jnp.float32
    )
    student_part = jnp.einsum(
        "blf,fd->bld", attn_mixed, student_out, preferred_element_type=jnp.float32
    )
    gate = student_mod[:, 2] * scale_norm
    cond_gate = (1.0 + strength)[:, None] * cond_mod[:, 2] * scale_norm
    null_gate = strength[:, None] * null_mod[:, 2] * scale_norm
    partial_cot = (
        gate[:, None] * student_part
        - cond_gate[:, None] * teacher_part[:samples]
        + null_gate[:, None] * teacher_part[samples:]
    )
    piece = lax.psum_scatter(
        partial_cot.astype(jnp.bfloat16), "tensor", scatter_dimension=2, tiled=True
    )
    cotangent = lax.all_gather(piece, "tensor", axis=2, tiled=True)
    grad_proj = (cotangent.astype(jnp.float32) * student_mod[:, 2][:, None]).astype(jnp.bfloat16)
    grad_mixed = jnp.einsum(
        "bld,ed->ble", grad_proj, student_out, preferred_element_type=jnp.float32
    )
    image_out = jnp.einsum("ble,bld->bed", attn_mixed, cotangent, preferred_element_type=jnp.float32)
    grad_out_rows = jnp.sum(image_out * student_mod[:, 2][:, None], axis=0)
    grad_gate = jnp.sum(image_out * student_out.astype(jnp.float32)[None], axis=1)
    grad_low = grad_mixed.astype(jnp.bfloat16).reshape(samples, seq_len, heads_here, HD)
    grad_qkv_act = attend_grad(heads_qkv, attn_prob, prob_low, grad_low)
    image_qkv = jnp.einsum("bld,blf->bdf", normed, grad_qkv_act, preferred_element_type=jnp.float32)
    column_sums = jnp.sum(grad_qkv_act.astype(jnp.float32), axis=1)
    grad_qkv_local = jnp.sum(
        image_qkv * (1.0 + student_mod[:, 1])[:, :, None]
        + student_mod[:, 0][:, :, None] * column_sums[:, None, :],
        axis=0,
    )
    weight = student_qkv.astype(jnp.float32)
    grad_scale = jnp.sum(image_qkv * weight[None], axis=2)
    grad_shift = jnp.einsum("bf,df->bd", column_sums, weight, precision=lax.Precision.HIGHEST)
    grad_modulation = lax.psum_scatter(
        jnp.stack([grad_shift, grad_scale, grad_gate], axis=1),
        "tensor",
        scatter_dimension=2,
        tiled=True,
    )
    all_mod = lax.all_gather(grad_modulation, "dp", axis=0, tiled=True)
    act_rows = lax.all_to_all(student_act, "dp", split_axis=1, concat_axis=0, tiled=True)
    grad_ada = jnp.einsum(
        "bd,bke->kde", act_rows.astype(jnp.float32), all_mod, precision=lax.Precision.HIGHEST
    )
    grad_qkv = lax.psum_scatter(
        grad_qkv_local.astype(jnp.bfloat16), "dp", scatter_dimension=0, tiled=True
    ).astype(jnp.float32)
    grad_out = lax.psum_scatter(
        grad_out_rows.astype(jnp.bfloat16), "dp", scatter_dimension=1, tiled=True
    ).astype(jnp.float32)
    return (grad_qkv, grad_out, grad_ada)


def solution(mesh):
    return jax.shard_map(
        local,
        mesh=mesh,
        in_specs=(
            P("dp", None, "tensor"),
            P("dp"),
            P("dp"),
            P("dp"),
            P(),
            P(),
            P(),
            P(),
            P(None, "tensor"),
            P("tensor", None),
            P(None, None, "tensor"),
            P(None, "tensor"),
            P("tensor", None),
            P(None, None, "tensor"),
        ),
        out_specs=(P("dp", "tensor"), P("tensor", "dp"), P(None, "dp", "tensor")),
        check_vma=False,
    )
```

```python
import math

import jax
import jax.numpy as jnp
from jax import lax
from jax.experimental import pallas as pl
from jax.experimental.pallas import tpu as pltpu
from jax.sharding import PartitionSpec as P

HD = 72
HW = 3 * HD
norm_eps = 1e-06
F32 = jnp.float32
BF16 = jnp.bfloat16
MESH = pl.DeviceIdType.MESH


def lookup_rows(indices, table_rows):
    one_hot = (
        indices[:, None] == jnp.arange(table_rows.shape[0], dtype=jnp.int32)[None, :]
    ).astype(table_rows.dtype)
    return jnp.dot(one_hot, table_rows, preferred_element_type=F32)


def dot(a, b, ca, cb):
    return lax.dot_general(a, b, (((ca,), (cb,)), ((), ())), preferred_element_type=F32)


def make_kernel(n_t, n_dp, images, seq, norm_scale):
    chips = n_t // 2
    width = HD * n_t
    block = 2 * HD
    dp_rows = width // n_dp

    def kernel(
        noisy, mods, acts, wq_t, wq_s, wo_t, wo_s,
        gq_out, go_out, gm_out, act_out,
        noisy_g, mod_g, mod_i, wq_g, wo_g, wq_cat, wo_cat, wo_tr,
        normed, mod_s, mod_t, mixed, proj_s, prob, qkv_s,
        part, rs_in, cot, gp, gqkv, acc_q, acc_o, gmod, gm_in, gm_sum,
        pair_q, pair_o, pair_q_in, pair_o_in, dp_q, dp_o, dp_q_in, dp_o_in,
        s_ag, r_ag, s_mod, r_mod, s_w, r_w, s_act, r_act, l_sem,
        s_rs, r_rs, s_c, r_c, s_gm, r_gm, s_pair, r_pair,
        s_dq, r_dq, s_do, r_do, s_gd, r_gd,
    ):
        t = lax.axis_index("tensor")
        j = lax.axis_index("dp")
        chip = t // 2
        core = lax.rem(t, 2)
        mate = 1 - core
        mate_t = 2 * chip + mate

        barrier = pltpu.get_barrier_semaphore()
        for d in range(1, n_t):
            pl.semaphore_signal(
                barrier, inc=1, device_id={"tensor": lax.rem(t + d, n_t)}, device_id_type=MESH
            )
        for d in range(1, n_dp):
            pl.semaphore_signal(
                barrier, inc=1, device_id={"dp": lax.rem(j + d, n_dp)}, device_id_type=MESH
            )
        pl.semaphore_wait(barrier, n_t + n_dp - 2)

        def to_tensor(src, dst, ss, rs, peer):
            return pltpu.make_async_remote_copy(
                src_ref=src, dst_ref=dst, send_sem=ss, recv_sem=rs,
                device_id={"tensor": peer}, device_id_type=MESH,
            )

        def to_dp(src, dst, ss, rs, peer):
            return pltpu.make_async_remote_copy(
                src_ref=src, dst_ref=dst, send_sem=ss, recv_sem=rs,
                device_id={"dp": peer}, device_id_type=MESH,
            )

        def mod_copy(d):
            peer = lax.rem(t + d, n_t)
            return to_tensor(
                mods.at[lax.rem(peer, 2)], mod_g.at[t], s_mod.at[d], r_mod.at[d], peer
            )

        def ag_copy(i, d):
            peer = lax.rem(t + d, n_t)
            return to_tensor(
                noisy.at[images * lax.rem(peer, 2) + i], noisy_g.at[i, t],
                s_ag.at[i, d], r_ag.at[i, d], peer,
            )

        def w_copies():
            return [
                to_tensor(wq_t, wq_g.at[0, core], s_w.at[0], r_w.at[0], mate_t),
                to_tensor(wq_s, wq_g.at[1, core], s_w.at[1], r_w.at[1], mate_t),
                to_tensor(wo_t, wo_g.at[0, core], s_w.at[2], r_w.at[2], mate_t),
                to_tensor(wo_s, wo_g.at[1, core], s_w.at[3], r_w.at[3], mate_t),
            ]

        def act_copy(d):
            peer = lax.rem(j + d, n_dp)
            return to_dp(
                acts.at[pl.ds(pl.multiple_of(peer * dp_rows, 16), dp_rows)], act_out.at[j],
                s_act.at[d], r_act.at[d], peer,
            )

        locals_ = [
            pltpu.make_async_copy(mods.at[core], mod_g.at[t], l_sem.at[0]),
            pltpu.make_async_copy(wq_t, wq_g.at[0, core], l_sem.at[1]),
            pltpu.make_async_copy(wq_s, wq_g.at[1, core], l_sem.at[2]),
            pltpu.make_async_copy(wo_t, wo_g.at[0, core], l_sem.at[3]),
            pltpu.make_async_copy(wo_s, wo_g.at[1, core], l_sem.at[4]),
            pltpu.make_async_copy(
                acts.at[pl.ds(pl.multiple_of(j * dp_rows, 16), dp_rows)], act_out.at[j], l_sem.at[5]
            ),
        ]
        for i in range(images):
            locals_.append(
                pltpu.make_async_copy(
                    noisy.at[images * core + i], noisy_g.at[i, t], l_sem.at[6 + i]
                )
            )
        for copy in w_copies():
            copy.start()
        for d in range(1, n_t):
            mod_copy(d).start()
        for copy in locals_:
            copy.start()
        for i in range(images):
            for d in range(1, n_t):
                ag_copy(i, d).start()
        for d in range(1, n_dp):
            act_copy(d).start()

        for copy in locals_:
            copy.wait()
        for copy in w_copies():
            copy.wait_recv()
        for m in range(2):
            for h in range(2):
                flat = wq_g[m, h].astype(F32)
                wq_cat[m, HW * h : HW * (h + 1), :] = jnp.transpose(flat)
                wo_cat[m, HD * h : HD * (h + 1), :] = wo_g[m, h].astype(F32)
        for m in range(2):
            wo_tr[m] = jnp.transpose(wo_cat[m]).astype(BF16)

        for d in range(1, n_t):
            mod_copy(d).wait_recv()
        for src in range(n_t):
            piece = mod_g[src].astype(F32)
            for b in range(images):
                shifted = piece if b == 0 else pltpu.roll(piece, 128 - 16 * b, 1)
                mod_i[b, HD * src : HD * (src + 1), :] = shifted

        acc_q[...] = jnp.zeros_like(acc_q)
        acc_o[...] = jnp.zeros_like(acc_o)
        gmod[...] = jnp.zeros_like(gmod)

        def rs_copy(i, d):
            peer = lax.rem(chip + d, chips)
            return to_tensor(
                part.at[i, peer], rs_in.at[i, chip], s_rs.at[i, d], r_rs.at[i, d], 2 * peer + core
            )

        def cot_copy(i, d):
            peer = lax.rem(chip + d, chips)
            return to_tensor(
                cot.at[i, chip], cot.at[i, chip], s_c.at[i, d], r_c.at[i, d], 2 * peer + core
            )

        def scores_of(q, k):
            scores = dot(k, q, 0, 0) * (1.0 / math.sqrt(HD))
            exponent = jnp.exp(scores - jnp.max(scores, axis=0, keepdims=True))
            return exponent * (1.0 / jnp.sum(exponent, axis=0, keepdims=True))

        def forward(i):
            for d in range(1, n_t):
                peer = lax.rem(t + d, n_t)
                to_tensor(
                    noisy.at[0], noisy_g.at[i, lax.rem(t + n_t - d, n_t)],
                    s_ag.at[i, d], r_ag.at[i, d], peer,
                ).wait_recv()
            total = jnp.zeros((1, seq), F32)
            square = jnp.zeros((1, seq), F32)
            for src in range(n_t):
                x = noisy_g[i, src].astype(F32)
                total = total + jnp.sum(x, axis=0, keepdims=True)
                square = square + jnp.sum(x * x, axis=0, keepdims=True)
            mean = total * (1.0 / width)
            rstd = lax.rsqrt(square * (1.0 / width) - mean * mean + norm_eps)
            for c in range(chips):
                rows = slice(block * c, block * (c + 1))
                x = jnp.concatenate(
                    [noisy_g[i, 2 * c].astype(F32), noisy_g[i, 2 * c + 1].astype(F32)], axis=0
                )
                n = ((x - mean) * rstd).astype(BF16)
                normed[i, rows, :] = n
                n = n.astype(F32)
                for a in range(3):
                    shift = mod_i[i, rows, 3 * a : 3 * a + 1]
                    scale = mod_i[i, rows, 3 * a + 1 : 3 * a + 2]
                    value = (n * (1.0 + scale) + shift).astype(BF16)
                    if a == 2:
                        mod_s[i, rows, :] = value
                    else:
                        mod_t[a, rows, :] = value
            for a in range(3):
                weight = wq_cat[0 if a < 2 else 1].astype(BF16)
                act = mod_s[i] if a == 2 else mod_t[a]
                qkv = dot(weight, act, 1, 0)
                heads = []
                for h in range(2):
                    q, k, v = (
                        qkv[HW * h + HD * e : HW * h + HD * (e + 1)].astype(BF16) for e in range(3)
                    )
                    p = scores_of(q, k)
                    heads.append(dot(v, p.astype(BF16), 1, 0))
                    if a == 2:
                        prob[i, h] = p
                        for e, value in enumerate((q, k, v)):
                            qkv_s[i, h, e] = value
                mixed[a] = jnp.concatenate(heads, axis=0).astype(BF16)
            for h in range(2):
                mixed_h = mixed[2].astype(F32)[HD * h : HD * (h + 1)]
                gqkv[i, h, 0:HD, :] = mixed_h.astype(BF16)
            for c in range(chips):
                rows = slice(block * c, block * (c + 1))
                sums = jnp.zeros((block, seq), F32)
                for a in range(3):
                    value = dot(wo_tr[0 if a < 2 else 1, rows, :], mixed[a], 1, 0)
                    gate = mod_i[i, rows, 3 * a + 2 : 3 * a + 3]
                    if a == 2:
                        proj_s[i, rows, :] = value.astype(BF16)
                        gate = gate * norm_scale
                    sums = sums + value * gate
                part[i, c] = sums.astype(BF16)
            for d in range(1, chips):
                rs_copy(i, d).start()

        def reduce(i):
            for d in range(1, chips):
                rs_copy(i, d).wait_recv()
            sums = part[i, chip].astype(F32)
            for d in range(1, chips):
                sums = sums + rs_in[i, lax.rem(chip + d, chips)].astype(F32)
            cot[i, chip] = sums.astype(BF16)
            for d in range(1, chips):
                cot_copy(i, d).start()

        def backward(i):
            for d in range(1, chips):
                cot_copy(i, d).wait_recv()
            grads = []
            for c in range(chips):
                rows = slice(block * c, block * (c + 1))
                value = cot[i, c].astype(F32)
                gp[rows, :] = (value * mod_i[i, rows, 8:9]).astype(BF16)
                grads.append(
                    jnp.sum(value * proj_s[i, rows, :].astype(F32), axis=1, keepdims=True)
                )
            grad_gate = jnp.concatenate(grads, axis=0)
            grad_mixed = dot(wo_cat[1].astype(BF16), gp[...], 1, 0)
            grad_input = jnp.zeros((width, seq), F32)
            for h in range(2):
                low = grad_mixed[HD * h : HD * (h + 1)].astype(BF16)
                acc_o[h] += dot(gp[...], gqkv[i, h, 0:HD, :], 1, 1)
                q, k, v = (qkv_s[i, h, e] for e in range(3))
                p = prob[i, h]
                grad_prob = dot(v, low, 0, 0)
                delta = jnp.sum(p * grad_prob, axis=0, keepdims=True)
                ds = (p * (grad_prob - delta) * (1.0 / math.sqrt(HD))).astype(BF16)
                grad_q = dot(k, ds, 1, 0)
                grad_k = dot(q, ds, 1, 1)
                grad_v = dot(low, p.astype(BF16), 1, 1)
                gqkv[i, h] = jnp.concatenate([grad_q, grad_k, grad_v], axis=0).astype(BF16)
                grad_act = gqkv[i, h]
                acc_q[h] += dot(mod_s[i], grad_act, 1, 1)
                grad_input = grad_input + dot(wq_g[1, h], grad_act, 1, 0)
            grad_shift = jnp.sum(grad_input, axis=1, keepdims=True)
            grad_scale = jnp.sum(grad_input * normed[i].astype(F32), axis=1, keepdims=True)
            lane = lax.broadcasted_iota(jnp.int32, (width, 128), 1)
            gmod[...] += (
                jnp.where(lane == 4 * i, grad_shift, 0.0)
                + jnp.where(lane == 4 * i + 1, grad_scale, 0.0)
                + jnp.where(lane == 4 * i + 2, grad_gate, 0.0)
            )

        def forward_step(i, carry):
            forward(i)

            @pl.when(i > 0)
            def _():
                reduce(i - 1)

            return carry

        lax.fori_loop(0, images, forward_step, 0)

        def backward_step(i, carry):
            backward(i)

            @pl.when(i == 0)
            def _():
                reduce(images - 1)

            return carry

        lax.fori_loop(0, images, backward_step, 0)

        def gm_copy(d):
            peer = lax.rem(t + d, n_t)
            return to_tensor(
                gmod.at[pl.ds(pl.multiple_of(peer * HD, 8), HD)], gm_in.at[t],
                s_gm.at[d], r_gm.at[d], peer,
            )

        def pair_copies():
            return [
                to_tensor(pair_q, pair_q_in, s_pair.at[0], r_pair.at[0], mate_t),
                to_tensor(pair_o, pair_o_in, s_pair.at[1], r_pair.at[1], mate_t),
            ]

        def dp_copies(d):
            peer = lax.rem(j + d, n_dp)
            return [
                to_dp(dp_q.at[peer], dp_q_in.at[j], s_dq.at[d], r_dq.at[d], peer),
                to_dp(dp_o.at[peer], dp_o_in.at[j], s_do.at[d], r_do.at[d], peer),
            ]

        def gd_copy(d):
            peer = lax.rem(j + d, n_dp)
            return to_dp(gm_sum, gm_out.at[j], s_gd.at[d], r_gd.at[d], peer)

        pair_q[...] = acc_q[mate].astype(BF16)
        pair_o[...] = acc_o[mate].astype(BF16)
        for copy in pair_copies():
            copy.start()
        for d in range(1, n_t):
            gm_copy(d).start()
        for copy in pair_copies():
            copy.wait_recv()
        for s in range(n_dp):
            rows = slice(dp_rows * s, dp_rows * (s + 1))
            dp_q[s] = (acc_q[core, rows, :] + pair_q_in[rows, :].astype(F32)).astype(BF16)
            dp_o[s] = (acc_o[core, rows, :] + pair_o_in[rows, :].astype(F32)).astype(BF16)
        for d in range(1, n_dp):
            for copy in dp_copies(d):
                copy.start()
        for d in range(1, n_t):
            gm_copy(d).wait_recv()
        own = gmod[pl.ds(pl.multiple_of(t * HD, 8), HD), :]
        gm_in[t] = own
        even = gm_in[0]
        odd = gm_in[1]
        for c in range(1, chips):
            even = even + gm_in[2 * c]
            odd = odd + gm_in[2 * c + 1]
        both = even + pltpu.roll(odd, 4 * images, 1)
        gm_sum[...] = both
        gm_out[j] = both
        for d in range(1, n_dp):
            gd_copy(d).start()
        total_q = dp_q[j].astype(F32)
        total_o = dp_o[j].astype(F32)
        for d in range(1, n_dp):
            for copy in dp_copies(d):
                copy.wait_recv()
        for d in range(1, n_dp):
            src = lax.rem(j + d, n_dp)
            total_q = total_q + dp_q_in[src].astype(F32)
            total_o = total_o + dp_o_in[src].astype(F32)
        gq_out[...] = total_q
        go_out[...] = jnp.transpose(total_o)
        for d in range(1, n_dp):
            gd_copy(d).wait_recv()
            act_copy(d).wait_recv()

        for copy in w_copies() + pair_copies():
            copy.wait_send()
        for d in range(1, n_t):
            mod_copy(d).wait_send()
            gm_copy(d).wait_send()
            for i in range(images):
                ag_copy(i, d).wait_send()
        for d in range(1, chips):
            for i in range(images):
                rs_copy(i, d).wait_send()
                cot_copy(i, d).wait_send()
        for d in range(1, n_dp):
            act_copy(d).wait_send()
            gd_copy(d).wait_send()
            for copy in dp_copies(d):
                copy.wait_send()

    vm = pltpu.VMEM
    dma = pltpu.SemaphoreType.DMA
    scratch = [
        vm((images, n_t, HD, seq), BF16),
        vm((n_t, HD, 128), BF16),
        vm((images, width, 128), F32),
        vm((2, 2, width, HW), BF16),
        vm((2, 2, HD, width), BF16),
        vm((2, 2 * HW, width), F32),
        vm((2, 2 * HD, width), F32),
        vm((2, width, 2 * HD), BF16),
        vm((images, width, seq), BF16),
        vm((images, width, seq), BF16),
        vm((2, width, seq), BF16),
        vm((3, 2 * HD, seq), BF16),
        vm((images, width, seq), BF16),
        vm((images, 2, seq, seq), F32),
        vm((images, 2, 3, HD, seq), BF16),
        vm((images, chips, block, seq), BF16),
        vm((images, chips, block, seq), BF16),
        vm((images, chips, block, seq), BF16),
        vm((width, seq), BF16),
        vm((images, 2, HW, seq), BF16),
        vm((2, width, HW), F32),
        vm((2, width, HD), F32),
        vm((width, 128), F32),
        vm((n_t, HD, 128), F32),
        vm((HD, 128), F32),
        vm((width, HW), BF16),
        vm((width, HD), BF16),
        vm((width, HW), BF16),
        vm((width, HD), BF16),
        vm((n_dp, dp_rows, HW), BF16),
        vm((n_dp, dp_rows, HD), BF16),
        vm((n_dp, dp_rows, HW), BF16),
        vm((n_dp, dp_rows, HD), BF16),
        dma((images, n_t)),
        dma((images, n_t)),
        dma((n_t,)),
        dma((n_t,)),
        dma((4,)),
        dma((4,)),
        dma((n_dp,)),
        dma((n_dp,)),
        dma((6 + images,)),
        dma((images, chips)),
        dma((images, chips)),
        dma((images, chips)),
        dma((images, chips)),
        dma((n_t,)),
        dma((n_t,)),
        dma((2,)),
        dma((2,)),
        dma((n_dp,)),
        dma((n_dp,)),
        dma((n_dp,)),
        dma((n_dp,)),
        dma((n_dp,)),
        dma((n_dp,)),
    ]
    any_spec = pl.BlockSpec(memory_space=pl.ANY)
    vmem_spec = pl.BlockSpec(memory_space=pltpu.VMEM)
    return pl.pallas_call(
        kernel,
        out_shape=(
            jax.ShapeDtypeStruct((dp_rows, HW), F32),
            jax.ShapeDtypeStruct((HD, dp_rows), F32),
            jax.ShapeDtypeStruct((n_dp, HD, 128), F32),
            jax.ShapeDtypeStruct((n_dp, dp_rows, 128), BF16),
        ),
        in_specs=[any_spec] * 7,
        out_specs=(vmem_spec,) * 4,
        scratch_shapes=scratch,
        compiler_params=pltpu.CompilerParams(
            collective_id=0, has_side_effects=True, vmem_limit_bytes=60 * 1024 * 1024
        ),
        name="step",
    )


def local(
    noisy,
    labels,
    tsteps,
    guide_index,
    class_table,
    time_table,
    guide_table,
    guide_weights,
    teacher_qkv,
    teacher_out,
    teacher_ada,
    student_qkv,
    student_out,
    student_ada,
):
    samples, seq_len, width_part = noisy.shape
    n_t = lax.axis_size("tensor")
    n_dp = lax.axis_size("dp")
    images = samples // 2
    batch_size = samples * n_dp
    norm_scale = 1.0 / math.sqrt(batch_size * seq_len)
    null_class = class_table.shape[0] - 1
    time_embed = lookup_rows(tsteps, time_table)
    cond_embed = lookup_rows(labels, class_table) + time_embed
    null_embed = class_table[null_class].astype(F32)[None, :] + time_embed
    guide_hot = guide_index[:, None] == jnp.arange(guide_table.shape[0], dtype=jnp.int32)[None, :]
    student_embed = cond_embed + jnp.dot(
        guide_hot.astype(BF16), guide_table, preferred_element_type=F32
    )
    strength = jnp.sum(jnp.where(guide_hot, guide_weights[None, :], 0.0), axis=1)
    cond_act = jax.nn.silu(cond_embed).astype(BF16)
    null_act = jax.nn.silu(null_embed).astype(BF16)
    student_act = jax.nn.silu(student_embed).astype(BF16)
    teacher_act = jnp.concatenate([cond_act, null_act], axis=0)
    mod_t = jnp.einsum("bd,kde->bke", teacher_act, teacher_ada, preferred_element_type=F32)
    mod_s = jnp.einsum("bd,kde->bke", student_act, student_ada, preferred_element_type=F32)
    mods = jnp.stack([mod_t[:samples], mod_t[samples:], mod_s], axis=1)
    ones = jnp.ones_like(strength)
    factor = jnp.stack(
        [-(1.0 + strength) * norm_scale, strength * norm_scale, ones], axis=1
    )
    mods = jnp.concatenate([mods[:, :, :2], mods[:, :, 2:] * factor[:, :, None, None]], axis=2)
    mods = mods.reshape(2, images, 9, width_part)
    mods = jnp.pad(mods, ((0, 0), (0, 0), (0, 7), (0, 0))).reshape(2, images * 16, width_part)
    mods = jnp.pad(
        jnp.swapaxes(mods, 1, 2), ((0, 0), (0, 0), (0, 128 - images * 16))
    ).astype(BF16)
    acts = jnp.pad(student_act.T, ((0, 0), (0, 128 - samples)))
    step = make_kernel(n_t, n_dp, images, seq_len, norm_scale)
    grad_qkv, grad_out, gm, act_rows = step(
        jnp.swapaxes(noisy, 1, 2), mods, acts,
        teacher_qkv, student_qkv, teacher_out, student_out,
    )
    gm = gm[:, :, : 4 * samples].reshape(n_dp, width_part, samples, 4)[..., :3]
    grad_ada = jnp.einsum(
        "jdb,jebk->kde",
        act_rows[:, :, :samples].astype(F32),
        gm,
        precision=lax.Precision.HIGHEST,
    )
    return (grad_qkv, grad_out, grad_ada)


def solution(mesh):
    return jax.shard_map(
        local,
        mesh=mesh,
        in_specs=(
            P("dp", None, "tensor"),
            P("dp"),
            P("dp"),
            P("dp"),
            P(),
            P(),
            P(),
            P(),
            P(None, "tensor"),
            P("tensor", None),
            P(None, None, "tensor"),
            P(None, "tensor"),
            P("tensor", None),
            P(None, None, "tensor"),
        ),
        out_specs=(P("dp", "tensor"), P("tensor", "dp"), P(None, "dp", "tensor")),
        check_vma=False,
    )
```

```python
import math

import jax
import jax.numpy as jnp
from jax import lax
from jax.experimental import pallas as pl
from jax.experimental.pallas import tpu as pltpu
from jax.sharding import PartitionSpec as P

HD = 72
HW = 3 * HD
HP = 80
norm_eps = 1e-06
F32 = jnp.float32
BF16 = jnp.bfloat16
MESH = pl.DeviceIdType.MESH
SPLIT = 40


def dot(a, b, ca, cb):
    return lax.dot_general(a, b, (((ca,), (cb,)), ((), ())), preferred_element_type=F32)


def iota(shape, dim):
    return lax.broadcasted_iota(jnp.int32, shape, dim)


def make_kernel(n_t, n_dp, samples, seq, norm_scale):
    chips = n_t // 2
    n_x = chips // 2
    images = samples // 2
    width = HD * n_t
    block = 2 * HD
    dp_rows = width // n_dp
    groups = HD // 8

    def kernel(
        labels, tsteps, guides, strengths,
        noisy, tab_c, tab_t, tab_g, wq_t, wq_s, wo_t, wo_s, ada_t, ada_s,
        gq_out, go_out, ga_out,
        noisy_p, noisy_g, c_tab, t_tab, g_tab, a_tab, mods, mod_g, mod_i, acts, act_g,
        wq_g, wo_g, wq_cat, wq_tr, wo_cat, wo_tr,
        normed, mod_s, mod_t, mixed, mixed_s, proj_s, prob, qkv_s,
        part, rs_in, cot, gp, gqkv, acc_q, acc_o, gmod, gm_send, gm_in, gm_sum, gm_all,
        pair_q, pair_o, pair_q_in, pair_o_in, dp_q, dp_o, dp_q_in, dp_o_in,
        l_sem, s_n, r_n, s_w, r_w, s_mod, r_mod, s_act, r_act,
        s_ag, r_ag, s_rs, r_rs, s_c, r_c, s_gm, r_gm, s_pair, r_pair,
        s_dq, r_dq, s_do, r_do, s_gd, r_gd,
    ):
        t = lax.axis_index("tensor")
        j = lax.axis_index("dp")
        chip = t // 2
        core = lax.rem(t, 2)
        x = chip // 2
        z = lax.rem(chip, 2)
        mate = 1 - core
        mate_t = 2 * chip + mate
        chip_z = 2 * x + 1 - z

        loads = [
            pltpu.make_async_copy(tab_c, c_tab, l_sem.at[0]),
            pltpu.make_async_copy(tab_t, t_tab, l_sem.at[1]),
            pltpu.make_async_copy(tab_g, g_tab, l_sem.at[2]),
            pltpu.make_async_copy(ada_t, a_tab.at[0], l_sem.at[3]),
            pltpu.make_async_copy(ada_s, a_tab.at[1], l_sem.at[4]),
            pltpu.make_async_copy(wq_t, wq_g.at[0, core], l_sem.at[5]),
            pltpu.make_async_copy(wq_s, wq_g.at[1, core], l_sem.at[6]),
            pltpu.make_async_copy(wo_t, wo_g.at[0, core], l_sem.at[7]),
            pltpu.make_async_copy(wo_s, wo_g.at[1, core], l_sem.at[8]),
        ]
        own_noisy = pltpu.make_async_copy(
            noisy.at[pl.ds(images * core, images)], noisy_p.at[core], l_sem.at[9]
        )
        own_noisy.start()
        for copy in loads:
            copy.start()

        barrier = pltpu.get_barrier_semaphore()
        for d in range(1, n_t):
            pl.semaphore_signal(
                barrier, inc=1, device_id={"tensor": lax.rem(t + d, n_t)}, device_id_type=MESH
            )
        for d in range(1, n_dp):
            pl.semaphore_signal(
                barrier, inc=1, device_id={"dp": lax.rem(j + d, n_dp)}, device_id_type=MESH
            )
        pl.semaphore_wait(barrier, n_t + n_dp - 2)

        def to_tensor(src, dst, ss, rs, peer):
            return pltpu.make_async_remote_copy(
                src_ref=src, dst_ref=dst, send_sem=ss, recv_sem=rs,
                device_id={"tensor": peer}, device_id_type=MESH,
            )

        def to_dp(src, dst, ss, rs, peer):
            return pltpu.make_async_remote_copy(
                src_ref=src, dst_ref=dst, send_sem=ss, recv_sem=rs,
                device_id={"dp": peer}, device_id_type=MESH,
            )

        def x_chip(d):
            return 2 * lax.rem(x + d, n_x) + z

        def device_of(c):
            return 2 * c + core

        def gather_z(buf, i, ss, rs):
            own = buf.at[i, chip]
            first = [to_tensor(own, own, ss.at[i, 0], rs.at[i, 0], device_of(chip_z))]
            first += [
                to_tensor(own, own, ss.at[i, d], rs.at[i, d], device_of(x_chip(d)))
                for d in range(1, n_x)
            ]
            other = buf.at[i, chip_z]
            second = [
                to_tensor(other, other, ss.at[i, n_x + d], rs.at[i, n_x + d], device_of(x_chip(d)))
                for d in range(1, n_x)
            ]
            return first, second, first[:1]

        def gather_x(buf, i, ss, rs):
            own = buf.at[i, chip]
            first = [
                to_tensor(own, own, ss.at[i, d], rs.at[i, d], device_of(x_chip(d)))
                for d in range(1, n_x)
            ]
            ahead = len(first)
            first.append(to_tensor(own, own, ss.at[i, n_x], rs.at[i, n_x], device_of(chip_z)))
            second = []
            for d in range(1, n_x):
                other = buf.at[i, 2 * lax.rem(x + n_x - d, n_x) + z]
                second.append(
                    to_tensor(
                        other, other, ss.at[i, n_x + d], rs.at[i, n_x + d], device_of(chip_z)
                    )
                )
            return first, second, first[:ahead]

        def by_parity(i, even, odd):
            @pl.when(lax.rem(i, 2) == 0)
            def _():
                even()

            @pl.when(lax.rem(i, 2) == 1)
            def _():
                odd()

        def gather_start(buf, i, ss, rs):
            def run(form):
                for copy in form(buf, i, ss, rs)[0]:
                    copy.start()

            by_parity(i, lambda: run(gather_z), lambda: run(gather_x))

        def gather_pass(buf, i, ss, rs):
            def run(form):
                _, second, needed = form(buf, i, ss, rs)
                for copy in needed:
                    copy.wait_recv()
                for copy in second:
                    copy.start()

            by_parity(i, lambda: run(gather_z), lambda: run(gather_x))

        def gather_end(buf, i, ss, rs):
            def run(form):
                first, second, needed = form(buf, i, ss, rs)
                for copy in first + second:
                    if not any(copy is other for other in needed):
                        copy.wait_recv()

            by_parity(i, lambda: run(gather_z), lambda: run(gather_x))

        def sum_z(i):
            first = [
                to_tensor(
                    part.at[i, 2 * e + 1 - z], rs_in.at[i, e],
                    s_rs.at[i, e], r_rs.at[i, e], device_of(chip_z),
                )
                for e in range(n_x)
            ]
            second = [
                to_tensor(
                    part.at[i, x_chip(d)], rs_in.at[i, n_x + d],
                    s_rs.at[i, n_x + d], r_rs.at[i, n_x + d], device_of(x_chip(d)),
                )
                for d in range(1, n_x)
            ]
            return first, second

        def sum_x(i):
            first = [
                to_tensor(
                    part.at[i, pl.ds(2 * lax.rem(x + d, n_x), 2)], rs_in.at[i, pl.ds(2 * d, 2)],
                    s_rs.at[i, d], r_rs.at[i, d], device_of(x_chip(d)),
                )
                for d in range(1, n_x)
            ]
            second = [
                to_tensor(
                    part.at[i, chip_z], rs_in.at[i, 0], s_rs.at[i, 0], r_rs.at[i, 0],
                    device_of(chip_z),
                )
            ]
            return first, second

        def sum_start(i):
            def run(form):
                for copy in form(i)[0]:
                    copy.start()

            by_parity(i, lambda: run(sum_z), lambda: run(sum_x))

        def sum_pass(i):
            def even():
                first, second = sum_z(i)
                for copy in first:
                    copy.wait_recv()
                for d in range(1, n_x):
                    e = lax.rem(x + d, n_x)
                    total = part[i, 2 * e + z].astype(F32) + rs_in[i, e].astype(F32)
                    part[i, 2 * e + z] = total.astype(BF16)
                for copy in second:
                    copy.start()

            def odd():
                first, second = sum_x(i)
                for copy in first:
                    copy.wait_recv()
                total = part[i, chip_z].astype(F32)
                for d in range(1, n_x):
                    total = total + rs_in[i, 2 * d + 1 - z].astype(F32)
                part[i, chip_z] = total.astype(BF16)
                for copy in second:
                    copy.start()

            by_parity(i, even, odd)

        def sum_end(i):
            def even():
                for copy in sum_z(i)[1]:
                    copy.wait_recv()
                total = part[i, chip].astype(F32) + rs_in[i, x].astype(F32)
                for d in range(1, n_x):
                    total = total + rs_in[i, n_x + d].astype(F32)
                cot[i, chip] = total.astype(BF16)

            def odd():
                for copy in sum_x(i)[1]:
                    copy.wait_recv()
                total = part[i, chip].astype(F32) + rs_in[i, 0].astype(F32)
                for d in range(1, n_x):
                    total = total + rs_in[i, 2 * d + z].astype(F32)
                cot[i, chip] = total.astype(BF16)

            by_parity(i, even, odd)

        mate_noisy = to_tensor(
            noisy.at[pl.ds(images * mate, images)], noisy_p.at[core], s_n.at[0], r_n.at[0], mate_t
        )
        w_copies = [
            to_tensor(wq_t, wq_g.at[0, core], s_w.at[0], r_w.at[0], mate_t),
            to_tensor(wq_s, wq_g.at[1, core], s_w.at[1], r_w.at[1], mate_t),
            to_tensor(wo_t, wo_g.at[0, core], s_w.at[2], r_w.at[2], mate_t),
            to_tensor(wo_s, wo_g.at[1, core], s_w.at[3], r_w.at[3], mate_t),
        ]
        mate_noisy.start()
        for copy in w_copies:
            copy.start()
        own_noisy.wait()
        mate_noisy.wait_recv()
        for i in range(images):
            both = jnp.concatenate(
                [noisy_p[0, i].astype(F32), noisy_p[1, i].astype(F32)], axis=0
            )
            noisy_g[i, chip] = both.astype(BF16)
        for i in range(min(2, images)):
            gather_start(noisy_g, i, s_ag, r_ag)

        for copy in loads[:5]:
            copy.wait()

        def one_hot(ref, size):
            row = iota((samples, size), 0)
            lane = iota((samples, size), 1)
            hot = jnp.zeros((samples, size), F32)
            for b in range(samples):
                hot = jnp.where((row == b) & (lane == ref[b]), 1.0, hot)
            return hot.astype(BF16)

        def lookup(ref, table, size):
            whole = size // 16 * 16
            hot = one_hot(ref, whole + 16)
            last = table[whole:size, :].astype(F32)
            last = jnp.concatenate([last, jnp.zeros((16 - size + whole, width), F32)], axis=0)
            return dot(hot[:, :whole], table[0:whole, :], 1, 0) + dot(
                hot[:, whole:], last.astype(BF16), 1, 0
            )

        time_embed = lookup(tsteps, t_tab, tab_t.shape[0])
        classes = tab_c.shape[0] - 1
        cond_embed = lookup(labels, c_tab, classes) + time_embed
        null_row = c_tab[classes - 8 :, :].astype(F32)[8:9]
        null_embed = null_row + time_embed
        student_embed = cond_embed + dot(one_hot(guides, tab_g.shape[0]), g_tab[...], 1, 0)

        def silu(v):
            return v / (1.0 + jnp.exp(-v))

        student_act = silu(student_embed)
        teacher_act = jnp.concatenate([silu(cond_embed), silu(null_embed)], axis=0).astype(BF16)
        acts[...] = jnp.zeros_like(acts)
        acts[:, 0:samples] = jnp.transpose(student_act).astype(BF16)
        student_act = jnp.concatenate([student_act, jnp.zeros_like(student_act)], axis=0).astype(BF16)
        lane_t = iota((1, 2 * samples), 1)
        factor = jnp.zeros((1, 2 * samples), F32)
        for b in range(samples):
            strength = strengths[guides[b]]
            factor = jnp.where(lane_t == b, -(1.0 + strength) * norm_scale, factor)
            factor = jnp.where(lane_t == samples + b, strength * norm_scale, factor)
        spread = jnp.zeros((HD, 256), F32)
        for k in range(3):
            value_t = dot(a_tab[0, k], teacher_act, 1, 1)
            value_s = dot(a_tab[1, k], student_act, 1, 1)
            if k == 2:
                value_t = value_t * factor
            for first, value in ((0, value_t), (2, value_s)):
                row = iota((2 * samples, 256), 0)
                lane = iota((2 * samples, 256), 1)
                b = lax.rem(row, samples)
                kind = first + row // samples
                target = 128 * (b // images) + 16 * lax.rem(b, images) + 3 * kind + k
                hot = jnp.where((lane == target) & (kind < 3), 1.0, 0.0).astype(BF16)
                spread = spread + dot(value.astype(BF16), hot, 1, 0)
        for kk in range(2):
            half = spread[:, 128 * kk : 128 * (kk + 1)]
            low = jnp.concatenate(
                [pltpu.roll(half[SPLIT:], 64, 1), jnp.zeros((2 * SPLIT - HD, 128), F32)], axis=0
            )
            mods[kk] = (half[:SPLIT] + low).astype(BF16)

        def mod_copy(d):
            peer = lax.rem(t + d, n_t)
            return to_tensor(
                mods.at[lax.rem(peer, 2)], mod_g.at[t], s_mod.at[d], r_mod.at[d], peer
            )

        def act_copy(d):
            peer = lax.rem(j + d, n_dp)
            return to_dp(
                acts.at[pl.ds(pl.multiple_of(peer * dp_rows, 16), dp_rows)], act_g.at[j],
                s_act.at[d], r_act.at[d], peer,
            )

        for d in range(1, n_t):
            mod_copy(d).start()
        gather_pass(noisy_g, 0, s_ag, r_ag)
        if images > 2:
            gather_start(noisy_g, 2, s_ag, r_ag)
        for d in range(1, n_dp):
            act_copy(d).start()
        mod_g[t] = mods[core]
        act_g[j] = acts[pl.ds(pl.multiple_of(j * dp_rows, 16), dp_rows), :]

        for copy in loads[5:]:
            copy.wait()
        for copy in w_copies:
            copy.wait_recv()
        for m in range(2):
            both = jnp.concatenate([wq_g[m, 0].astype(F32), wq_g[m, 1].astype(F32)], axis=0)
            wq_cat[m] = both.astype(BF16)
            if m == 1:
                wq_tr[...] = jnp.transpose(both).astype(BF16)
            both = jnp.concatenate([wo_g[m, 0].astype(F32), wo_g[m, 1].astype(F32)], axis=0)
            if m == 1:
                wo_cat[...] = both.astype(BF16)
            wo_tr[m] = jnp.transpose(both).astype(BF16)
        acc_q[...] = jnp.zeros_like(acc_q)
        acc_o[...] = jnp.zeros_like(acc_o)
        gmod[...] = jnp.zeros_like(gmod)
        gather_pass(noisy_g, 1, s_ag, r_ag)
        if images > 3:
            gather_start(noisy_g, 3, s_ag, r_ag)

        for d in range(1, n_t):
            mod_copy(d).wait_recv()
        for src in range(n_t):
            piece = mod_g[src].astype(F32)
            for b in range(images):
                near = piece if b == 0 else pltpu.roll(piece, 128 - 16 * b, 1)
                far = pltpu.roll(piece, 64 - 16 * b, 1)
                mod_i[b, HD * src : HD * src + SPLIT, :] = near
                mod_i[b, HD * src + SPLIT : HD * (src + 1), :] = far[: HD - SPLIT]

        def padded(value):
            rows = jnp.zeros((HP - HD, seq), F32)
            return jnp.concatenate([value, rows], axis=0).astype(BF16)

        def attend(q, k, v):
            scores = dot(k, q, 0, 0) * (1.0 / math.sqrt(HD))
            exponent = jnp.exp(scores - jnp.max(scores, axis=0, keepdims=True))
            p = exponent * (1.0 / jnp.sum(exponent, axis=0, keepdims=True))
            return p, dot(v, p.astype(BF16), 1, 0)[:HD]

        def forward_in(i):
            gather_end(noisy_g, i, s_ag, r_ag)
            total = jnp.zeros((1, seq), F32)
            square = jnp.zeros((1, seq), F32)
            for c in range(chips):
                value = noisy_g[i, c].astype(F32)
                total = total + jnp.sum(value, axis=0, keepdims=True)
                square = square + jnp.sum(value * value, axis=0, keepdims=True)
            mean = total * (1.0 / width)
            rstd = lax.rsqrt(square * (1.0 / width) - mean * mean + norm_eps)
            for c in range(chips):
                rows = slice(block * c, block * (c + 1))
                n = ((noisy_g[i, c].astype(F32) - mean) * rstd).astype(BF16)
                normed[i, rows, :] = n
                n = n.astype(F32)
                for a in range(3):
                    shift = mod_i[i, rows, 3 * a : 3 * a + 1]
                    scale = mod_i[i, rows, 3 * a + 1 : 3 * a + 2]
                    value = (n * (1.0 + scale) + shift).astype(BF16)
                    if a == 2:
                        mod_s[i, rows, :] = value
                    else:
                        mod_t[a, rows, :] = value

        def forward_model(i, a):
            act = mod_s[i] if a == 2 else mod_t[a]
            qkv = dot(wq_cat[0 if a < 2 else 1], act, 1, 0)
            heads = []
            for h in range(2):
                q, k, v = (
                    padded(qkv[HW * h + HD * e : HW * h + HD * (e + 1)]) for e in range(3)
                )
                p, mix = attend(q, k, v)
                heads.append(mix)
                if a == 2:
                    prob[i, h] = p
                    mixed_s[i, h] = mix.astype(BF16)
                    for e, value in enumerate((q, k, v)):
                        qkv_s[i, h, e] = value
            mixed[a] = jnp.concatenate(heads, axis=0).astype(BF16)

        def forward_out(i):
            for c in range(chips):
                rows = slice(block * c, block * (c + 1))
                sums = jnp.zeros((block, seq), F32)
                for a in range(3):
                    value = dot(wo_tr[0 if a < 2 else 1, rows, :], mixed[a], 1, 0)
                    gate = mod_i[i, rows, 3 * a + 2 : 3 * a + 3]
                    if a == 2:
                        proj_s[i, rows, :] = value.astype(BF16)
                        gate = gate * norm_scale
                    sums = sums + value * gate
                part[i, c] = sums.astype(BF16)
            sum_start(i)

        def backward_in(i):
            gather_end(cot, i, s_c, r_c)
            grads = []
            for c in range(chips):
                rows = slice(block * c, block * (c + 1))
                value = cot[i, c].astype(F32)
                gp[rows, :] = (value * mod_i[i, rows, 8:9]).astype(BF16)
                grads.append(
                    jnp.sum(value * proj_s[i, rows, :].astype(F32), axis=1, keepdims=True)
                )
            grad_gate = jnp.concatenate(grads, axis=0)
            lane = iota((width, 128), 1)
            gmod[...] += jnp.where(lane == 8 + i, grad_gate, 0.0)
            grad_mixed = dot(wo_cat[...], gp[...], 1, 0)
            acts_grad = []
            for h in range(2):
                low = padded(grad_mixed[HD * h : HD * (h + 1)])
                acc_o[h] += dot(gp[...], mixed_s[i, h], 1, 1)
                q, k, v = (qkv_s[i, h, e] for e in range(3))
                p = prob[i, h]
                grad_prob = dot(v, low, 0, 0)
                delta = jnp.sum(p * grad_prob, axis=0, keepdims=True)
                ds = (p * (grad_prob - delta) * (1.0 / math.sqrt(HD))).astype(BF16)
                acts_grad.append(dot(k, ds, 1, 0)[:HD])
                acts_grad.append(dot(q, ds, 1, 1)[:HD])
                acts_grad.append(dot(low, p.astype(BF16), 1, 1)[:HD])
            gqkv[...] = jnp.concatenate(acts_grad, axis=0).astype(BF16)
            for h in range(2):
                head = jnp.concatenate(acts_grad[3 * h : 3 * h + 3], axis=0).astype(BF16)
                acc_q[h] += dot(mod_s[i], head, 1, 1)

        def backward_out(i):
            shifts = []
            scales = []
            for c in range(chips):
                rows = slice(block * c, block * (c + 1))
                value = dot(wq_tr[rows, :], gqkv[...], 1, 0)
                shifts.append(jnp.sum(value, axis=1, keepdims=True))
                scales.append(
                    jnp.sum(value * normed[i, rows, :].astype(F32), axis=1, keepdims=True)
                )
            lane = iota((width, 128), 1)
            gmod[...] += jnp.where(lane == i, jnp.concatenate(shifts, axis=0), 0.0) + jnp.where(
                lane == 4 + i, jnp.concatenate(scales, axis=0), 0.0
            )

        def forward_step(i, carry):
            forward_in(i)

            @pl.when(i < images - 2)
            def _():
                gather_pass(noisy_g, i + 2, s_ag, r_ag)

            forward_model(i, 0)

            @pl.when(i > 0)
            def _():
                sum_pass(i - 1)

            forward_model(i, 1)

            @pl.when(i > 1)
            def _():
                gather_pass(cot, i - 2, s_c, r_c)

            forward_model(i, 2)

            @pl.when(i > 0)
            def _():
                sum_end(i - 1)
                gather_start(cot, i - 1, s_c, r_c)

            forward_out(i)
            return carry

        lax.fori_loop(0, images, forward_step, 0)
        if images > 1:
            gather_pass(cot, images - 2, s_c, r_c)
        sum_pass(images - 1)

        def backward_step(i, carry):
            backward_in(i)

            @pl.when(i == 0)
            def _():
                sum_end(images - 1)
                gather_start(cot, images - 1, s_c, r_c)

            backward_out(i)

            @pl.when(i == 0)
            def _():
                gather_pass(cot, images - 1, s_c, r_c)

            return carry

        lax.fori_loop(0, images, backward_step, 0)

        def gm_copy(d):
            peer = lax.rem(t + d, n_t)
            return to_tensor(gm_send.at[peer], gm_in.at[t], s_gm.at[d], r_gm.at[d], peer)

        pair_copies = [
            to_tensor(pair_q, pair_q_in, s_pair.at[0], r_pair.at[0], mate_t),
            to_tensor(pair_o, pair_o_in, s_pair.at[1], r_pair.at[1], mate_t),
        ]

        def dp_copies(d):
            peer = lax.rem(j + d, n_dp)
            return [
                to_dp(dp_q.at[peer], dp_q_in.at[j], s_dq.at[d], r_dq.at[d], peer),
                to_dp(dp_o.at[peer], dp_o_in.at[j], s_do.at[d], r_do.at[d], peer),
            ]

        def gd_copy(d):
            peer = lax.rem(j + d, n_dp)
            return to_dp(gm_sum, gm_all.at[j], s_gd.at[d], r_gd.at[d], peer)

        pair_q[...] = acc_q[mate].astype(BF16)
        pair_o[...] = acc_o[mate].astype(BF16)
        for copy in pair_copies:
            copy.start()
        for src in range(n_t):
            packed = gmod[HD * src : HD * src + 8, :]
            for g in range(1, groups):
                rows = slice(HD * src + 8 * g, HD * src + 8 * (g + 1))
                packed = packed + pltpu.roll(gmod[rows, :], 12 * g, 1)
            gm_send[src] = packed
        for d in range(1, n_t):
            gm_copy(d).start()
        gm_in[t] = gm_send[t]
        for copy in pair_copies:
            copy.wait_recv()
        for s in range(n_dp):
            rows = slice(dp_rows * s, dp_rows * (s + 1))
            dp_q[s] = (acc_q[core, rows, :] + pair_q_in[rows, :].astype(F32)).astype(BF16)
            dp_o[s] = (acc_o[core, rows, :] + pair_o_in[rows, :].astype(F32)).astype(BF16)
        for d in range(1, n_dp):
            for copy in dp_copies(d):
                copy.start()
        for d in range(1, n_t):
            gm_copy(d).wait_recv()
        for kk in range(2):
            total = gm_in[kk]
            for c in range(1, chips):
                total = total + gm_in[2 * c + kk]
            gm_sum[kk] = total
        for d in range(1, n_dp):
            gd_copy(d).start()
        gm_all[j] = gm_sum[...]
        for d in range(1, n_dp):
            act_copy(d).wait_recv()
        rows_act = act_g[0].astype(F32)
        for s in range(1, n_dp):
            rows_act = rows_act + pltpu.roll(act_g[s].astype(F32), samples * s, 1)

        total_q = dp_q[j].astype(F32)
        total_o = dp_o[j].astype(F32)
        for d in range(1, n_dp):
            for copy in dp_copies(d):
                copy.wait_recv()
        for d in range(1, n_dp):
            src = lax.rem(j + d, n_dp)
            total_q = total_q + dp_q_in[src].astype(F32)
            total_o = total_o + dp_o_in[src].astype(F32)
        gq_out[...] = total_q
        go_out[...] = jnp.transpose(total_o)

        for d in range(1, n_dp):
            gd_copy(d).wait_recv()
        lane = iota((8, 128), 1)
        for k in range(3):
            pieces = []
            for g in range(groups):
                value = jnp.zeros((8, 128), F32)
                for s in range(n_dp):
                    for kk in range(2):
                        at = samples * s + images * kk
                        shift = (at - 12 * g - 4 * k) % 128
                        moved = gm_all[s, kk]
                        if shift:
                            moved = pltpu.roll(moved, shift, 1)
                        value = jnp.where((lane >= at) & (lane < at + images), moved, value)
                pieces.append(value)
            ga_out[k] = lax.dot_general(
                rows_act, jnp.concatenate(pieces, axis=0), (((1,), (1,)), ((), ())),
                precision=lax.Precision.HIGHEST, preferred_element_type=F32,
            )

        mate_noisy.wait_send()
        for copy in w_copies + pair_copies:
            copy.wait_send()
        for d in range(1, n_t):
            mod_copy(d).wait_send()
            gm_copy(d).wait_send()
        for d in range(1, n_dp):
            act_copy(d).wait_send()
            gd_copy(d).wait_send()
            for copy in dp_copies(d):
                copy.wait_send()
        for i in range(images):
            form = gather_z if i % 2 == 0 else gather_x
            sums = sum_z(i) if i % 2 == 0 else sum_x(i)
            for copy in (
                sum(form(noisy_g, i, s_ag, r_ag)[:2], [])
                + sum(form(cot, i, s_c, r_c)[:2], [])
                + sum(sums, [])
            ):
                copy.wait_send()

    vm = pltpu.VMEM
    dma = pltpu.SemaphoreType.DMA
    scratch = [
        vm((2, images, HD, seq), BF16),
        vm((images, chips, block, seq), BF16),
        vm((1001, width), BF16),
        vm((1000, width), BF16),
        vm((32, width), BF16),
        vm((2, 3, HD, width), BF16),
        vm((2, SPLIT, 128), BF16),
        vm((n_t, SPLIT, 128), BF16),
        vm((images, width, 128), F32),
        vm((width, 128), BF16),
        vm((n_dp, dp_rows, 128), BF16),
        vm((2, 2, HW, width), BF16),
        vm((2, 2, HD, width), BF16),
        vm((2, 2 * HW, width), BF16),
        vm((width, 2 * HW), BF16),
        vm((2 * HD, width), BF16),
        vm((2, width, 2 * HD), BF16),
        vm((images, width, seq), BF16),
        vm((images, width, seq), BF16),
        vm((2, width, seq), BF16),
        vm((3, 2 * HD, seq), BF16),
        vm((images, 2, HD, seq), BF16),
        vm((images, width, seq), BF16),
        vm((images, 2, seq, seq), F32),
        vm((images, 2, 3, HP, seq), BF16),
        vm((images, chips, block, seq), BF16),
        vm((images, 2 * n_x, block, seq), BF16),
        vm((images, chips, block, seq), BF16),
        vm((width, seq), BF16),
        vm((2 * HW, seq), BF16),
        vm((2, width, HW), F32),
        vm((2, width, HD), F32),
        vm((width, 128), F32),
        vm((n_t, 8, 128), F32),
        vm((n_t, 8, 128), F32),
        vm((2, 8, 128), F32),
        vm((n_dp, 2, 8, 128), F32),
        vm((width, HW), BF16),
        vm((width, HD), BF16),
        vm((width, HW), BF16),
        vm((width, HD), BF16),
        vm((n_dp, dp_rows, HW), BF16),
        vm((n_dp, dp_rows, HD), BF16),
        vm((n_dp, dp_rows, HW), BF16),
        vm((n_dp, dp_rows, HD), BF16),
        dma((10,)),
        dma((1,)),
        dma((1,)),
        dma((4,)),
        dma((4,)),
        dma((n_t,)),
        dma((n_t,)),
        dma((n_dp,)),
        dma((n_dp,)),
        dma((images, 2 * n_x)),
        dma((images, 2 * n_x)),
        dma((images, 2 * n_x)),
        dma((images, 2 * n_x)),
        dma((images, 2 * n_x)),
        dma((images, 2 * n_x)),
        dma((n_t,)),
        dma((n_t,)),
        dma((2,)),
        dma((2,)),
        dma((n_dp,)),
        dma((n_dp,)),
        dma((n_dp,)),
        dma((n_dp,)),
        dma((n_dp,)),
        dma((n_dp,)),
    ]
    any_spec = pl.BlockSpec(memory_space=pl.ANY)
    smem_spec = pl.BlockSpec(memory_space=pltpu.SMEM)
    vmem_spec = pl.BlockSpec(memory_space=pltpu.VMEM)
    return pl.pallas_call(
        kernel,
        out_shape=(
            jax.ShapeDtypeStruct((dp_rows, HW), F32),
            jax.ShapeDtypeStruct((HD, dp_rows), F32),
            jax.ShapeDtypeStruct((3, dp_rows, HD), F32),
        ),
        in_specs=[smem_spec] * 4 + [any_spec] * 10,
        out_specs=(vmem_spec,) * 3,
        scratch_shapes=scratch,
        compiler_params=pltpu.CompilerParams(
            collective_id=0, has_side_effects=True, vmem_limit_bytes=60 * 1024 * 1024
        ),
        name="step",
    )


def pass_on(*refs):
    half = len(refs) // 2
    for src, dst in zip(refs[:half], refs[half:]):
        dst[...] = src[...]


def local(
    noisy,
    labels,
    tsteps,
    guide_index,
    class_table,
    time_table,
    guide_table,
    guide_weights,
    teacher_qkv,
    teacher_out,
    teacher_ada,
    student_qkv,
    student_out,
    student_ada,
):
    samples, seq_len, _ = noisy.shape
    n_t = lax.axis_size("tensor")
    n_dp = lax.axis_size("dp")
    norm_scale = 1.0 / math.sqrt(samples * n_dp * seq_len)
    step = make_kernel(n_t, n_dp, samples, seq_len, norm_scale)
    grads = step(
        labels, tsteps, guide_index, guide_weights,
        jnp.swapaxes(noisy, 1, 2), class_table, time_table, guide_table,
        teacher_qkv.T, student_qkv.T, teacher_out, student_out,
        jnp.swapaxes(teacher_ada, 1, 2), jnp.swapaxes(student_ada, 1, 2),
    )
    return pl.pallas_call(
        pass_on,
        out_shape=tuple(jax.ShapeDtypeStruct(g.shape, g.dtype) for g in grads),
        name="pass_on",
    )(*grads)


def solution(mesh):
    return jax.shard_map(
        local,
        mesh=mesh,
        in_specs=(
            P("dp", None, "tensor"),
            P("dp"),
            P("dp"),
            P("dp"),
            P(),
            P(),
            P(),
            P(),
            P(None, "tensor"),
            P("tensor", None),
            P(None, None, "tensor"),
            P(None, "tensor"),
            P("tensor", None),
            P(None, None, "tensor"),
        ),
        out_specs=(P("dp", "tensor"), P("tensor", "dp"), P(None, "dp", "tensor")),
        check_vma=False,
    )
```

```python
import math

import jax
import jax.numpy as jnp
from jax import lax
from jax.experimental import pallas as pl
from jax.experimental.pallas import tpu as pltpu
from jax.sharding import PartitionSpec as P

HD = 72
HW = 3 * HD
HP = 80
norm_eps = 1e-06
F32 = jnp.float32
BF16 = jnp.bfloat16
MESH = pl.DeviceIdType.MESH
SPLIT = 40

NOISY = (True, True, True, True)
COT = (True, False, False, True)
FORWARD = {
    (0, 2): (("n_pass", 2), ("n_start", 3)),
    (1, 1): (("n_pass", 3),),
    (2, 2): (("s_pass", 0),),
    (3, 1): (("s_end", 0),),
    (3, 2): (("s_pass", 1),),
    (3, 4): (("c_pass", 0), ("s_end", 1)),
}
BACKWARD = {
    (0, 0): (("s_pass", 2),),
    (0, 1): (("c_pass", 1),),
    (0, 2): (("s_end", 2), ("s_pass", 3)),
    (1, 1): (("c_pass", 2), ("s_end", 3)),
    (1, 2): (("c_pass", 3),),
}


def dot(a, b, ca, cb):
    return lax.dot_general(a, b, (((ca,), (cb,)), ((), ())), preferred_element_type=F32)


def iota(shape, dim):
    return lax.broadcasted_iota(jnp.int32, shape, dim)


def make_kernel(n_t, n_dp, samples, seq, norm_scale):
    chips = n_t // 2
    n_x = chips // 2
    images = samples // 2
    width = HD * n_t
    block = 2 * HD
    dp_rows = width // n_dp
    groups = HD // 8

    def kernel(
        labels, tsteps, guides, strengths,
        noisy, tab_c, tab_t, tab_g, wq_t, wq_s, wo_t, wo_s, ada_t, ada_s,
        gq_out, go_out, ga_out,
        noisy_p, noisy_g, c_tab, t_tab, g_tab, a_tab, mods, mod_g, mod_i, acts, act_g,
        wq_g, wo_g, wq_cat, wq_tr, wo_cat, wo_tr,
        normed, mod_s, mod_t, mixed, mixed_s, proj_s, prob, qkv_s,
        part, rs_in, cot, gp, gqkv, acc_q, acc_o, gmod, gm_send, gm_in, gm_sum, gm_all,
        pair, pair_in, dp_sum, dp_in,
        l_sem, s_n, r_n, s_w, r_w, s_mod, r_mod, s_act, r_act,
        s_ag, r_ag, s_rs, r_rs, s_c, r_c, s_gm, r_gm, s_pair, r_pair,
        s_dq, r_dq, s_gd, r_gd,
    ):
        t = lax.axis_index("tensor")
        j = lax.axis_index("dp")
        chip = t // 2
        core = lax.rem(t, 2)
        x = chip // 2
        z = lax.rem(chip, 2)
        mate = 1 - core
        mate_t = 2 * chip + mate
        chip_z = 2 * x + 1 - z

        loads = [
            pltpu.make_async_copy(tab_c, c_tab, l_sem.at[0]),
            pltpu.make_async_copy(tab_t, t_tab, l_sem.at[1]),
            pltpu.make_async_copy(tab_g, g_tab, l_sem.at[2]),
            pltpu.make_async_copy(ada_t, a_tab.at[0], l_sem.at[3]),
            pltpu.make_async_copy(ada_s, a_tab.at[1], l_sem.at[4]),
            pltpu.make_async_copy(wq_t, wq_g.at[0, core], l_sem.at[5]),
            pltpu.make_async_copy(wq_s, wq_g.at[1, core], l_sem.at[6]),
            pltpu.make_async_copy(wo_t, wo_g.at[0, core], l_sem.at[7]),
            pltpu.make_async_copy(wo_s, wo_g.at[1, core], l_sem.at[8]),
        ]
        own_noisy = pltpu.make_async_copy(
            noisy.at[pl.ds(images * core, images)], noisy_p.at[core], l_sem.at[9]
        )
        own_noisy.start()
        for copy in loads:
            copy.start()

        barrier = pltpu.get_barrier_semaphore()
        for d in range(1, n_t):
            pl.semaphore_signal(
                barrier, inc=1, device_id={"tensor": lax.rem(t + d, n_t)}, device_id_type=MESH
            )
        for d in range(1, n_dp):
            pl.semaphore_signal(
                barrier, inc=1, device_id={"dp": lax.rem(j + d, n_dp)}, device_id_type=MESH
            )
        def to_tensor(src, dst, ss, rs, peer):
            return pltpu.make_async_remote_copy(
                src_ref=src, dst_ref=dst, send_sem=ss, recv_sem=rs,
                device_id={"tensor": peer}, device_id_type=MESH,
            )

        def to_dp(src, dst, ss, rs, peer):
            return pltpu.make_async_remote_copy(
                src_ref=src, dst_ref=dst, send_sem=ss, recv_sem=rs,
                device_id={"dp": peer}, device_id_type=MESH,
            )

        def x_chip(d):
            return 2 * lax.rem(x + d, n_x) + z

        def device_of(c):
            return 2 * c + core

        def gather_z(buf, i, ss, rs):
            own = buf.at[i, chip]
            first = [to_tensor(own, own, ss.at[i, 0], rs.at[i, 0], device_of(chip_z))]
            first += [
                to_tensor(own, own, ss.at[i, d], rs.at[i, d], device_of(x_chip(d)))
                for d in range(1, n_x)
            ]
            other = buf.at[i, chip_z]
            second = [
                to_tensor(other, other, ss.at[i, n_x + d], rs.at[i, n_x + d], device_of(x_chip(d)))
                for d in range(1, n_x)
            ]
            return first, second, first[:1]

        def gather_x(buf, i, ss, rs):
            own = buf.at[i, chip]
            first = [
                to_tensor(own, own, ss.at[i, d], rs.at[i, d], device_of(x_chip(d)))
                for d in range(1, n_x)
            ]
            ahead = len(first)
            first.append(to_tensor(own, own, ss.at[i, n_x], rs.at[i, n_x], device_of(chip_z)))
            second = []
            for d in range(1, n_x):
                other = buf.at[i, 2 * lax.rem(x + n_x - d, n_x) + z]
                second.append(
                    to_tensor(
                        other, other, ss.at[i, n_x + d], rs.at[i, n_x + d], device_of(chip_z)
                    )
                )
            return first, second, first[:ahead]

        def gather_start(buf, i, ss, rs, z_first):
            for copy in (gather_z if z_first else gather_x)(buf, i, ss, rs)[0]:
                copy.start()

        def gather_pass(buf, i, ss, rs, z_first):
            _, second, needed = (gather_z if z_first else gather_x)(buf, i, ss, rs)
            for copy in needed:
                copy.wait_recv()
            for copy in second:
                copy.start()

        def gather_end(buf, i, ss, rs, z_first):
            first, second, needed = (gather_z if z_first else gather_x)(buf, i, ss, rs)
            for copy in first + second:
                if not any(copy is other for other in needed):
                    copy.wait_recv()

        def sum_z(i):
            first = [
                to_tensor(
                    part.at[i, 2 * e + 1 - z], rs_in.at[i, e],
                    s_rs.at[i, e], r_rs.at[i, e], device_of(chip_z),
                )
                for e in range(n_x)
            ]
            second = [
                to_tensor(
                    part.at[i, x_chip(d)], rs_in.at[i, n_x + d],
                    s_rs.at[i, n_x + d], r_rs.at[i, n_x + d], device_of(x_chip(d)),
                )
                for d in range(1, n_x)
            ]
            return first, second

        def sum_start(i):
            for copy in sum_z(i)[0]:
                copy.start()

        def sum_pass(i):
            first, second = sum_z(i)
            for copy in first:
                copy.wait_recv()
            for d in range(1, n_x):
                e = lax.rem(x + d, n_x)
                total = part[i, 2 * e + z].astype(F32) + rs_in[i, e].astype(F32)
                part[i, 2 * e + z] = total.astype(BF16)
            for copy in second:
                copy.start()

        def sum_end(i):
            for copy in sum_z(i)[1]:
                copy.wait_recv()
            total = part[i, chip].astype(F32) + rs_in[i, x].astype(F32)
            for d in range(1, n_x):
                total = total + rs_in[i, n_x + d].astype(F32)
            cot[i, chip] = total.astype(BF16)
            gather_start(cot, i, s_c, r_c, COT[i])

        mate_noisy = to_tensor(
            noisy.at[pl.ds(images * mate, images)], noisy_p.at[core], s_n.at[0], r_n.at[0], mate_t
        )
        w_copies = [
            to_tensor(wq_t, wq_g.at[0, core], s_w.at[0], r_w.at[0], mate_t),
            to_tensor(wq_s, wq_g.at[1, core], s_w.at[1], r_w.at[1], mate_t),
            to_tensor(wo_t, wo_g.at[0, core], s_w.at[2], r_w.at[2], mate_t),
            to_tensor(wo_s, wo_g.at[1, core], s_w.at[3], r_w.at[3], mate_t),
        ]
        def mod_copy(d):
            peer = lax.rem(t + d, n_t)
            return to_tensor(
                mods.at[lax.rem(peer, 2)], mod_g.at[t], s_mod.at[d], r_mod.at[d], peer
            )

        def act_copy(d):
            peer = lax.rem(j + d, n_dp)
            return to_dp(
                acts.at[pl.ds(pl.multiple_of(peer * dp_rows, 16), dp_rows)], act_g.at[j],
                s_act.at[d], r_act.at[d], peer,
            )

        for copy in loads[:5]:
            copy.wait()

        def one_hot(ref, size):
            row = iota((samples, size), 0)
            lane = iota((samples, size), 1)
            hot = jnp.zeros((samples, size), F32)
            for b in range(samples):
                hot = jnp.where((row == b) & (lane == ref[b]), 1.0, hot)
            return hot.astype(BF16)

        def lookup(ref, table, size):
            whole = size // 16 * 16
            hot = one_hot(ref, whole + 16)
            last = table[whole:size, :].astype(F32)
            last = jnp.concatenate([last, jnp.zeros((16 - size + whole, width), F32)], axis=0)
            return dot(hot[:, :whole], table[0:whole, :], 1, 0) + dot(
                hot[:, whole:], last.astype(BF16), 1, 0
            )

        time_embed = lookup(tsteps, t_tab, tab_t.shape[0])
        classes = tab_c.shape[0] - 1
        cond_embed = lookup(labels, c_tab, classes) + time_embed
        null_row = c_tab[classes - 8 :, :].astype(F32)[8:9]
        null_embed = null_row + time_embed
        student_embed = cond_embed + dot(one_hot(guides, tab_g.shape[0]), g_tab[...], 1, 0)

        def silu(v):
            return v / (1.0 + jnp.exp(-v))

        student_act = silu(student_embed)
        teacher_act = jnp.concatenate([silu(cond_embed), silu(null_embed)], axis=0).astype(BF16)
        acts[...] = jnp.zeros_like(acts)
        acts[:, 0:samples] = jnp.transpose(student_act).astype(BF16)
        student_act = jnp.concatenate([student_act, jnp.zeros_like(student_act)], axis=0).astype(BF16)
        lane_t = iota((1, 2 * samples), 1)
        factor = jnp.zeros((1, 2 * samples), F32)
        for b in range(samples):
            strength = strengths[guides[b]]
            factor = jnp.where(lane_t == b, -(1.0 + strength) * norm_scale, factor)
            factor = jnp.where(lane_t == samples + b, strength * norm_scale, factor)
        spread = jnp.zeros((HD, 256), F32)
        for k in range(3):
            value_t = dot(a_tab[0, k], teacher_act, 1, 1)
            value_s = dot(a_tab[1, k], student_act, 1, 1)
            if k == 2:
                value_t = value_t * factor
            for first, value in ((0, value_t), (2, value_s)):
                row = iota((2 * samples, 256), 0)
                lane = iota((2 * samples, 256), 1)
                b = lax.rem(row, samples)
                kind = first + row // samples
                target = 128 * (b // images) + 16 * lax.rem(b, images) + 3 * kind + k
                hot = jnp.where((lane == target) & (kind < 3), 1.0, 0.0).astype(BF16)
                spread = spread + dot(value.astype(BF16), hot, 1, 0)
        for kk in range(2):
            half = spread[:, 128 * kk : 128 * (kk + 1)]
            low = jnp.concatenate(
                [pltpu.roll(half[SPLIT:], 64, 1), jnp.zeros((2 * SPLIT - HD, 128), F32)], axis=0
            )
            mods[kk] = (half[:SPLIT] + low).astype(BF16)

        pl.semaphore_wait(barrier, n_t + n_dp - 2)
        mate_noisy.start()
        for d in range(1, n_t):
            mod_copy(d).start()
        own_noisy.wait()
        mate_noisy.wait_recv()
        for i in range(images):
            both = jnp.concatenate(
                [noisy_p[0, i].astype(F32), noisy_p[1, i].astype(F32)], axis=0
            )
            noisy_g[i, chip] = both.astype(BF16)
            if i == 0:
                gather_start(noisy_g, 0, s_ag, r_ag, NOISY[0])
        for copy in w_copies:
            copy.start()
        mod_g[t] = mods[core]
        act_g[j] = acts[pl.ds(pl.multiple_of(j * dp_rows, 16), dp_rows), :]

        gather_pass(noisy_g, 0, s_ag, r_ag, NOISY[0])
        gather_start(noisy_g, 1, s_ag, r_ag, NOISY[1])
        for d in range(1, n_dp):
            act_copy(d).start()

        for copy in loads[5:]:
            copy.wait()
        for copy in w_copies:
            copy.wait_recv()
        for m in range(2):
            both = jnp.concatenate([wq_g[m, 0].astype(F32), wq_g[m, 1].astype(F32)], axis=0)
            wq_cat[m] = both.astype(BF16)
            if m == 1:
                wq_tr[...] = jnp.transpose(both).astype(BF16)
            both = jnp.concatenate([wo_g[m, 0].astype(F32), wo_g[m, 1].astype(F32)], axis=0)
            if m == 1:
                wo_cat[...] = both.astype(BF16)
            wo_tr[m] = jnp.transpose(both).astype(BF16)
        acc_q[...] = jnp.zeros_like(acc_q)
        acc_o[...] = jnp.zeros_like(acc_o)
        gmod[...] = jnp.zeros_like(gmod)
        gather_pass(noisy_g, 1, s_ag, r_ag, NOISY[1])
        gather_start(noisy_g, 2, s_ag, r_ag, NOISY[2])

        for d in range(1, n_t):
            mod_copy(d).wait_recv()
        for src in range(n_t):
            piece = mod_g[src].astype(F32)
            for b in range(images):
                near = piece if b == 0 else pltpu.roll(piece, 128 - 16 * b, 1)
                far = pltpu.roll(piece, 64 - 16 * b, 1)
                mod_i[b, HD * src : HD * src + SPLIT, :] = near
                mod_i[b, HD * src + SPLIT : HD * (src + 1), :] = far[: HD - SPLIT]

        def padded(value):
            rows = jnp.zeros((HP - HD, seq), F32)
            return jnp.concatenate([value, rows], axis=0).astype(BF16)

        def attend(q, k, v):
            scores = dot(k, q, 0, 0) * (1.0 / math.sqrt(HD))
            exponent = jnp.exp(scores - jnp.max(scores, axis=0, keepdims=True))
            p = exponent * (1.0 / jnp.sum(exponent, axis=0, keepdims=True))
            return p, dot(v, p.astype(BF16), 1, 0)[:HD]

        def forward_in(i):
            for q in range(images):

                @pl.when(i == q)
                def _():
                    gather_end(noisy_g, q, s_ag, r_ag, NOISY[q])

            total = jnp.zeros((1, seq), F32)
            square = jnp.zeros((1, seq), F32)
            for c in range(chips):
                value = noisy_g[i, c].astype(F32)
                total = total + jnp.sum(value, axis=0, keepdims=True)
                square = square + jnp.sum(value * value, axis=0, keepdims=True)
            mean = total * (1.0 / width)
            rstd = lax.rsqrt(square * (1.0 / width) - mean * mean + norm_eps)
            for c in range(chips):
                rows = slice(block * c, block * (c + 1))
                n = ((noisy_g[i, c].astype(F32) - mean) * rstd).astype(BF16)
                normed[i, rows, :] = n
                n = n.astype(F32)
                for a in range(3):
                    shift = mod_i[i, rows, 3 * a : 3 * a + 1]
                    scale = mod_i[i, rows, 3 * a + 1 : 3 * a + 2]
                    value = (n * (1.0 + scale) + shift).astype(BF16)
                    if a == 2:
                        mod_s[i, rows, :] = value
                    else:
                        mod_t[a, rows, :] = value

        def forward_model(i, a):
            act = mod_s[i] if a == 2 else mod_t[a]
            qkv = dot(wq_cat[0 if a < 2 else 1], act, 1, 0)
            heads = []
            for h in range(2):
                q, k, v = (
                    padded(qkv[HW * h + HD * e : HW * h + HD * (e + 1)]) for e in range(3)
                )
                p, mix = attend(q, k, v)
                heads.append(mix)
                if a == 2:
                    prob[i, h] = p
                    mixed_s[i, h] = mix.astype(BF16)
                    for e, value in enumerate((q, k, v)):
                        qkv_s[i, h, e] = value
            mixed[a] = jnp.concatenate(heads, axis=0).astype(BF16)

        def forward_out(i):
            for c in range(chips):
                rows = slice(block * c, block * (c + 1))
                sums = jnp.zeros((block, seq), F32)
                for a in range(3):
                    value = dot(wo_tr[0 if a < 2 else 1, rows, :], mixed[a], 1, 0)
                    gate = mod_i[i, rows, 3 * a + 2 : 3 * a + 3]
                    if a == 2:
                        proj_s[i, rows, :] = value.astype(BF16)
                        gate = gate * norm_scale
                    sums = sums + value * gate
                part[i, c] = sums.astype(BF16)
            sum_start(i)

        def backward_in(i):
            for q in range(images):

                @pl.when(i == q)
                def _():
                    gather_end(cot, q, s_c, r_c, COT[q])

            grads = []
            for c in range(chips):
                rows = slice(block * c, block * (c + 1))
                value = cot[i, c].astype(F32)
                gp[rows, :] = (value * mod_i[i, rows, 8:9]).astype(BF16)
                grads.append(
                    jnp.sum(value * proj_s[i, rows, :].astype(F32), axis=1, keepdims=True)
                )
            grad_gate = jnp.concatenate(grads, axis=0)
            lane = iota((width, 128), 1)
            gmod[...] += jnp.where(lane == 8 + i, grad_gate, 0.0)
            grad_mixed = dot(wo_cat[...], gp[...], 1, 0)
            acts_grad = []
            for h in range(2):
                low = padded(grad_mixed[HD * h : HD * (h + 1)])
                acc_o[h] += dot(gp[...], mixed_s[i, h], 1, 1)
                q, k, v = (qkv_s[i, h, e] for e in range(3))
                p = prob[i, h]
                grad_prob = dot(v, low, 0, 0)
                delta = jnp.sum(p * grad_prob, axis=0, keepdims=True)
                ds = (p * (grad_prob - delta) * (1.0 / math.sqrt(HD))).astype(BF16)
                acts_grad.append(dot(k, ds, 1, 0)[:HD])
                acts_grad.append(dot(q, ds, 1, 1)[:HD])
                acts_grad.append(dot(low, p.astype(BF16), 1, 1)[:HD])
            gqkv[...] = jnp.concatenate(acts_grad, axis=0).astype(BF16)
            for h in range(2):
                head = jnp.concatenate(acts_grad[3 * h : 3 * h + 3], axis=0).astype(BF16)
                acc_q[h] += dot(mod_s[i], head, 1, 1)

        def backward_out(i):
            shifts = []
            scales = []
            for c in range(chips):
                rows = slice(block * c, block * (c + 1))
                value = dot(wq_tr[rows, :], gqkv[...], 1, 0)
                shifts.append(jnp.sum(value, axis=1, keepdims=True))
                scales.append(
                    jnp.sum(value * normed[i, rows, :].astype(F32), axis=1, keepdims=True)
                )
            lane = iota((width, 128), 1)
            gmod[...] += jnp.where(lane == i, jnp.concatenate(shifts, axis=0), 0.0) + jnp.where(
                lane == 4 + i, jnp.concatenate(scales, axis=0), 0.0
            )

        stages = {
            "n_start": lambda q: gather_start(noisy_g, q, s_ag, r_ag, NOISY[q]),
            "n_pass": lambda q: gather_pass(noisy_g, q, s_ag, r_ag, NOISY[q]),
            "s_pass": sum_pass,
            "s_end": sum_end,
            "c_pass": lambda q: gather_pass(cot, q, s_c, r_c, COT[q]),
        }

        def at(i, point, table):
            for (step, where), names in table.items():
                if where == point:

                    @pl.when(i == step)
                    def _():
                        for name, q in names:
                            stages[name](q)

        def forward_step(i, carry):
            forward_in(i)
            at(i, 1, FORWARD)
            forward_model(i, 0)
            at(i, 2, FORWARD)
            forward_model(i, 1)
            at(i, 3, FORWARD)
            forward_model(i, 2)
            at(i, 4, FORWARD)
            forward_out(i)
            return carry

        lax.fori_loop(0, images, forward_step, 0)

        def gm_copy(d):
            peer = lax.rem(t + d, n_t)
            return to_tensor(gm_send.at[peer], gm_in.at[t], s_gm.at[d], r_gm.at[d], peer)

        def pair_copy(s):
            return to_tensor(pair.at[s], pair_in.at[s], s_pair.at[s], r_pair.at[s], mate_t)

        def dp_copy(d):
            peer = lax.rem(j + d, n_dp)
            return to_dp(dp_sum.at[peer], dp_in.at[j], s_dq.at[d], r_dq.at[d], peer)

        def gd_copy(d):
            peer = lax.rem(j + d, n_dp)
            return to_dp(gm_sum, gm_all.at[j], s_gd.at[d], r_gd.at[d], peer)

        def chunk(s):
            return pl.ds(pl.multiple_of(s * dp_rows, 16), dp_rows)

        def backward_step(i, carry):
            at(i, 0, BACKWARD)
            backward_in(i)
            at(i, 1, BACKWARD)

            @pl.when(i == images - 1)
            def _():
                for d in range(1, n_dp + 1):
                    s = lax.rem(j + d, n_dp)
                    pair[s, :, 0:HW] = acc_q[mate, chunk(s), :].astype(BF16)
                    pair[s, :, 256 : 256 + HD] = acc_o[mate, chunk(s), :].astype(BF16)
                    pair_copy(s).start()

            backward_out(i)
            at(i, 2, BACKWARD)
            return carry

        lax.fori_loop(0, images, backward_step, 0)

        for src in range(n_t):
            packed = gmod[HD * src : HD * src + 8, :]
            for g in range(1, groups):
                rows = slice(HD * src + 8 * g, HD * src + 8 * (g + 1))
                packed = packed + pltpu.roll(gmod[rows, :], 12 * g, 1)
            gm_send[src] = packed
        for d in range(1, n_t):
            gm_copy(d).start()
        gm_in[t] = gm_send[t]
        for d in range(1, n_dp + 1):
            s = lax.rem(j + d, n_dp)
            pair_copy(s).wait_recv()
            dp_sum[s, :, 0:HW] = (
                acc_q[core, chunk(s), :] + pair_in[s, :, 0:HW].astype(F32)
            ).astype(BF16)
            dp_sum[s, :, 256 : 256 + HD] = (
                acc_o[core, chunk(s), :] + pair_in[s, :, 256 : 256 + HD].astype(F32)
            ).astype(BF16)
            if d < n_dp:
                dp_copy(d).start()
        for d in range(1, n_t):
            gm_copy(d).wait_recv()
        for kk in range(2):
            total = gm_in[kk]
            for c in range(1, chips):
                total = total + gm_in[2 * c + kk]
            gm_sum[kk] = total
        for d in range(1, n_dp):
            gd_copy(d).start()
        gm_all[j] = gm_sum[...]
        for d in range(1, n_dp):
            act_copy(d).wait_recv()
        rows_act = act_g[0].astype(F32)
        for s in range(1, n_dp):
            rows_act = rows_act + pltpu.roll(act_g[s].astype(F32), samples * s, 1)

        total_q = dp_sum[j, :, 0:HW].astype(F32)
        total_o = dp_sum[j, :, 256 : 256 + HD].astype(F32)
        for d in range(1, n_dp):
            dp_copy(d).wait_recv()
        for d in range(1, n_dp):
            src = lax.rem(j + d, n_dp)
            total_q = total_q + dp_in[src, :, 0:HW].astype(F32)
            total_o = total_o + dp_in[src, :, 256 : 256 + HD].astype(F32)
        gq_out[...] = total_q
        go_out[...] = jnp.transpose(total_o)

        for d in range(1, n_dp):
            gd_copy(d).wait_recv()
        lane = iota((8, 128), 1)
        for k in range(3):
            pieces = []
            for g in range(groups):
                value = jnp.zeros((8, 128), F32)
                for s in range(n_dp):
                    for kk in range(2):
                        at = samples * s + images * kk
                        shift = (at - 12 * g - 4 * k) % 128
                        moved = gm_all[s, kk]
                        if shift:
                            moved = pltpu.roll(moved, shift, 1)
                        value = jnp.where((lane >= at) & (lane < at + images), moved, value)
                pieces.append(value)
            ga_out[k] = lax.dot_general(
                rows_act, jnp.concatenate(pieces, axis=0), (((1,), (1,)), ((), ())),
                precision=lax.Precision.HIGHEST, preferred_element_type=F32,
            )

        mate_noisy.wait_send()
        for copy in w_copies:
            copy.wait_send()
        for s in range(n_dp):
            pair_copy(s).wait_send()
        for d in range(1, n_t):
            mod_copy(d).wait_send()
            gm_copy(d).wait_send()
        for d in range(1, n_dp):
            act_copy(d).wait_send()
            gd_copy(d).wait_send()
            dp_copy(d).wait_send()
        for i in range(images):
            of_noisy = gather_z if NOISY[i] else gather_x
            of_cot = gather_z if COT[i] else gather_x
            for copy in (
                sum(of_noisy(noisy_g, i, s_ag, r_ag)[:2], [])
                + sum(of_cot(cot, i, s_c, r_c)[:2], [])
                + sum(sum_z(i), [])
            ):
                copy.wait_send()

    vm = pltpu.VMEM
    dma = pltpu.SemaphoreType.DMA
    scratch = [
        vm((2, images, HD, seq), BF16),
        vm((images, chips, block, seq), BF16),
        vm((1001, width), BF16),
        vm((1000, width), BF16),
        vm((32, width), BF16),
        vm((2, 3, HD, width), BF16),
        vm((2, SPLIT, 128), BF16),
        vm((n_t, SPLIT, 128), BF16),
        vm((images, width, 128), F32),
        vm((width, 128), BF16),
        vm((n_dp, dp_rows, 128), BF16),
        vm((2, 2, HW, width), BF16),
        vm((2, 2, HD, width), BF16),
        vm((2, 2 * HW, width), BF16),
        vm((width, 2 * HW), BF16),
        vm((2 * HD, width), BF16),
        vm((2, width, 2 * HD), BF16),
        vm((images, width, seq), BF16),
        vm((images, width, seq), BF16),
        vm((2, width, seq), BF16),
        vm((3, 2 * HD, seq), BF16),
        vm((images, 2, HD, seq), BF16),
        vm((images, width, seq), BF16),
        vm((images, 2, seq, seq), F32),
        vm((images, 2, 3, HP, seq), BF16),
        vm((images, chips, block, seq), BF16),
        vm((images, 2 * n_x, block, seq), BF16),
        vm((images, chips, block, seq), BF16),
        vm((width, seq), BF16),
        vm((2 * HW, seq), BF16),
        vm((2, width, HW), F32),
        vm((2, width, HD), F32),
        vm((width, 128), F32),
        vm((n_t, 8, 128), F32),
        vm((n_t, 8, 128), F32),
        vm((2, 8, 128), F32),
        vm((n_dp, 2, 8, 128), F32),
        vm((n_dp, dp_rows, 384), BF16),
        vm((n_dp, dp_rows, 384), BF16),
        vm((n_dp, dp_rows, 384), BF16),
        vm((n_dp, dp_rows, 384), BF16),
        dma((10,)),
        dma((1,)),
        dma((1,)),
        dma((4,)),
        dma((4,)),
        dma((n_t,)),
        dma((n_t,)),
        dma((n_dp,)),
        dma((n_dp,)),
        dma((images, 2 * n_x)),
        dma((images, 2 * n_x)),
        dma((images, 2 * n_x)),
        dma((images, 2 * n_x)),
        dma((images, 2 * n_x)),
        dma((images, 2 * n_x)),
        dma((n_t,)),
        dma((n_t,)),
        dma((n_dp,)),
        dma((n_dp,)),
        dma((n_dp,)),
        dma((n_dp,)),
        dma((n_dp,)),
        dma((n_dp,)),
    ]
    any_spec = pl.BlockSpec(memory_space=pl.ANY)
    smem_spec = pl.BlockSpec(memory_space=pltpu.SMEM)
    vmem_spec = pl.BlockSpec(memory_space=pltpu.VMEM)
    return pl.pallas_call(
        kernel,
        out_shape=(
            jax.ShapeDtypeStruct((dp_rows, HW), F32),
            jax.ShapeDtypeStruct((HD, dp_rows), F32),
            jax.ShapeDtypeStruct((3, dp_rows, HD), F32),
        ),
        in_specs=[smem_spec] * 4 + [any_spec] * 10,
        out_specs=(vmem_spec,) * 3,
        scratch_shapes=scratch,
        compiler_params=pltpu.CompilerParams(
            collective_id=0, has_side_effects=True, vmem_limit_bytes=60 * 1024 * 1024
        ),
        name="step",
    )


def pass_on(*refs):
    half = len(refs) // 2
    for src, dst in zip(refs[:half], refs[half:]):
        dst[...] = src[...]


def local(
    noisy,
    labels,
    tsteps,
    guide_index,
    class_table,
    time_table,
    guide_table,
    guide_weights,
    teacher_qkv,
    teacher_out,
    teacher_ada,
    student_qkv,
    student_out,
    student_ada,
):
    samples, seq_len, _ = noisy.shape
    n_t = lax.axis_size("tensor")
    n_dp = lax.axis_size("dp")
    norm_scale = 1.0 / math.sqrt(samples * n_dp * seq_len)
    step = make_kernel(n_t, n_dp, samples, seq_len, norm_scale)
    grads = step(
        labels, tsteps, guide_index, guide_weights,
        jnp.swapaxes(noisy, 1, 2), class_table, time_table, guide_table,
        teacher_qkv.T, student_qkv.T, teacher_out, student_out,
        jnp.swapaxes(teacher_ada, 1, 2), jnp.swapaxes(student_ada, 1, 2),
    )
    return pl.pallas_call(
        pass_on,
        out_shape=tuple(jax.ShapeDtypeStruct(g.shape, g.dtype) for g in grads),
        name="pass_on",
    )(*grads)


def solution(mesh):
    return jax.shard_map(
        local,
        mesh=mesh,
        in_specs=(
            P("dp", None, "tensor"),
            P("dp"),
            P("dp"),
            P("dp"),
            P(),
            P(),
            P(),
            P(),
            P(None, "tensor"),
            P("tensor", None),
            P(None, None, "tensor"),
            P(None, "tensor"),
            P("tensor", None),
            P(None, None, "tensor"),
        ),
        out_specs=(P("dp", "tensor"), P("tensor", "dp"), P(None, "dp", "tensor")),
        check_vma=False,
    )
```

```python
import math

import jax
import jax.numpy as jnp
from jax import lax
from jax.experimental import pallas as pl
from jax.experimental.pallas import tpu as pltpu
from jax.sharding import PartitionSpec as P

HD = 72
HW = 3 * HD
HP = 80
FREE = 256 - HW
norm_eps = 1e-06
F32 = jnp.float32
BF16 = jnp.bfloat16
MESH = pl.DeviceIdType.MESH
SPLIT = 40

NOISY = (True, True, True, True)
COT = (True, False, False, True)
FORWARD = {
    (0, 1): (("n_pass", 1), ("n_start", 2)),
    (0, 4): (("n_pass", 2), ("n_start", 3)),
    (1, 2): (("n_pass", 3),),
    (2, 2): (("s_pass", 0),),
    (3, 1): (("s_end", 0),),
    (3, 2): (("s_pass", 1),),
    (3, 4): (("c_pass", 0), ("s_end", 1)),
}
BACKWARD = {
    (0, 0): (("s_pass", 2),),
    (0, 1): (("c_pass", 1),),
    (0, 2): (("s_end", 2), ("s_pass", 3)),
    (1, 1): (("c_pass", 2), ("s_end", 3)),
    (1, 2): (("c_pass", 3),),
}


def dot(a, b, ca, cb):
    return lax.dot_general(a, b, (((ca,), (cb,)), ((), ())), preferred_element_type=F32)


def iota(shape, dim):
    return lax.broadcasted_iota(jnp.int32, shape, dim)


def make_kernel(n_t, n_dp, samples, seq, norm_scale):
    chips = n_t // 2
    n_x = chips // 2
    images = samples // 2
    width = HD * n_t
    block = 2 * HD
    dp_rows = width // n_dp
    groups = HD // 8

    def kernel(
        labels, tsteps, guides, strengths,
        noisy, tab_c, tab_t, tab_g, wq_t, wq_s, wo_t, wo_s, ada_t, ada_s,
        gq_out, go_out, ga_out,
        noisy_p, noisy_v, noisy_g, c_tab, t_tab, g_tab, a_tab, mods, mod_g, mod_i, acts, act_g,
        wq_g, wo_g, wq_cat, wq_tr, wo_cat, wo_tr,
        normed, mod_s, mod_t, mixed, mixed_s, proj_s, prob, qkv_s,
        part, rs_in, cot, gp, gqkv, acc_q, acc_o, gmod, gm_send, gm_in, gm_sum, gm_all,
        pair, pair_in, dp_sum, dp_in, dp_ex, dp_ex_in,
        l_sem, s_n, r_n, s_w, r_w, s_mod, r_mod, s_act, r_act,
        s_ag, r_ag, s_rs, r_rs, s_c, r_c, s_gm, r_gm, s_pair, r_pair,
        s_dq, r_dq, s_do, r_do, s_gd, r_gd,
    ):
        t = lax.axis_index("tensor")
        j = lax.axis_index("dp")
        chip = t // 2
        core = lax.rem(t, 2)
        x = chip // 2
        z = lax.rem(chip, 2)
        mate = 1 - core
        mate_t = 2 * chip + mate
        chip_z = 2 * x + 1 - z

        loads = [
            pltpu.make_async_copy(tab_c, c_tab, l_sem.at[0]),
            pltpu.make_async_copy(tab_t, t_tab, l_sem.at[1]),
            pltpu.make_async_copy(tab_g, g_tab, l_sem.at[2]),
            pltpu.make_async_copy(ada_t, a_tab.at[0], l_sem.at[3]),
            pltpu.make_async_copy(ada_s, a_tab.at[1], l_sem.at[4]),
            pltpu.make_async_copy(wq_t, wq_g.at[0, core], l_sem.at[5]),
            pltpu.make_async_copy(wq_s, wq_g.at[1, core], l_sem.at[6]),
            pltpu.make_async_copy(wo_t, wo_g.at[0, core], l_sem.at[7]),
            pltpu.make_async_copy(wo_s, wo_g.at[1, core], l_sem.at[8]),
        ]
        own_noisy = pltpu.make_async_copy(noisy, noisy_v, l_sem.at[9])
        own_noisy.start()
        for copy in loads:
            copy.start()

        barrier = pltpu.get_barrier_semaphore()
        for d in range(1, n_t):
            pl.semaphore_signal(
                barrier, inc=1, device_id={"tensor": lax.rem(t + d, n_t)}, device_id_type=MESH
            )
        for d in range(1, n_dp):
            pl.semaphore_signal(
                barrier, inc=1, device_id={"dp": lax.rem(j + d, n_dp)}, device_id_type=MESH
            )
        def to_tensor(src, dst, ss, rs, peer):
            return pltpu.make_async_remote_copy(
                src_ref=src, dst_ref=dst, send_sem=ss, recv_sem=rs,
                device_id={"tensor": peer}, device_id_type=MESH,
            )

        def to_dp(src, dst, ss, rs, peer):
            return pltpu.make_async_remote_copy(
                src_ref=src, dst_ref=dst, send_sem=ss, recv_sem=rs,
                device_id={"dp": peer}, device_id_type=MESH,
            )

        def x_chip(d):
            return 2 * lax.rem(x + d, n_x) + z

        def device_of(c):
            return 2 * c + core

        def gather_z(buf, i, ss, rs):
            own = buf.at[i, chip]
            first = [to_tensor(own, own, ss.at[i, 0], rs.at[i, 0], device_of(chip_z))]
            first += [
                to_tensor(own, own, ss.at[i, d], rs.at[i, d], device_of(x_chip(d)))
                for d in range(1, n_x)
            ]
            other = buf.at[i, chip_z]
            second = [
                to_tensor(other, other, ss.at[i, n_x + d], rs.at[i, n_x + d], device_of(x_chip(d)))
                for d in range(1, n_x)
            ]
            return first, second, first[:1]

        def gather_x(buf, i, ss, rs):
            own = buf.at[i, chip]
            first = [
                to_tensor(own, own, ss.at[i, d], rs.at[i, d], device_of(x_chip(d)))
                for d in range(1, n_x)
            ]
            ahead = len(first)
            first.append(to_tensor(own, own, ss.at[i, n_x], rs.at[i, n_x], device_of(chip_z)))
            second = []
            for d in range(1, n_x):
                other = buf.at[i, 2 * lax.rem(x + n_x - d, n_x) + z]
                second.append(
                    to_tensor(
                        other, other, ss.at[i, n_x + d], rs.at[i, n_x + d], device_of(chip_z)
                    )
                )
            return first, second, first[:ahead]

        def gather_start(buf, i, ss, rs, z_first):
            for copy in (gather_z if z_first else gather_x)(buf, i, ss, rs)[0]:
                copy.start()

        def gather_pass(buf, i, ss, rs, z_first):
            _, second, needed = (gather_z if z_first else gather_x)(buf, i, ss, rs)
            for copy in needed:
                copy.wait_recv()
            for copy in second:
                copy.start()

        def gather_end(buf, i, ss, rs, z_first):
            first, second, needed = (gather_z if z_first else gather_x)(buf, i, ss, rs)
            for copy in first + second:
                if not any(copy is other for other in needed):
                    copy.wait_recv()

        def sum_z(i):
            first = [
                to_tensor(
                    part.at[i, 2 * e + 1 - z], rs_in.at[i, e],
                    s_rs.at[i, e], r_rs.at[i, e], device_of(chip_z),
                )
                for e in range(n_x)
            ]
            second = [
                to_tensor(
                    part.at[i, x_chip(d)], rs_in.at[i, n_x + d],
                    s_rs.at[i, n_x + d], r_rs.at[i, n_x + d], device_of(x_chip(d)),
                )
                for d in range(1, n_x)
            ]
            return first, second

        def sum_start(i):
            for copy in sum_z(i)[0]:
                copy.start()

        def sum_pass(i):
            first, second = sum_z(i)
            for copy in first:
                copy.wait_recv()
            for d in range(1, n_x):
                e = lax.rem(x + d, n_x)
                total = part[i, 2 * e + z].astype(F32) + rs_in[i, e].astype(F32)
                part[i, 2 * e + z] = total.astype(BF16)
            for copy in second:
                copy.start()

        def sum_end(i):
            for copy in sum_z(i)[1]:
                copy.wait_recv()
            total = part[i, chip].astype(F32) + rs_in[i, x].astype(F32)
            for d in range(1, n_x):
                total = total + rs_in[i, n_x + d].astype(F32)
            cot[i, chip] = total.astype(BF16)
            gather_start(cot, i, s_c, r_c, COT[i])

        mate_noisy = [
            to_tensor(noisy_v.at[images * mate + i], noisy_p.at[i], s_n.at[i], r_n.at[i], mate_t)
            for i in range(images)
        ]
        w_copies = [
            to_tensor(wq_t, wq_g.at[0, core], s_w.at[0], r_w.at[0], mate_t),
            to_tensor(wq_s, wq_g.at[1, core], s_w.at[1], r_w.at[1], mate_t),
            to_tensor(wo_t, wo_g.at[0, core], s_w.at[2], r_w.at[2], mate_t),
            to_tensor(wo_s, wo_g.at[1, core], s_w.at[3], r_w.at[3], mate_t),
        ]
        def mod_copy(d):
            peer = lax.rem(t + d, n_t)
            return to_tensor(
                mods.at[lax.rem(peer, 2)], mod_g.at[t], s_mod.at[d], r_mod.at[d], peer
            )

        def act_copy(d):
            peer = lax.rem(j + d, n_dp)
            return to_dp(
                acts.at[pl.ds(pl.multiple_of(peer * dp_rows, 16), dp_rows)], act_g.at[j],
                s_act.at[d], r_act.at[d], peer,
            )

        for copy in loads[:5]:
            copy.wait()

        def one_hot(ref, size):
            row = iota((samples, size), 0)
            lane = iota((samples, size), 1)
            hot = jnp.zeros((samples, size), F32)
            for b in range(samples):
                hot = jnp.where((row == b) & (lane == ref[b]), 1.0, hot)
            return hot.astype(BF16)

        def lookup(ref, table, size):
            whole = size // 16 * 16
            hot = one_hot(ref, whole + 16)
            last = table[whole:size, :].astype(F32)
            last = jnp.concatenate([last, jnp.zeros((16 - size + whole, width), F32)], axis=0)
            return dot(hot[:, :whole], table[0:whole, :], 1, 0) + dot(
                hot[:, whole:], last.astype(BF16), 1, 0
            )

        time_embed = lookup(tsteps, t_tab, tab_t.shape[0])
        classes = tab_c.shape[0] - 1
        cond_embed = lookup(labels, c_tab, classes) + time_embed
        null_row = c_tab[classes - 8 :, :].astype(F32)[8:9]
        null_embed = null_row + time_embed
        student_embed = cond_embed + dot(one_hot(guides, tab_g.shape[0]), g_tab[...], 1, 0)

        def silu(v):
            return v / (1.0 + jnp.exp(-v))

        student_act = silu(student_embed)
        teacher_act = jnp.concatenate([silu(cond_embed), silu(null_embed)], axis=0).astype(BF16)
        acts[...] = jnp.zeros_like(acts)
        acts[:, 0:samples] = jnp.transpose(student_act).astype(BF16)
        student_act = jnp.concatenate([student_act, jnp.zeros_like(student_act)], axis=0).astype(BF16)
        lane_t = iota((1, 2 * samples), 1)
        factor = jnp.zeros((1, 2 * samples), F32)
        for b in range(samples):
            strength = strengths[guides[b]]
            factor = jnp.where(lane_t == b, -(1.0 + strength) * norm_scale, factor)
            factor = jnp.where(lane_t == samples + b, strength * norm_scale, factor)
        spread = jnp.zeros((HD, 256), F32)
        for k in range(3):
            value_t = dot(a_tab[0, k], teacher_act, 1, 1)
            value_s = dot(a_tab[1, k], student_act, 1, 1)
            if k == 2:
                value_t = value_t * factor
            for first, value in ((0, value_t), (2, value_s)):
                row = iota((2 * samples, 256), 0)
                lane = iota((2 * samples, 256), 1)
                b = lax.rem(row, samples)
                kind = first + row // samples
                target = 128 * (b // images) + 16 * lax.rem(b, images) + 3 * kind + k
                hot = jnp.where((lane == target) & (kind < 3), 1.0, 0.0).astype(BF16)
                spread = spread + dot(value.astype(BF16), hot, 1, 0)
        for kk in range(2):
            half = spread[:, 128 * kk : 128 * (kk + 1)]
            low = jnp.concatenate(
                [pltpu.roll(half[SPLIT:], 64, 1), jnp.zeros((2 * SPLIT - HD, 128), F32)], axis=0
            )
            mods[kk] = (half[:SPLIT] + low).astype(BF16)

        pl.semaphore_wait(barrier, n_t + n_dp - 2)
        own_noisy.wait()
        for copy in mate_noisy:
            copy.start()
        for d in range(1, n_t):
            mod_copy(d).start()
        for i in range(images):
            mate_noisy[i].wait_recv()
            own = noisy_v[images * core + i].astype(F32)
            other = noisy_p[i].astype(F32)
            first = jnp.where(core == 0, own, other)
            second = jnp.where(core == 0, other, own)
            noisy_g[i, chip] = jnp.concatenate([first, second], axis=0).astype(BF16)
            if i == 0:
                gather_start(noisy_g, 0, s_ag, r_ag, NOISY[0])
        for copy in w_copies:
            copy.start()
        mod_g[t] = mods[core]
        act_g[j] = acts[pl.ds(pl.multiple_of(j * dp_rows, 16), dp_rows), :]

        gather_pass(noisy_g, 0, s_ag, r_ag, NOISY[0])
        gather_start(noisy_g, 1, s_ag, r_ag, NOISY[1])
        for d in range(1, n_dp):
            act_copy(d).start()

        for copy in loads[5:]:
            copy.wait()
        for copy in w_copies:
            copy.wait_recv()
        for m in range(2):
            both = jnp.concatenate([wq_g[m, 0].astype(F32), wq_g[m, 1].astype(F32)], axis=0)
            wq_cat[m] = both.astype(BF16)
            if m == 1:
                wq_tr[...] = jnp.transpose(both).astype(BF16)
            both = jnp.concatenate([wo_g[m, 0].astype(F32), wo_g[m, 1].astype(F32)], axis=0)
            if m == 1:
                wo_cat[...] = both.astype(BF16)
            wo_tr[m] = jnp.transpose(both).astype(BF16)
        acc_q[...] = jnp.zeros_like(acc_q)
        acc_o[...] = jnp.zeros_like(acc_o)
        gmod[...] = jnp.zeros_like(gmod)

        for d in range(1, n_t):
            mod_copy(d).wait_recv()
        for src in range(n_t):
            piece = mod_g[src].astype(F32)
            for b in range(images):
                near = piece if b == 0 else pltpu.roll(piece, 128 - 16 * b, 1)
                far = pltpu.roll(piece, 64 - 16 * b, 1)
                mod_i[b, HD * src : HD * src + SPLIT, :] = near
                mod_i[b, HD * src + SPLIT : HD * (src + 1), :] = far[: HD - SPLIT]

        def padded(value):
            rows = jnp.zeros((HP - HD, seq), F32)
            return jnp.concatenate([value, rows], axis=0).astype(BF16)

        def attend(q, k, v):
            scores = dot(k, q, 0, 0) * (1.0 / math.sqrt(HD))
            exponent = jnp.exp(scores - jnp.max(scores, axis=0, keepdims=True))
            p = exponent * (1.0 / jnp.sum(exponent, axis=0, keepdims=True))
            return p, dot(v, p.astype(BF16), 1, 0)[:HD]

        def forward_in(i):
            for q in range(images):

                @pl.when(i == q)
                def _():
                    gather_end(noisy_g, q, s_ag, r_ag, NOISY[q])

            total = jnp.zeros((1, seq), F32)
            square = jnp.zeros((1, seq), F32)
            for c in range(chips):
                value = noisy_g[i, c].astype(F32)
                total = total + jnp.sum(value, axis=0, keepdims=True)
                square = square + jnp.sum(value * value, axis=0, keepdims=True)
            mean = total * (1.0 / width)
            rstd = lax.rsqrt(square * (1.0 / width) - mean * mean + norm_eps)
            for c in range(chips):
                rows = slice(block * c, block * (c + 1))
                n = ((noisy_g[i, c].astype(F32) - mean) * rstd).astype(BF16)
                normed[i, rows, :] = n
                n = n.astype(F32)
                for a in range(3):
                    shift = mod_i[i, rows, 3 * a : 3 * a + 1]
                    scale = mod_i[i, rows, 3 * a + 1 : 3 * a + 2]
                    value = (n * (1.0 + scale) + shift).astype(BF16)
                    if a == 2:
                        mod_s[i, rows, :] = value
                    else:
                        mod_t[a, rows, :] = value

        def forward_model(i, a):
            act = mod_s[i] if a == 2 else mod_t[a]
            qkv = dot(wq_cat[0 if a < 2 else 1], act, 1, 0)
            heads = []
            for h in range(2):
                q, k, v = (
                    padded(qkv[HW * h + HD * e : HW * h + HD * (e + 1)]) for e in range(3)
                )
                p, mix = attend(q, k, v)
                heads.append(mix)
                if a == 2:
                    prob[i, h] = p
                    mixed_s[i, h] = mix.astype(BF16)
                    for e, value in enumerate((q, k, v)):
                        qkv_s[i, h, e] = value
            mixed[a] = jnp.concatenate(heads, axis=0).astype(BF16)

        def forward_out(i):
            for c in range(chips):
                rows = slice(block * c, block * (c + 1))
                sums = jnp.zeros((block, seq), F32)
                for a in range(3):
                    value = dot(wo_tr[0 if a < 2 else 1, rows, :], mixed[a], 1, 0)
                    gate = mod_i[i, rows, 3 * a + 2 : 3 * a + 3]
                    if a == 2:
                        proj_s[i, rows, :] = value.astype(BF16)
                        gate = gate * norm_scale
                    sums = sums + value * gate
                part[i, c] = sums.astype(BF16)
            sum_start(i)

        def backward_in(i):
            for q in range(images):

                @pl.when(i == q)
                def _():
                    gather_end(cot, q, s_c, r_c, COT[q])

            grads = []
            for c in range(chips):
                rows = slice(block * c, block * (c + 1))
                value = cot[i, c].astype(F32)
                gp[rows, :] = (value * mod_i[i, rows, 8:9]).astype(BF16)
                grads.append(
                    jnp.sum(value * proj_s[i, rows, :].astype(F32), axis=1, keepdims=True)
                )
            grad_gate = jnp.concatenate(grads, axis=0)
            lane = iota((width, 128), 1)
            gmod[...] += jnp.where(lane == 8 + i, grad_gate, 0.0)
            grad_mixed = dot(wo_cat[...], gp[...], 1, 0)
            acts_grad = []
            for h in range(2):
                low = padded(grad_mixed[HD * h : HD * (h + 1)])
                acc_o[h, :, 0:HD] += dot(gp[...], mixed_s[i, h], 1, 1)
                q, k, v = (qkv_s[i, h, e] for e in range(3))
                p = prob[i, h]
                grad_prob = dot(v, low, 0, 0)
                delta = jnp.sum(p * grad_prob, axis=0, keepdims=True)
                ds = (p * (grad_prob - delta) * (1.0 / math.sqrt(HD))).astype(BF16)
                acts_grad.append(dot(k, ds, 1, 0)[:HD])
                acts_grad.append(dot(q, ds, 1, 1)[:HD])
                acts_grad.append(dot(low, p.astype(BF16), 1, 1)[:HD])
            gqkv[...] = jnp.concatenate(acts_grad, axis=0).astype(BF16)
            for h in range(2):
                head = jnp.concatenate(acts_grad[3 * h : 3 * h + 3], axis=0).astype(BF16)
                acc_q[h, :, 0:HW] += dot(mod_s[i], head, 1, 1)

        def backward_out(i):
            shifts = []
            scales = []
            for c in range(chips):
                rows = slice(block * c, block * (c + 1))
                value = dot(wq_tr[rows, :], gqkv[...], 1, 0)
                shifts.append(jnp.sum(value, axis=1, keepdims=True))
                scales.append(
                    jnp.sum(value * normed[i, rows, :].astype(F32), axis=1, keepdims=True)
                )
            lane = iota((width, 128), 1)
            gmod[...] += jnp.where(lane == i, jnp.concatenate(shifts, axis=0), 0.0) + jnp.where(
                lane == 4 + i, jnp.concatenate(scales, axis=0), 0.0
            )

        stages = {
            "n_start": lambda q: gather_start(noisy_g, q, s_ag, r_ag, NOISY[q]),
            "n_pass": lambda q: gather_pass(noisy_g, q, s_ag, r_ag, NOISY[q]),
            "s_pass": sum_pass,
            "s_end": sum_end,
            "c_pass": lambda q: gather_pass(cot, q, s_c, r_c, COT[q]),
        }

        def at(i, point, table):
            for (step, where), names in table.items():
                if where == point:

                    @pl.when(i == step)
                    def _():
                        for name, q in names:
                            stages[name](q)

        def forward_step(i, carry):
            forward_in(i)
            at(i, 1, FORWARD)
            forward_model(i, 0)
            at(i, 2, FORWARD)
            forward_model(i, 1)
            at(i, 3, FORWARD)
            forward_model(i, 2)
            at(i, 4, FORWARD)
            forward_out(i)
            return carry

        lax.fori_loop(0, images, forward_step, 0)

        def gm_copy(d):
            peer = lax.rem(t + d, n_t)
            return to_tensor(gm_send.at[peer], gm_in.at[t], s_gm.at[d], r_gm.at[d], peer)

        def pair_copy(s):
            return to_tensor(pair.at[s], pair_in.at[s], s_pair.at[s], r_pair.at[s], mate_t)

        def dp_copies(d):
            peer = lax.rem(j + d, n_dp)
            return [
                to_dp(dp_sum.at[peer], dp_in.at[j], s_dq.at[d], r_dq.at[d], peer),
                to_dp(dp_ex.at[peer], dp_ex_in.at[j], s_do.at[d], r_do.at[d], peer),
            ]

        third = dp_rows // 3
        early = [d for d in (1, 3, 4, 5) if d < n_dp]

        def gd_copy(d):
            peer = lax.rem(j + d, n_dp)
            return to_dp(gm_sum, gm_all.at[j], s_gd.at[d], r_gd.at[d], peer)

        def chunk(s):
            return pl.ds(pl.multiple_of(s * dp_rows, 16), dp_rows)

        def backward_step(i, carry):
            at(i, 0, BACKWARD)
            backward_in(i)
            at(i, 1, BACKWARD)

            @pl.when(i == images - 1)
            def _():
                for d in range(1, n_dp + 1):
                    s = lax.rem(j + d, n_dp)
                    pair[s, :, 0:256] = acc_q[mate, chunk(s), :].astype(BF16)
                    pair[s, :, 256:384] = acc_o[mate, chunk(s), :].astype(BF16)
                    pair_copy(s).start()

            backward_out(i)
            at(i, 2, BACKWARD)
            return carry

        lax.fori_loop(0, images, backward_step, 0)

        for src in range(n_t):
            packed = gmod[HD * src : HD * src + 8, :]
            for g in range(1, groups):
                rows = slice(HD * src + 8 * g, HD * src + 8 * (g + 1))
                packed = packed + pltpu.roll(gmod[rows, :], 12 * g, 1)
            gm_send[src] = packed
        for d in range(1, n_t):
            gm_copy(d).start()
        gm_in[t] = gm_send[t]
        for d in range(1, n_dp + 1):
            s = lax.rem(j + d, n_dp)
            pair_copy(s).wait_recv()
            sums_q = acc_q[core, chunk(s), :] + pair_in[s, :, 0:256].astype(F32)
            sums_o = acc_o[core, chunk(s), :] + pair_in[s, :, 256:384].astype(F32)
            moved = pltpu.roll(sums_o, 128 - FREE, 1)
            lane = iota((dp_rows, 128), 1)
            dp_sum[s, :, 0:128] = sums_q[:, :128].astype(BF16)
            dp_sum[s, :, 128:256] = (
                sums_q[:, 128:] + jnp.where(lane >= 128 - FREE, moved, 0.0)
            ).astype(BF16)
            rest = jnp.where(lane < HD - FREE, moved, 0.0)
            dp_ex[s] = (
                rest[:third]
                + pltpu.roll(rest[third : 2 * third], 32, 1)
                + pltpu.roll(rest[2 * third :], 64, 1)
            ).astype(BF16)
            if d in early:
                for copy in dp_copies(d):
                    copy.start()
        for d in range(1, n_t):
            gm_copy(d).wait_recv()
        for kk in range(2):
            total = gm_in[kk]
            for c in range(1, chips):
                total = total + gm_in[2 * c + kk]
            gm_sum[kk] = total
        for d in range(1, n_dp):
            gd_copy(d).start()
        for d in range(1, n_dp):
            if d not in early:
                for copy in dp_copies(d):
                    copy.start()
        gm_all[j] = gm_sum[...]
        for d in range(1, n_dp):
            act_copy(d).wait_recv()
        rows_act = act_g[0].astype(F32)
        for s in range(1, n_dp):
            rows_act = rows_act + pltpu.roll(act_g[s].astype(F32), samples * s, 1)

        total = dp_sum[j].astype(F32)
        rest = dp_ex[j].astype(F32)
        for d in range(1, n_dp):
            for copy in dp_copies(d):
                copy.wait_recv()
        for d in range(1, n_dp):
            src = lax.rem(j + d, n_dp)
            total = total + dp_in[src].astype(F32)
            rest = rest + dp_ex_in[src].astype(F32)
        gq_out[...] = total[:, :HW]
        lane = iota((dp_rows, 128), 1)
        spread = jnp.concatenate(
            [rest, pltpu.roll(rest, 128 - 32, 1), pltpu.roll(rest, 128 - 64, 1)], axis=0
        )
        total_o = jnp.where(lane >= 128 - FREE, total[:, 128:], 0.0) + jnp.where(
            lane < HD - FREE, spread, 0.0
        )
        go_out[...] = jnp.transpose(pltpu.roll(total_o, FREE, 1))[:HD]

        for d in range(1, n_dp):
            gd_copy(d).wait_recv()
        lane = iota((8, 128), 1)
        for k in range(3):
            pieces = []
            for g in range(groups):
                value = jnp.zeros((8, 128), F32)
                for s in range(n_dp):
                    for kk in range(2):
                        at = samples * s + images * kk
                        shift = (at - 12 * g - 4 * k) % 128
                        moved = gm_all[s, kk]
                        if shift:
                            moved = pltpu.roll(moved, shift, 1)
                        value = jnp.where((lane >= at) & (lane < at + images), moved, value)
                pieces.append(value)
            ga_out[k] = lax.dot_general(
                rows_act, jnp.concatenate(pieces, axis=0), (((1,), (1,)), ((), ())),
                precision=lax.Precision.HIGHEST, preferred_element_type=F32,
            )

        for copy in mate_noisy + w_copies:
            copy.wait_send()
        for s in range(n_dp):
            pair_copy(s).wait_send()
        for d in range(1, n_t):
            mod_copy(d).wait_send()
            gm_copy(d).wait_send()
        for d in range(1, n_dp):
            act_copy(d).wait_send()
            gd_copy(d).wait_send()
            for copy in dp_copies(d):
                copy.wait_send()
        for i in range(images):
            of_noisy = gather_z if NOISY[i] else gather_x
            of_cot = gather_z if COT[i] else gather_x
            for copy in (
                sum(of_noisy(noisy_g, i, s_ag, r_ag)[:2], [])
                + sum(of_cot(cot, i, s_c, r_c)[:2], [])
                + sum(sum_z(i), [])
            ):
                copy.wait_send()

    vm = pltpu.VMEM
    dma = pltpu.SemaphoreType.DMA
    scratch = [
        vm((images, HD, seq), BF16),
        vm((samples, HD, seq), BF16),
        vm((images, chips, block, seq), BF16),
        vm((1001, width), BF16),
        vm((1000, width), BF16),
        vm((32, width), BF16),
        vm((2, 3, HD, width), BF16),
        vm((2, SPLIT, 128), BF16),
        vm((n_t, SPLIT, 128), BF16),
        vm((images, width, 128), F32),
        vm((width, 128), BF16),
        vm((n_dp, dp_rows, 128), BF16),
        vm((2, 2, HW, width), BF16),
        vm((2, 2, HD, width), BF16),
        vm((2, 2 * HW, width), BF16),
        vm((width, 2 * HW), BF16),
        vm((2 * HD, width), BF16),
        vm((2, width, 2 * HD), BF16),
        vm((images, width, seq), BF16),
        vm((images, width, seq), BF16),
        vm((2, width, seq), BF16),
        vm((3, 2 * HD, seq), BF16),
        vm((images, 2, HD, seq), BF16),
        vm((images, width, seq), BF16),
        vm((images, 2, seq, seq), F32),
        vm((images, 2, 3, HP, seq), BF16),
        vm((images, chips, block, seq), BF16),
        vm((images, 2 * n_x, block, seq), BF16),
        vm((images, chips, block, seq), BF16),
        vm((width, seq), BF16),
        vm((2 * HW, seq), BF16),
        vm((2, width, 256), F32),
        vm((2, width, 128), F32),
        vm((width, 128), F32),
        vm((n_t, 8, 128), F32),
        vm((n_t, 8, 128), F32),
        vm((2, 8, 128), F32),
        vm((n_dp, 2, 8, 128), F32),
        vm((n_dp, dp_rows, 384), BF16),
        vm((n_dp, dp_rows, 384), BF16),
        vm((n_dp, dp_rows, 256), BF16),
        vm((n_dp, dp_rows, 256), BF16),
        vm((n_dp, dp_rows // 3, 128), BF16),
        vm((n_dp, dp_rows // 3, 128), BF16),
        dma((10,)),
        dma((images,)),
        dma((images,)),
        dma((4,)),
        dma((4,)),
        dma((n_t,)),
        dma((n_t,)),
        dma((n_dp,)),
        dma((n_dp,)),
        dma((images, 2 * n_x)),
        dma((images, 2 * n_x)),
        dma((images, 2 * n_x)),
        dma((images, 2 * n_x)),
        dma((images, 2 * n_x)),
        dma((images, 2 * n_x)),
        dma((n_t,)),
        dma((n_t,)),
        dma((n_dp,)),
        dma((n_dp,)),
        dma((n_dp,)),
        dma((n_dp,)),
        dma((n_dp,)),
        dma((n_dp,)),
        dma((n_dp,)),
        dma((n_dp,)),
    ]
    any_spec = pl.BlockSpec(memory_space=pl.ANY)
    smem_spec = pl.BlockSpec(memory_space=pltpu.SMEM)
    vmem_spec = pl.BlockSpec(memory_space=pltpu.VMEM)
    return pl.pallas_call(
        kernel,
        out_shape=(
            jax.ShapeDtypeStruct((dp_rows, HW), F32),
            jax.ShapeDtypeStruct((HD, dp_rows), F32),
            jax.ShapeDtypeStruct((3, dp_rows, HD), F32),
        ),
        in_specs=[smem_spec] * 4 + [any_spec] * 10,
        out_specs=(vmem_spec,) * 3,
        scratch_shapes=scratch,
        compiler_params=pltpu.CompilerParams(
            collective_id=0, has_side_effects=True, vmem_limit_bytes=60 * 1024 * 1024
        ),
        name="step",
    )


def pass_on(*refs):
    half = len(refs) // 2
    for src, dst in zip(refs[:half], refs[half:]):
        dst[...] = src[...]


def local(
    noisy,
    labels,
    tsteps,
    guide_index,
    class_table,
    time_table,
    guide_table,
    guide_weights,
    teacher_qkv,
    teacher_out,
    teacher_ada,
    student_qkv,
    student_out,
    student_ada,
):
    samples, seq_len, _ = noisy.shape
    n_t = lax.axis_size("tensor")
    n_dp = lax.axis_size("dp")
    norm_scale = 1.0 / math.sqrt(samples * n_dp * seq_len)
    step = make_kernel(n_t, n_dp, samples, seq_len, norm_scale)
    grads = step(
        labels, tsteps, guide_index, guide_weights,
        jnp.swapaxes(noisy, 1, 2), class_table, time_table, guide_table,
        teacher_qkv.T, student_qkv.T, teacher_out, student_out,
        jnp.swapaxes(teacher_ada, 1, 2), jnp.swapaxes(student_ada, 1, 2),
    )
    return pl.pallas_call(
        pass_on,
        out_shape=tuple(jax.ShapeDtypeStruct(g.shape, g.dtype) for g in grads),
        name="pass_on",
    )(*grads)


def solution(mesh):
    return jax.shard_map(
        local,
        mesh=mesh,
        in_specs=(
            P("dp", None, "tensor"),
            P("dp"),
            P("dp"),
            P("dp"),
            P(),
            P(),
            P(),
            P(),
            P(None, "tensor"),
            P("tensor", None),
            P(None, None, "tensor"),
            P(None, "tensor"),
            P("tensor", None),
            P(None, None, "tensor"),
        ),
        out_specs=(P("dp", "tensor"), P("tensor", "dp"), P(None, "dp", "tensor")),
        check_vma=False,
    )
```

```python
import math

import jax
import jax.numpy as jnp
from jax import lax
from jax.experimental import pallas as pl
from jax.experimental.pallas import tpu as pltpu
from jax.sharding import PartitionSpec as P

HD = 72
HW = 3 * HD
HP = 80
FREE = 256 - HW
norm_eps = 1e-06
F32 = jnp.float32
BF16 = jnp.bfloat16
MESH = pl.DeviceIdType.MESH
SPLIT = 40

NOISY = (True, True, True, True)
COT = (True, False, False, True)
FORWARD = {
    (0, 1): (("n_pass", 1), ("n_start", 2)),
    (0, 4): (("n_pass", 2), ("n_start", 3)),
    (1, 2): (("n_pass", 3),),
    (2, 2): (("s_pass", 0),),
    (3, 1): (("s_end", 0),),
    (3, 2): (("s_pass", 1),),
    (3, 4): (("c_pass", 0), ("s_end", 1)),
}
BACKWARD = {
    (0, 0): (("s_pass", 2),),
    (0, 1): (("c_pass", 1),),
    (0, 2): (("s_end", 2), ("s_pass", 3)),
    (1, 1): (("c_pass", 2), ("s_end", 3)),
    (1, 2): (("c_pass", 3),),
}


def dot(a, b, ca, cb):
    return lax.dot_general(a, b, (((ca,), (cb,)), ((), ())), preferred_element_type=F32)


def iota(shape, dim):
    return lax.broadcasted_iota(jnp.int32, shape, dim)


def make_kernel(n_t, n_dp, samples, seq, norm_scale):
    chips = n_t // 2
    n_x = chips // 2
    images = samples // 2
    width = HD * n_t
    block = 2 * HD
    dp_rows = width // n_dp
    groups = HD // 8

    def kernel(
        labels, tsteps, guides, strengths,
        noisy, tab_c, tab_t, tab_g, wq_t, wq_s, wo_t, wo_s, ada_t, ada_s,
        gq_out, go_out, ga_out,
        noisy_p, noisy_v, noisy_g, c_tab, t_tab, g_tab, a_tab, mods, mod_g, mod_i, acts, act_g,
        wq_g, wo_g, wq_cat, wq_tr, wo_cat, wo_tr,
        normed, mod_s, mod_t, mixed, mixed_s, proj_s, prob, qkv_s,
        part, rs_in, cot, gp, gqkv, acc_q, acc_o, gmod, gm_send, gm_in, gm_sum, gm_all,
        pair, pair_in, dp_sum, dp_in, dp_ex, dp_ex_in,
        l_sem, s_n, r_n, s_w, r_w, s_mod, r_mod, s_act, r_act,
        s_ag, r_ag, s_rs, r_rs, s_c, r_c, s_gm, r_gm, s_pair, r_pair,
        s_dq, r_dq, s_do, r_do, s_gd, r_gd,
    ):
        t = lax.axis_index("tensor")
        j = lax.axis_index("dp")
        chip = t // 2
        core = lax.rem(t, 2)
        x = chip // 2
        z = lax.rem(chip, 2)
        mate = 1 - core
        mate_t = 2 * chip + mate
        chip_z = 2 * x + 1 - z

        loads = [
            pltpu.make_async_copy(tab_c, c_tab, l_sem.at[0]),
            pltpu.make_async_copy(tab_t, t_tab, l_sem.at[1]),
            pltpu.make_async_copy(tab_g, g_tab, l_sem.at[2]),
            pltpu.make_async_copy(ada_t, a_tab.at[0], l_sem.at[3]),
            pltpu.make_async_copy(ada_s, a_tab.at[1], l_sem.at[4]),
            pltpu.make_async_copy(wq_t, wq_g.at[0, core], l_sem.at[5]),
            pltpu.make_async_copy(wq_s, wq_g.at[1, core], l_sem.at[6]),
            pltpu.make_async_copy(wo_t, wo_g.at[0, core], l_sem.at[7]),
            pltpu.make_async_copy(wo_s, wo_g.at[1, core], l_sem.at[8]),
        ]
        own_noisy = pltpu.make_async_copy(noisy, noisy_v, l_sem.at[9])
        own_noisy.start()
        for copy in loads:
            copy.start()

        barrier = pltpu.get_barrier_semaphore()
        for d in range(1, n_t):
            pl.semaphore_signal(
                barrier, inc=1, device_id={"tensor": lax.rem(t + d, n_t)}, device_id_type=MESH
            )
        for d in range(1, n_dp):
            pl.semaphore_signal(
                barrier, inc=1, device_id={"dp": lax.rem(j + d, n_dp)}, device_id_type=MESH
            )
        def to_tensor(src, dst, ss, rs, peer):
            return pltpu.make_async_remote_copy(
                src_ref=src, dst_ref=dst, send_sem=ss, recv_sem=rs,
                device_id={"tensor": peer}, device_id_type=MESH,
            )

        def to_dp(src, dst, ss, rs, peer):
            return pltpu.make_async_remote_copy(
                src_ref=src, dst_ref=dst, send_sem=ss, recv_sem=rs,
                device_id={"dp": peer}, device_id_type=MESH,
            )

        def x_chip(d):
            return 2 * lax.rem(x + d, n_x) + z

        def device_of(c):
            return 2 * c + core

        def gather_z(buf, i, ss, rs):
            own = buf.at[i, chip]
            first = [to_tensor(own, own, ss.at[i, 0], rs.at[i, 0], device_of(chip_z))]
            first += [
                to_tensor(own, own, ss.at[i, d], rs.at[i, d], device_of(x_chip(d)))
                for d in range(1, n_x)
            ]
            other = buf.at[i, chip_z]
            second = [
                to_tensor(other, other, ss.at[i, n_x + d], rs.at[i, n_x + d], device_of(x_chip(d)))
                for d in range(1, n_x)
            ]
            return first, second, first[:1]

        def gather_x(buf, i, ss, rs):
            own = buf.at[i, chip]
            first = [
                to_tensor(own, own, ss.at[i, d], rs.at[i, d], device_of(x_chip(d)))
                for d in range(1, n_x)
            ]
            ahead = len(first)
            first.append(to_tensor(own, own, ss.at[i, n_x], rs.at[i, n_x], device_of(chip_z)))
            second = []
            for d in range(1, n_x):
                other = buf.at[i, 2 * lax.rem(x + n_x - d, n_x) + z]
                second.append(
                    to_tensor(
                        other, other, ss.at[i, n_x + d], rs.at[i, n_x + d], device_of(chip_z)
                    )
                )
            return first, second, first[:ahead]

        def gather_start(buf, i, ss, rs, z_first):
            for copy in (gather_z if z_first else gather_x)(buf, i, ss, rs)[0]:
                copy.start()

        def gather_pass(buf, i, ss, rs, z_first):
            _, second, needed = (gather_z if z_first else gather_x)(buf, i, ss, rs)
            for copy in needed:
                copy.wait_recv()
            for copy in second:
                copy.start()

        def gather_end(buf, i, ss, rs, z_first):
            first, second, needed = (gather_z if z_first else gather_x)(buf, i, ss, rs)
            for copy in first + second:
                if not any(copy is other for other in needed):
                    copy.wait_recv()

        def sum_z(i):
            first = [
                to_tensor(
                    part.at[i, 2 * e + 1 - z], rs_in.at[i, e],
                    s_rs.at[i, e], r_rs.at[i, e], device_of(chip_z),
                )
                for e in range(n_x)
            ]
            second = [
                to_tensor(
                    part.at[i, x_chip(d)], rs_in.at[i, n_x + d],
                    s_rs.at[i, n_x + d], r_rs.at[i, n_x + d], device_of(x_chip(d)),
                )
                for d in range(1, n_x)
            ]
            return first, second

        def sum_start(i):
            for copy in sum_z(i)[0]:
                copy.start()

        def sum_pass(i):
            first, second = sum_z(i)
            for copy in first:
                copy.wait_recv()
            for d in range(1, n_x):
                e = lax.rem(x + d, n_x)
                total = part[i, 2 * e + z].astype(F32) + rs_in[i, e].astype(F32)
                part[i, 2 * e + z] = total.astype(BF16)
            for copy in second:
                copy.start()

        def sum_end(i):
            for copy in sum_z(i)[1]:
                copy.wait_recv()
            total = part[i, chip].astype(F32) + rs_in[i, x].astype(F32)
            for d in range(1, n_x):
                total = total + rs_in[i, n_x + d].astype(F32)
            cot[i, chip] = total.astype(BF16)
            gather_start(cot, i, s_c, r_c, COT[i])

        mate_noisy = [
            to_tensor(noisy_v.at[images * mate + i], noisy_p.at[i], s_n.at[i], r_n.at[i], mate_t)
            for i in range(images)
        ]
        w_copies = [
            to_tensor(wq_t, wq_g.at[0, core], s_w.at[0], r_w.at[0], mate_t),
            to_tensor(wq_s, wq_g.at[1, core], s_w.at[1], r_w.at[1], mate_t),
            to_tensor(wo_t, wo_g.at[0, core], s_w.at[2], r_w.at[2], mate_t),
            to_tensor(wo_s, wo_g.at[1, core], s_w.at[3], r_w.at[3], mate_t),
        ]
        def mod_copy(d):
            peer = lax.rem(t + d, n_t)
            return to_tensor(
                mods.at[lax.rem(peer, 2)], mod_g.at[t], s_mod.at[d], r_mod.at[d], peer
            )

        def act_copy(d):
            peer = lax.rem(j + d, n_dp)
            return to_dp(
                acts.at[pl.ds(pl.multiple_of(peer * dp_rows, 16), dp_rows)], act_g.at[j],
                s_act.at[d], r_act.at[d], peer,
            )

        for copy in loads[:5]:
            copy.wait()

        def one_hot(ref, size):
            row = iota((samples, size), 0)
            lane = iota((samples, size), 1)
            hot = jnp.zeros((samples, size), F32)
            for b in range(samples):
                hot = jnp.where((row == b) & (lane == ref[b]), 1.0, hot)
            return hot.astype(BF16)

        def lookup(ref, table, size):
            whole = size // 16 * 16
            hot = one_hot(ref, whole + 16)
            last = table[whole:size, :].astype(F32)
            last = jnp.concatenate([last, jnp.zeros((16 - size + whole, width), F32)], axis=0)
            return dot(hot[:, :whole], table[0:whole, :], 1, 0) + dot(
                hot[:, whole:], last.astype(BF16), 1, 0
            )

        time_embed = lookup(tsteps, t_tab, tab_t.shape[0])
        classes = tab_c.shape[0] - 1
        cond_embed = lookup(labels, c_tab, classes) + time_embed
        null_row = c_tab[classes - 8 :, :].astype(F32)[8:9]
        null_embed = null_row + time_embed
        student_embed = cond_embed + dot(one_hot(guides, tab_g.shape[0]), g_tab[...], 1, 0)

        def silu(v):
            return v / (1.0 + jnp.exp(-v))

        student_act = silu(student_embed)
        teacher_act = jnp.concatenate([silu(cond_embed), silu(null_embed)], axis=0).astype(BF16)
        acts[...] = jnp.zeros_like(acts)
        acts[:, 0:samples] = jnp.transpose(student_act).astype(BF16)
        student_act = jnp.concatenate([student_act, jnp.zeros_like(student_act)], axis=0).astype(BF16)
        lane_t = iota((1, 2 * samples), 1)
        factor = jnp.zeros((1, 2 * samples), F32)
        for b in range(samples):
            strength = strengths[guides[b]]
            factor = jnp.where(lane_t == b, -(1.0 + strength) * norm_scale, factor)
            factor = jnp.where(lane_t == samples + b, strength * norm_scale, factor)
        spread = jnp.zeros((HD, 256), F32)
        for k in range(3):
            value_t = dot(a_tab[0, k], teacher_act, 1, 1)
            value_s = dot(a_tab[1, k], student_act, 1, 1)
            if k == 2:
                value_t = value_t * factor
            for first, value in ((0, value_t), (2, value_s)):
                row = iota((2 * samples, 256), 0)
                lane = iota((2 * samples, 256), 1)
                b = lax.rem(row, samples)
                kind = first + row // samples
                target = 128 * (b // images) + 16 * lax.rem(b, images) + 3 * kind + k
                hot = jnp.where((lane == target) & (kind < 3), 1.0, 0.0).astype(BF16)
                spread = spread + dot(value.astype(BF16), hot, 1, 0)
        for kk in range(2):
            half = spread[:, 128 * kk : 128 * (kk + 1)]
            low = jnp.concatenate(
                [pltpu.roll(half[SPLIT:], 64, 1), jnp.zeros((2 * SPLIT - HD, 128), F32)], axis=0
            )
            mods[kk] = (half[:SPLIT] + low).astype(BF16)

        pl.semaphore_wait(barrier, n_t + n_dp - 2)
        own_noisy.wait()
        for copy in mate_noisy:
            copy.start()
        for d in range(1, n_t):
            mod_copy(d).start()
        for i in range(images):
            mate_noisy[i].wait_recv()
            own = noisy_v[images * core + i].astype(F32)
            other = noisy_p[i].astype(F32)
            first = jnp.where(core == 0, own, other)
            second = jnp.where(core == 0, other, own)
            noisy_g[i, chip] = jnp.concatenate([first, second], axis=0).astype(BF16)
            if i == 0:
                gather_start(noisy_g, 0, s_ag, r_ag, NOISY[0])
        for copy in w_copies:
            copy.start()
        mod_g[t] = mods[core]
        act_g[j] = acts[pl.ds(pl.multiple_of(j * dp_rows, 16), dp_rows), :]

        gather_pass(noisy_g, 0, s_ag, r_ag, NOISY[0])
        gather_start(noisy_g, 1, s_ag, r_ag, NOISY[1])
        for d in range(1, n_dp):
            act_copy(d).start()

        for copy in loads[5:]:
            copy.wait()
        for copy in w_copies:
            copy.wait_recv()
        for m in range(2):
            both = jnp.concatenate([wq_g[m, 0].astype(F32), wq_g[m, 1].astype(F32)], axis=0)
            wq_cat[m] = both.astype(BF16)
            if m == 1:
                wq_tr[...] = jnp.transpose(both).astype(BF16)
            both = jnp.concatenate([wo_g[m, 0].astype(F32), wo_g[m, 1].astype(F32)], axis=0)
            if m == 1:
                wo_cat[...] = both.astype(BF16)
            wo_tr[m] = jnp.transpose(both).astype(BF16)
        acc_q[...] = jnp.zeros_like(acc_q)
        acc_o[...] = jnp.zeros_like(acc_o)
        gmod[...] = jnp.zeros_like(gmod)

        for d in range(1, n_t):
            mod_copy(d).wait_recv()
        for src in range(n_t):
            piece = mod_g[src].astype(F32)
            for b in range(images):
                near = piece if b == 0 else pltpu.roll(piece, 128 - 16 * b, 1)
                far = pltpu.roll(piece, 64 - 16 * b, 1)
                mod_i[b, HD * src : HD * src + SPLIT, :] = near
                mod_i[b, HD * src + SPLIT : HD * (src + 1), :] = far[: HD - SPLIT]

        def padded(value):
            rows = jnp.zeros((HP - HD, seq), F32)
            return jnp.concatenate([value, rows], axis=0).astype(BF16)

        def attend(q, k, v):
            scores = dot(k, q, 0, 0) * (1.0 / math.sqrt(HD))
            exponent = jnp.exp(scores - jnp.max(scores, axis=0, keepdims=True))
            p = exponent * (1.0 / jnp.sum(exponent, axis=0, keepdims=True))
            return p, dot(v, p.astype(BF16), 1, 0)[:HD]

        def forward_in(i):
            for q in range(images):

                @pl.when(i == q)
                def _():
                    gather_end(noisy_g, q, s_ag, r_ag, NOISY[q])

            total = jnp.zeros((1, seq), F32)
            square = jnp.zeros((1, seq), F32)
            for c in range(chips):
                value = noisy_g[i, c].astype(F32)
                total = total + jnp.sum(value, axis=0, keepdims=True)
                square = square + jnp.sum(value * value, axis=0, keepdims=True)
            mean = total * (1.0 / width)
            rstd = lax.rsqrt(square * (1.0 / width) - mean * mean + norm_eps)
            for c in range(chips):
                rows = slice(block * c, block * (c + 1))
                n = ((noisy_g[i, c].astype(F32) - mean) * rstd).astype(BF16)
                normed[i, rows, :] = n
                n = n.astype(F32)
                for a in range(3):
                    shift = mod_i[i, rows, 3 * a : 3 * a + 1]
                    scale = mod_i[i, rows, 3 * a + 1 : 3 * a + 2]
                    value = (n * (1.0 + scale) + shift).astype(BF16)
                    if a == 2:
                        mod_s[i, rows, :] = value
                    else:
                        mod_t[a, rows, :] = value

        def forward_model(i, a):
            act = mod_s[i] if a == 2 else mod_t[a]
            qkv = dot(wq_cat[0 if a < 2 else 1], act, 1, 0)
            heads = []
            for h in range(2):
                q, k, v = (
                    padded(qkv[HW * h + HD * e : HW * h + HD * (e + 1)]) for e in range(3)
                )
                p, mix = attend(q, k, v)
                heads.append(mix)
                if a == 2:
                    prob[i, h] = p
                    mixed_s[i, h] = mix.astype(BF16)
                    for e, value in enumerate((q, k, v)):
                        qkv_s[i, h, e] = value
            mixed[a] = jnp.concatenate(heads, axis=0).astype(BF16)

        def forward_out(i):
            for c in range(chips):
                rows = slice(block * c, block * (c + 1))
                sums = jnp.zeros((block, seq), F32)
                for a in range(3):
                    value = dot(wo_tr[0 if a < 2 else 1, rows, :], mixed[a], 1, 0)
                    gate = mod_i[i, rows, 3 * a + 2 : 3 * a + 3]
                    if a == 2:
                        proj_s[i, rows, :] = value.astype(BF16)
                        gate = gate * norm_scale
                    sums = sums + value * gate
                part[i, c] = sums.astype(BF16)
            sum_start(i)

        def backward_in(i):
            for q in range(images):

                @pl.when(i == q)
                def _():
                    gather_end(cot, q, s_c, r_c, COT[q])

            grads = []
            for c in range(chips):
                rows = slice(block * c, block * (c + 1))
                value = cot[i, c].astype(F32)
                gp[rows, :] = (value * mod_i[i, rows, 8:9]).astype(BF16)
                grads.append(
                    jnp.sum(value * proj_s[i, rows, :].astype(F32), axis=1, keepdims=True)
                )
            grad_gate = jnp.concatenate(grads, axis=0)
            lane = iota((width, 128), 1)
            gmod[...] += jnp.where(lane == 8 + i, grad_gate, 0.0)
            grad_mixed = dot(wo_cat[...], gp[...], 1, 0)
            acts_grad = []
            for h in range(2):
                low = padded(grad_mixed[HD * h : HD * (h + 1)])
                acc_o[h, :, 0:HD] += dot(gp[...], mixed_s[i, h], 1, 1)
                q, k, v = (qkv_s[i, h, e] for e in range(3))
                p = prob[i, h]
                grad_prob = dot(v, low, 0, 0)
                delta = jnp.sum(p * grad_prob, axis=0, keepdims=True)
                ds = (p * (grad_prob - delta) * (1.0 / math.sqrt(HD))).astype(BF16)
                acts_grad.append(dot(k, ds, 1, 0)[:HD])
                acts_grad.append(dot(q, ds, 1, 1)[:HD])
                acts_grad.append(dot(low, p.astype(BF16), 1, 1)[:HD])
            gqkv[...] = jnp.concatenate(acts_grad, axis=0).astype(BF16)
            for h in range(2):
                head = jnp.concatenate(acts_grad[3 * h : 3 * h + 3], axis=0).astype(BF16)
                acc_q[h, :, 0:HW] += dot(mod_s[i], head, 1, 1)

        def backward_out(i):
            shifts = []
            scales = []
            for c in range(chips):
                rows = slice(block * c, block * (c + 1))
                value = dot(wq_tr[rows, :], gqkv[...], 1, 0)
                shifts.append(jnp.sum(value, axis=1, keepdims=True))
                scales.append(
                    jnp.sum(value * normed[i, rows, :].astype(F32), axis=1, keepdims=True)
                )
            lane = iota((width, 128), 1)
            gmod[...] += jnp.where(lane == i, jnp.concatenate(shifts, axis=0), 0.0) + jnp.where(
                lane == 4 + i, jnp.concatenate(scales, axis=0), 0.0
            )

        stages = {
            "n_start": lambda q: gather_start(noisy_g, q, s_ag, r_ag, NOISY[q]),
            "n_pass": lambda q: gather_pass(noisy_g, q, s_ag, r_ag, NOISY[q]),
            "s_pass": sum_pass,
            "s_end": sum_end,
            "c_pass": lambda q: gather_pass(cot, q, s_c, r_c, COT[q]),
        }

        def at(i, point, table):
            for (step, where), names in table.items():
                if where == point:

                    @pl.when(i == step)
                    def _():
                        for name, q in names:
                            stages[name](q)

        def forward_step(i, carry):
            forward_in(i)
            at(i, 1, FORWARD)
            forward_model(i, 0)
            at(i, 2, FORWARD)
            forward_model(i, 1)
            at(i, 3, FORWARD)
            forward_model(i, 2)
            at(i, 4, FORWARD)
            forward_out(i)
            return carry

        lax.fori_loop(0, images, forward_step, 0)

        def gm_copy(d):
            peer = lax.rem(t + d, n_t)
            return to_tensor(gm_send.at[peer], gm_in.at[t], s_gm.at[d], r_gm.at[d], peer)

        def pair_copy(s):
            return to_tensor(pair.at[s], pair_in.at[s], s_pair.at[s], r_pair.at[s], mate_t)

        def dp_copies(d):
            peer = lax.rem(j + d, n_dp)
            return [
                to_dp(dp_sum.at[peer], dp_in.at[j], s_dq.at[d], r_dq.at[d], peer),
                to_dp(dp_ex.at[peer], dp_ex_in.at[j], s_do.at[d], r_do.at[d], peer),
            ]

        third = dp_rows // 3
        early = [d for d in range(1, n_dp)]

        def gd_copy(d):
            peer = lax.rem(j + d, n_dp)
            return to_dp(gm_sum, gm_all.at[j], s_gd.at[d], r_gd.at[d], peer)

        def chunk(s):
            return pl.ds(pl.multiple_of(s * dp_rows, 16), dp_rows)

        def backward_step(i, carry):
            at(i, 0, BACKWARD)
            backward_in(i)
            at(i, 1, BACKWARD)

            @pl.when(i == images - 1)
            def _():
                for d in range(1, n_dp + 1):
                    s = lax.rem(j + d, n_dp)
                    pair[s, :, 0:256] = acc_q[mate, chunk(s), :].astype(BF16)
                    pair[s, :, 256:384] = acc_o[mate, chunk(s), :].astype(BF16)
                    pair_copy(s).start()

            backward_out(i)
            at(i, 2, BACKWARD)
            return carry

        lax.fori_loop(0, images, backward_step, 0)

        for src in range(n_t):
            packed = gmod[HD * src : HD * src + 8, :]
            for g in range(1, groups):
                rows = slice(HD * src + 8 * g, HD * src + 8 * (g + 1))
                packed = packed + pltpu.roll(gmod[rows, :], 12 * g, 1)
            gm_send[src] = packed
        for d in range(1, n_t):
            gm_copy(d).start()
        gm_in[t] = gm_send[t]
        for d in range(1, n_dp + 1):
            s = lax.rem(j + d, n_dp)
            pair_copy(s).wait_recv()
            sums_q = acc_q[core, chunk(s), :] + pair_in[s, :, 0:256].astype(F32)
            sums_o = acc_o[core, chunk(s), :] + pair_in[s, :, 256:384].astype(F32)
            moved = pltpu.roll(sums_o, 128 - FREE, 1)
            lane = iota((dp_rows, 128), 1)
            dp_sum[s, :, 0:128] = sums_q[:, :128].astype(BF16)
            dp_sum[s, :, 128:256] = (
                sums_q[:, 128:] + jnp.where(lane >= 128 - FREE, moved, 0.0)
            ).astype(BF16)
            rest = jnp.where(lane < HD - FREE, moved, 0.0)
            dp_ex[s] = (
                rest[:third]
                + pltpu.roll(rest[third : 2 * third], 32, 1)
                + pltpu.roll(rest[2 * third :], 64, 1)
            ).astype(BF16)
            if d in early:
                for copy in dp_copies(d):
                    copy.start()
        for d in range(1, n_t):
            gm_copy(d).wait_recv()
        for kk in range(2):
            total = gm_in[kk]
            for c in range(1, chips):
                total = total + gm_in[2 * c + kk]
            gm_sum[kk] = total
        for d in range(1, n_dp):
            gd_copy(d).start()
        for d in range(1, n_dp):
            if d not in early:
                for copy in dp_copies(d):
                    copy.start()
        gm_all[j] = gm_sum[...]
        for d in range(1, n_dp):
            act_copy(d).wait_recv()
        rows_act = act_g[0].astype(F32)
        for s in range(1, n_dp):
            rows_act = rows_act + pltpu.roll(act_g[s].astype(F32), samples * s, 1)

        total = dp_sum[j].astype(F32)
        rest = dp_ex[j].astype(F32)
        for d in range(1, n_dp):
            for copy in dp_copies(d):
                copy.wait_recv()
        for d in range(1, n_dp):
            src = lax.rem(j + d, n_dp)
            total = total + dp_in[src].astype(F32)
            rest = rest + dp_ex_in[src].astype(F32)
        gq_out[...] = total[:, :HW]
        lane = iota((dp_rows, 128), 1)
        spread = jnp.concatenate(
            [rest, pltpu.roll(rest, 128 - 32, 1), pltpu.roll(rest, 128 - 64, 1)], axis=0
        )
        total_o = jnp.where(lane >= 128 - FREE, total[:, 128:], 0.0) + jnp.where(
            lane < HD - FREE, spread, 0.0
        )
        go_out[...] = jnp.transpose(pltpu.roll(total_o, FREE, 1))[:HD]

        for d in range(1, n_dp):
            gd_copy(d).wait_recv()
        lane = iota((8, 128), 1)
        for k in range(3):
            pieces = []
            for g in range(groups):
                value = jnp.zeros((8, 128), F32)
                for s in range(n_dp):
                    for kk in range(2):
                        at = samples * s + images * kk
                        shift = (at - 12 * g - 4 * k) % 128
                        moved = gm_all[s, kk]
                        if shift:
                            moved = pltpu.roll(moved, shift, 1)
                        value = jnp.where((lane >= at) & (lane < at + images), moved, value)
                pieces.append(value)
            ga_out[k] = lax.dot_general(
                rows_act, jnp.concatenate(pieces, axis=0), (((1,), (1,)), ((), ())),
                precision=lax.Precision.HIGHEST, preferred_element_type=F32,
            )

        for copy in mate_noisy + w_copies:
            copy.wait_send()
        for s in range(n_dp):
            pair_copy(s).wait_send()
        for d in range(1, n_t):
            mod_copy(d).wait_send()
            gm_copy(d).wait_send()
        for d in range(1, n_dp):
            act_copy(d).wait_send()
            gd_copy(d).wait_send()
            for copy in dp_copies(d):
                copy.wait_send()
        for i in range(images):
            of_noisy = gather_z if NOISY[i] else gather_x
            of_cot = gather_z if COT[i] else gather_x
            for copy in (
                sum(of_noisy(noisy_g, i, s_ag, r_ag)[:2], [])
                + sum(of_cot(cot, i, s_c, r_c)[:2], [])
                + sum(sum_z(i), [])
            ):
                copy.wait_send()

    vm = pltpu.VMEM
    dma = pltpu.SemaphoreType.DMA
    scratch = [
        vm((images, HD, seq), BF16),
        vm((samples, HD, seq), BF16),
        vm((images, chips, block, seq), BF16),
        vm((1001, width), BF16),
        vm((1000, width), BF16),
        vm((32, width), BF16),
        vm((2, 3, HD, width), BF16),
        vm((2, SPLIT, 128), BF16),
        vm((n_t, SPLIT, 128), BF16),
        vm((images, width, 128), F32),
        vm((width, 128), BF16),
        vm((n_dp, dp_rows, 128), BF16),
        vm((2, 2, HW, width), BF16),
        vm((2, 2, HD, width), BF16),
        vm((2, 2 * HW, width), BF16),
        vm((width, 2 * HW), BF16),
        vm((2 * HD, width), BF16),
        vm((2, width, 2 * HD), BF16),
        vm((images, width, seq), BF16),
        vm((images, width, seq), BF16),
        vm((2, width, seq), BF16),
        vm((3, 2 * HD, seq), BF16),
        vm((images, 2, HD, seq), BF16),
        vm((images, width, seq), BF16),
        vm((images, 2, seq, seq), F32),
        vm((images, 2, 3, HP, seq), BF16),
        vm((images, chips, block, seq), BF16),
        vm((images, 2 * n_x, block, seq), BF16),
        vm((images, chips, block, seq), BF16),
        vm((width, seq), BF16),
        vm((2 * HW, seq), BF16),
        vm((2, width, 256), F32),
        vm((2, width, 128), F32),
        vm((width, 128), F32),
        vm((n_t, 8, 128), F32),
        vm((n_t, 8, 128), F32),
        vm((2, 8, 128), F32),
        vm((n_dp, 2, 8, 128), F32),
        vm((n_dp, dp_rows, 384), BF16),
        vm((n_dp, dp_rows, 384), BF16),
        vm((n_dp, dp_rows, 256), BF16),
        vm((n_dp, dp_rows, 256), BF16),
        vm((n_dp, dp_rows // 3, 128), BF16),
        vm((n_dp, dp_rows // 3, 128), BF16),
        dma((10,)),
        dma((images,)),
        dma((images,)),
        dma((4,)),
        dma((4,)),
        dma((n_t,)),
        dma((n_t,)),
        dma((n_dp,)),
        dma((n_dp,)),
        dma((images, 2 * n_x)),
        dma((images, 2 * n_x)),
        dma((images, 2 * n_x)),
        dma((images, 2 * n_x)),
        dma((images, 2 * n_x)),
        dma((images, 2 * n_x)),
        dma((n_t,)),
        dma((n_t,)),
        dma((n_dp,)),
        dma((n_dp,)),
        dma((n_dp,)),
        dma((n_dp,)),
        dma((n_dp,)),
        dma((n_dp,)),
        dma((n_dp,)),
        dma((n_dp,)),
    ]
    any_spec = pl.BlockSpec(memory_space=pl.ANY)
    smem_spec = pl.BlockSpec(memory_space=pltpu.SMEM)
    vmem_spec = pl.BlockSpec(memory_space=pltpu.VMEM)
    return pl.pallas_call(
        kernel,
        out_shape=(
            jax.ShapeDtypeStruct((dp_rows, HW), F32),
            jax.ShapeDtypeStruct((HD, dp_rows), F32),
            jax.ShapeDtypeStruct((3, dp_rows, HD), F32),
        ),
        in_specs=[smem_spec] * 4 + [any_spec] * 10,
        out_specs=(vmem_spec,) * 3,
        scratch_shapes=scratch,
        compiler_params=pltpu.CompilerParams(
            collective_id=0, has_side_effects=True, vmem_limit_bytes=60 * 1024 * 1024
        ),
        name="step",
    )


def pass_on(*refs):
    half = len(refs) // 2
    for src, dst in zip(refs[:half], refs[half:]):
        dst[...] = src[...]


def local(
    noisy,
    labels,
    tsteps,
    guide_index,
    class_table,
    time_table,
    guide_table,
    guide_weights,
    teacher_qkv,
    teacher_out,
    teacher_ada,
    student_qkv,
    student_out,
    student_ada,
):
    samples, seq_len, _ = noisy.shape
    n_t = lax.axis_size("tensor")
    n_dp = lax.axis_size("dp")
    norm_scale = 1.0 / math.sqrt(samples * n_dp * seq_len)
    step = make_kernel(n_t, n_dp, samples, seq_len, norm_scale)
    grads = step(
        labels, tsteps, guide_index, guide_weights,
        jnp.swapaxes(noisy, 1, 2), class_table, time_table, guide_table,
        teacher_qkv.T, student_qkv.T, teacher_out, student_out,
        jnp.swapaxes(teacher_ada, 1, 2), jnp.swapaxes(student_ada, 1, 2),
    )
    return pl.pallas_call(
        pass_on,
        out_shape=tuple(jax.ShapeDtypeStruct(g.shape, g.dtype) for g in grads),
        name="pass_on",
    )(*grads)


def solution(mesh):
    return jax.shard_map(
        local,
        mesh=mesh,
        in_specs=(
            P("dp", None, "tensor"),
            P("dp"),
            P("dp"),
            P("dp"),
            P(),
            P(),
            P(),
            P(),
            P(None, "tensor"),
            P("tensor", None),
            P(None, None, "tensor"),
            P(None, "tensor"),
            P("tensor", None),
            P(None, None, "tensor"),
        ),
        out_specs=(P("dp", "tensor"), P("tensor", "dp"), P(None, "dp", "tensor")),
        check_vma=False,
    )
```

```python
import math

import jax
import jax.numpy as jnp
from jax import lax
from jax.experimental import pallas as pl
from jax.experimental.pallas import tpu as pltpu
from jax.sharding import PartitionSpec as P

HD = 72
HW = 3 * HD
HP = 80
FREE = 256 - HW
norm_eps = 1e-06
F32 = jnp.float32
BF16 = jnp.bfloat16
MESH = pl.DeviceIdType.MESH
SPLIT = 40

NOISY = (True, True, True, True)
COT = (True, False, False, True)
FORWARD = {
    (0, 1): (("n_pass", 1), ("n_start", 2)),
    (0, 4): (("n_pass", 2), ("n_start", 3)),
    (1, 2): (("n_pass", 3),),
    (2, 2): (("s_pass", 0),),
    (3, 1): (("s_end", 0),),
    (3, 2): (("s_pass", 1),),
    (3, 4): (("c_pass", 0), ("s_end", 1)),
}
BACKWARD = {
    (0, 0): (("s_pass", 2),),
    (0, 1): (("c_pass", 1),),
    (0, 2): (("s_end", 2), ("s_pass", 3)),
    (1, 1): (("c_pass", 2), ("s_end", 3)),
    (1, 2): (("c_pass", 3),),
}


def dot(a, b, ca, cb):
    return lax.dot_general(a, b, (((ca,), (cb,)), ((), ())), preferred_element_type=F32)


def iota(shape, dim):
    return lax.broadcasted_iota(jnp.int32, shape, dim)


def make_kernel(n_t, n_dp, samples, seq, norm_scale):
    chips = n_t // 2
    n_x = chips // 2
    images = samples // 2
    width = HD * n_t
    block = 2 * HD
    dp_rows = width // n_dp
    groups = HD // 8

    def kernel(
        labels, tsteps, guides, strengths,
        noisy, tab_c, tab_t, tab_g, wq_t, wq_s, wo_t, wo_s, ada_t, ada_s,
        gq_out, go_out, ga_out,
        noisy_p, noisy_v, noisy_g, c_tab, t_tab, g_tab, a_tab, mods, mod_g, mod_i, acts, act_g,
        wq_g, wo_g, wq_cat, wq_tr, wo_cat, wo_tr,
        normed, mod_s, mod_t, mixed, mixed_s, proj_s, prob, qkv_s,
        part, rs_in, cot, gp, gqkv, acc_q, acc_o, gmod, gm_send, gm_in, gm_sum, gm_all,
        pair, pair_in, dp_sum, dp_in, dp_ex, dp_ex_in,
        l_sem, s_n, r_n, s_w, r_w, s_mod, r_mod, s_act, r_act,
        s_ag, r_ag, s_rs, r_rs, s_c, r_c, s_gm, r_gm, s_pair, r_pair,
        s_dq, r_dq, s_do, r_do, s_gd, r_gd,
    ):
        t = lax.axis_index("tensor")
        j = lax.axis_index("dp")
        chip = t // 2
        core = lax.rem(t, 2)
        x = chip // 2
        z = lax.rem(chip, 2)
        mate = 1 - core
        mate_t = 2 * chip + mate
        chip_z = 2 * x + 1 - z

        loads = [
            pltpu.make_async_copy(tab_c, c_tab, l_sem.at[0]),
            pltpu.make_async_copy(tab_t, t_tab, l_sem.at[1]),
            pltpu.make_async_copy(tab_g, g_tab, l_sem.at[2]),
            pltpu.make_async_copy(ada_t, a_tab.at[0], l_sem.at[3]),
            pltpu.make_async_copy(ada_s, a_tab.at[1], l_sem.at[4]),
            pltpu.make_async_copy(wq_t, wq_g.at[0, core], l_sem.at[5]),
            pltpu.make_async_copy(wq_s, wq_g.at[1, core], l_sem.at[6]),
            pltpu.make_async_copy(wo_t, wo_g.at[0, core], l_sem.at[7]),
            pltpu.make_async_copy(wo_s, wo_g.at[1, core], l_sem.at[8]),
        ]
        own_noisy = pltpu.make_async_copy(noisy, noisy_v, l_sem.at[9])
        own_noisy.start()
        for copy in loads:
            copy.start()

        barrier = pltpu.get_barrier_semaphore()
        for d in range(1, n_t):
            pl.semaphore_signal(
                barrier, inc=1, device_id={"tensor": lax.rem(t + d, n_t)}, device_id_type=MESH
            )
        for d in range(1, n_dp):
            pl.semaphore_signal(
                barrier, inc=1, device_id={"dp": lax.rem(j + d, n_dp)}, device_id_type=MESH
            )
        def to_tensor(src, dst, ss, rs, peer):
            return pltpu.make_async_remote_copy(
                src_ref=src, dst_ref=dst, send_sem=ss, recv_sem=rs,
                device_id={"tensor": peer}, device_id_type=MESH,
            )

        def to_dp(src, dst, ss, rs, peer):
            return pltpu.make_async_remote_copy(
                src_ref=src, dst_ref=dst, send_sem=ss, recv_sem=rs,
                device_id={"dp": peer}, device_id_type=MESH,
            )

        def x_chip(d):
            return 2 * lax.rem(x + d, n_x) + z

        def device_of(c):
            return 2 * c + core

        def gather_z(buf, i, ss, rs):
            own = buf.at[i, chip]
            first = [to_tensor(own, own, ss.at[i, 0], rs.at[i, 0], device_of(chip_z))]
            first += [
                to_tensor(own, own, ss.at[i, d], rs.at[i, d], device_of(x_chip(d)))
                for d in range(1, n_x)
            ]
            other = buf.at[i, chip_z]
            second = [
                to_tensor(other, other, ss.at[i, n_x + d], rs.at[i, n_x + d], device_of(x_chip(d)))
                for d in range(1, n_x)
            ]
            return first, second, first[:1]

        def gather_x(buf, i, ss, rs):
            own = buf.at[i, chip]
            first = [
                to_tensor(own, own, ss.at[i, d], rs.at[i, d], device_of(x_chip(d)))
                for d in range(1, n_x)
            ]
            ahead = len(first)
            first.append(to_tensor(own, own, ss.at[i, n_x], rs.at[i, n_x], device_of(chip_z)))
            second = []
            for d in range(1, n_x):
                other = buf.at[i, 2 * lax.rem(x + n_x - d, n_x) + z]
                second.append(
                    to_tensor(
                        other, other, ss.at[i, n_x + d], rs.at[i, n_x + d], device_of(chip_z)
                    )
                )
            return first, second, first[:ahead]

        def gather_start(buf, i, ss, rs, z_first):
            for copy in (gather_z if z_first else gather_x)(buf, i, ss, rs)[0]:
                copy.start()

        def gather_pass(buf, i, ss, rs, z_first):
            _, second, needed = (gather_z if z_first else gather_x)(buf, i, ss, rs)
            for copy in needed:
                copy.wait_recv()
            for copy in second:
                copy.start()

        def gather_end(buf, i, ss, rs, z_first):
            first, second, needed = (gather_z if z_first else gather_x)(buf, i, ss, rs)
            for copy in first + second:
                if not any(copy is other for other in needed):
                    copy.wait_recv()

        def sum_z(i):
            first = [
                to_tensor(
                    part.at[i, 2 * e + 1 - z], rs_in.at[i, e],
                    s_rs.at[i, e], r_rs.at[i, e], device_of(chip_z),
                )
                for e in range(n_x)
            ]
            second = [
                to_tensor(
                    part.at[i, x_chip(d)], rs_in.at[i, n_x + d],
                    s_rs.at[i, n_x + d], r_rs.at[i, n_x + d], device_of(x_chip(d)),
                )
                for d in range(1, n_x)
            ]
            return first, second

        def sum_start(i):
            for copy in sum_z(i)[0]:
                copy.start()

        def sum_pass(i):
            first, second = sum_z(i)
            for copy in first:
                copy.wait_recv()
            for d in range(1, n_x):
                e = lax.rem(x + d, n_x)
                total = part[i, 2 * e + z].astype(F32) + rs_in[i, e].astype(F32)
                part[i, 2 * e + z] = total.astype(BF16)
            for copy in second:
                copy.start()

        def sum_end(i):
            for copy in sum_z(i)[1]:
                copy.wait_recv()
            total = part[i, chip].astype(F32) + rs_in[i, x].astype(F32)
            for d in range(1, n_x):
                total = total + rs_in[i, n_x + d].astype(F32)
            cot[i, chip] = total.astype(BF16)
            gather_start(cot, i, s_c, r_c, COT[i])

        mate_noisy = [
            to_tensor(noisy_v.at[images * mate + i], noisy_p.at[i], s_n.at[i], r_n.at[i], mate_t)
            for i in range(images)
        ]
        w_copies = [
            to_tensor(wq_t, wq_g.at[0, core], s_w.at[0], r_w.at[0], mate_t),
            to_tensor(wq_s, wq_g.at[1, core], s_w.at[1], r_w.at[1], mate_t),
            to_tensor(wo_t, wo_g.at[0, core], s_w.at[2], r_w.at[2], mate_t),
            to_tensor(wo_s, wo_g.at[1, core], s_w.at[3], r_w.at[3], mate_t),
        ]
        def mod_copy(d):
            peer = lax.rem(t + d, n_t)
            return to_tensor(
                mods.at[lax.rem(peer, 2)], mod_g.at[t], s_mod.at[d], r_mod.at[d], peer
            )

        def act_copy(d):
            peer = lax.rem(j + d, n_dp)
            return to_dp(
                acts.at[pl.ds(pl.multiple_of(peer * dp_rows, 16), dp_rows)], act_g.at[j],
                s_act.at[d], r_act.at[d], peer,
            )

        for copy in loads[:5]:
            copy.wait()

        def one_hot(ref, size):
            row = iota((samples, size), 0)
            lane = iota((samples, size), 1)
            hot = jnp.zeros((samples, size), F32)
            for b in range(samples):
                hot = jnp.where((row == b) & (lane == ref[b]), 1.0, hot)
            return hot.astype(BF16)

        def lookup(ref, table, size):
            whole = size // 16 * 16
            hot = one_hot(ref, whole + 16)
            last = table[whole:size, :].astype(F32)
            last = jnp.concatenate([last, jnp.zeros((16 - size + whole, width), F32)], axis=0)
            return dot(hot[:, :whole], table[0:whole, :], 1, 0) + dot(
                hot[:, whole:], last.astype(BF16), 1, 0
            )

        time_embed = lookup(tsteps, t_tab, tab_t.shape[0])
        classes = tab_c.shape[0] - 1
        cond_embed = lookup(labels, c_tab, classes) + time_embed
        null_row = c_tab[classes - 8 :, :].astype(F32)[8:9]
        null_embed = null_row + time_embed
        student_embed = cond_embed + dot(one_hot(guides, tab_g.shape[0]), g_tab[...], 1, 0)

        def silu(v):
            return v / (1.0 + jnp.exp(-v))

        student_act = silu(student_embed)
        teacher_act = jnp.concatenate([silu(cond_embed), silu(null_embed)], axis=0).astype(BF16)
        acts[...] = jnp.zeros_like(acts)
        acts[:, 0:samples] = jnp.transpose(student_act).astype(BF16)
        student_act = jnp.concatenate([student_act, jnp.zeros_like(student_act)], axis=0).astype(BF16)
        lane_t = iota((1, 2 * samples), 1)
        factor = jnp.zeros((1, 2 * samples), F32)
        for b in range(samples):
            strength = strengths[guides[b]]
            factor = jnp.where(lane_t == b, -(1.0 + strength) * norm_scale, factor)
            factor = jnp.where(lane_t == samples + b, strength * norm_scale, factor)
        spread = jnp.zeros((HD, 256), F32)
        for k in range(3):
            value_t = dot(a_tab[0, k], teacher_act, 1, 1)
            value_s = dot(a_tab[1, k], student_act, 1, 1)
            if k == 2:
                value_t = value_t * factor
            for first, value in ((0, value_t), (2, value_s)):
                row = iota((2 * samples, 256), 0)
                lane = iota((2 * samples, 256), 1)
                b = lax.rem(row, samples)
                kind = first + row // samples
                target = 128 * (b // images) + 16 * lax.rem(b, images) + 3 * kind + k
                hot = jnp.where((lane == target) & (kind < 3), 1.0, 0.0).astype(BF16)
                spread = spread + dot(value.astype(BF16), hot, 1, 0)
        for kk in range(2):
            half = spread[:, 128 * kk : 128 * (kk + 1)]
            low = jnp.concatenate(
                [pltpu.roll(half[SPLIT:], 64, 1), jnp.zeros((2 * SPLIT - HD, 128), F32)], axis=0
            )
            mods[kk] = (half[:SPLIT] + low).astype(BF16)

        pl.semaphore_wait(barrier, n_t + n_dp - 2)
        own_noisy.wait()
        for copy in mate_noisy:
            copy.start()
        for d in range(1, n_t):
            mod_copy(d).start()
        for i in range(images):
            mate_noisy[i].wait_recv()
            own = noisy_v[images * core + i].astype(F32)
            other = noisy_p[i].astype(F32)
            first = jnp.where(core == 0, own, other)
            second = jnp.where(core == 0, other, own)
            noisy_g[i, chip] = jnp.concatenate([first, second], axis=0).astype(BF16)
            if i == 0:
                gather_start(noisy_g, 0, s_ag, r_ag, NOISY[0])
        for copy in w_copies:
            copy.start()
        mod_g[t] = mods[core]
        act_g[j] = acts[pl.ds(pl.multiple_of(j * dp_rows, 16), dp_rows), :]

        gather_pass(noisy_g, 0, s_ag, r_ag, NOISY[0])
        gather_start(noisy_g, 1, s_ag, r_ag, NOISY[1])
        for d in range(1, n_dp):
            act_copy(d).start()

        for copy in loads[5:]:
            copy.wait()
        for copy in w_copies:
            copy.wait_recv()
        for m in range(2):
            both = jnp.concatenate([wq_g[m, 0].astype(F32), wq_g[m, 1].astype(F32)], axis=0)
            wq_cat[m] = both.astype(BF16)
            if m == 1:
                wq_tr[...] = jnp.transpose(both).astype(BF16)
            both = jnp.concatenate([wo_g[m, 0].astype(F32), wo_g[m, 1].astype(F32)], axis=0)
            if m == 1:
                wo_cat[...] = both.astype(BF16)
            wo_tr[m] = jnp.transpose(both).astype(BF16)
        acc_q[...] = jnp.zeros_like(acc_q)
        acc_o[...] = jnp.zeros_like(acc_o)
        gmod[...] = jnp.zeros_like(gmod)

        for d in range(1, n_t):
            mod_copy(d).wait_recv()
        for src in range(n_t):
            piece = mod_g[src].astype(F32)
            for b in range(images):
                near = piece if b == 0 else pltpu.roll(piece, 128 - 16 * b, 1)
                far = pltpu.roll(piece, 64 - 16 * b, 1)
                mod_i[b, HD * src : HD * src + SPLIT, :] = near
                mod_i[b, HD * src + SPLIT : HD * (src + 1), :] = far[: HD - SPLIT]

        def padded(value):
            rows = jnp.zeros((HP - HD, seq), F32)
            return jnp.concatenate([value, rows], axis=0).astype(BF16)

        def attend(q, k, v):
            scores = dot(k, q, 0, 0) * (1.0 / math.sqrt(HD))
            exponent = jnp.exp(scores - jnp.max(scores, axis=0, keepdims=True))
            p = exponent * (1.0 / jnp.sum(exponent, axis=0, keepdims=True))
            return p, dot(v, p.astype(BF16), 1, 0)[:HD]

        def forward_in(i):
            for q in range(images):

                @pl.when(i == q)
                def _():
                    gather_end(noisy_g, q, s_ag, r_ag, NOISY[q])

            total = jnp.zeros((1, seq), F32)
            square = jnp.zeros((1, seq), F32)
            for c in range(chips):
                value = noisy_g[i, c].astype(F32)
                total = total + jnp.sum(value, axis=0, keepdims=True)
                square = square + jnp.sum(value * value, axis=0, keepdims=True)
            mean = total * (1.0 / width)
            rstd = lax.rsqrt(square * (1.0 / width) - mean * mean + norm_eps)
            for c in range(chips):
                rows = slice(block * c, block * (c + 1))
                n = ((noisy_g[i, c].astype(F32) - mean) * rstd).astype(BF16)
                normed[i, rows, :] = n
                n = n.astype(F32)
                for a in range(3):
                    shift = mod_i[i, rows, 3 * a : 3 * a + 1]
                    scale = mod_i[i, rows, 3 * a + 1 : 3 * a + 2]
                    value = (n * (1.0 + scale) + shift).astype(BF16)
                    if a == 2:
                        mod_s[i, rows, :] = value
                    else:
                        mod_t[a, rows, :] = value

        def forward_model(i, a):
            act = mod_s[i] if a == 2 else mod_t[a]
            qkv = dot(wq_cat[0 if a < 2 else 1], act, 1, 0)
            heads = []
            for h in range(2):
                q, k, v = (
                    padded(qkv[HW * h + HD * e : HW * h + HD * (e + 1)]) for e in range(3)
                )
                p, mix = attend(q, k, v)
                heads.append(mix)
                if a == 2:
                    prob[i, h] = p
                    mixed_s[i, h] = mix.astype(BF16)
                    for e, value in enumerate((q, k, v)):
                        qkv_s[i, h, e] = value
            mixed[a] = jnp.concatenate(heads, axis=0).astype(BF16)

        def forward_out(i):
            for c in range(chips):
                rows = slice(block * c, block * (c + 1))
                sums = jnp.zeros((block, seq), F32)
                for a in range(3):
                    value = dot(wo_tr[0 if a < 2 else 1, rows, :], mixed[a], 1, 0)
                    gate = mod_i[i, rows, 3 * a + 2 : 3 * a + 3]
                    if a == 2:
                        proj_s[i, rows, :] = value.astype(BF16)
                        gate = gate * norm_scale
                    sums = sums + value * gate
                part[i, c] = sums.astype(BF16)
            sum_start(i)

        def backward_in(i):
            for q in range(images):

                @pl.when(i == q)
                def _():
                    gather_end(cot, q, s_c, r_c, COT[q])

            grads = []
            for c in range(chips):
                rows = slice(block * c, block * (c + 1))
                value = cot[i, c].astype(F32)
                gp[rows, :] = (value * mod_i[i, rows, 8:9]).astype(BF16)
                grads.append(
                    jnp.sum(value * proj_s[i, rows, :].astype(F32), axis=1, keepdims=True)
                )
            grad_gate = jnp.concatenate(grads, axis=0)
            lane = iota((width, 128), 1)
            gmod[...] += jnp.where(lane == 8 + i, grad_gate, 0.0)
            grad_mixed = dot(wo_cat[...], gp[...], 1, 0)
            acts_grad = []
            for h in range(2):
                low = padded(grad_mixed[HD * h : HD * (h + 1)])
                acc_o[h, :, 0:HD] += dot(gp[...], mixed_s[i, h], 1, 1)
                q, k, v = (qkv_s[i, h, e] for e in range(3))
                p = prob[i, h]
                grad_prob = dot(v, low, 0, 0)
                delta = jnp.sum(p * grad_prob, axis=0, keepdims=True)
                ds = (p * (grad_prob - delta) * (1.0 / math.sqrt(HD))).astype(BF16)
                acts_grad.append(dot(k, ds, 1, 0)[:HD])
                acts_grad.append(dot(q, ds, 1, 1)[:HD])
                acts_grad.append(dot(low, p.astype(BF16), 1, 1)[:HD])
            gqkv[...] = jnp.concatenate(acts_grad, axis=0).astype(BF16)
            for h in range(2):
                head = jnp.concatenate(acts_grad[3 * h : 3 * h + 3], axis=0).astype(BF16)
                acc_q[h, :, 0:HW] += dot(mod_s[i], head, 1, 1)

        def backward_out(i):
            shifts = []
            scales = []
            for c in range(chips):
                rows = slice(block * c, block * (c + 1))
                value = dot(wq_tr[rows, :], gqkv[...], 1, 0)
                shifts.append(jnp.sum(value, axis=1, keepdims=True))
                scales.append(
                    jnp.sum(value * normed[i, rows, :].astype(F32), axis=1, keepdims=True)
                )
            lane = iota((width, 128), 1)
            gmod[...] += jnp.where(lane == i, jnp.concatenate(shifts, axis=0), 0.0) + jnp.where(
                lane == 4 + i, jnp.concatenate(scales, axis=0), 0.0
            )

        stages = {
            "n_start": lambda q: gather_start(noisy_g, q, s_ag, r_ag, NOISY[q]),
            "n_pass": lambda q: gather_pass(noisy_g, q, s_ag, r_ag, NOISY[q]),
            "s_pass": sum_pass,
            "s_end": sum_end,
            "c_pass": lambda q: gather_pass(cot, q, s_c, r_c, COT[q]),
        }

        def at(i, point, table):
            for (step, where), names in table.items():
                if where == point:

                    @pl.when(i == step)
                    def _():
                        for name, q in names:
                            stages[name](q)

        def forward_step(i, carry):
            forward_in(i)
            at(i, 1, FORWARD)
            forward_model(i, 0)
            at(i, 2, FORWARD)
            forward_model(i, 1)
            at(i, 3, FORWARD)
            forward_model(i, 2)
            at(i, 4, FORWARD)
            forward_out(i)
            return carry

        lax.fori_loop(0, images, forward_step, 0)

        def gm_copy(d):
            peer = lax.rem(t + d, n_t)
            return to_tensor(gm_send.at[peer], gm_in.at[t], s_gm.at[d], r_gm.at[d], peer)

        def pair_copy(s):
            return to_tensor(pair.at[s], pair_in.at[s], s_pair.at[s], r_pair.at[s], mate_t)

        def dp_copies(d):
            peer = lax.rem(j + d, n_dp)
            return [
                to_dp(dp_sum.at[peer], dp_in.at[j], s_dq.at[d], r_dq.at[d], peer),
                to_dp(dp_ex.at[peer], dp_ex_in.at[j], s_do.at[d], r_do.at[d], peer),
            ]

        third = dp_rows // 3
        early = [d for d in range(1, n_dp)]
        far = (6, 2, 5, 3, 4, 7, 1)
        order = [d for d in far if d < n_dp] + [d for d in range(8, n_dp)] + [n_dp]

        def gd_copy(d):
            peer = lax.rem(j + d, n_dp)
            return to_dp(gm_sum, gm_all.at[j], s_gd.at[d], r_gd.at[d], peer)

        def chunk(s):
            return pl.ds(pl.multiple_of(s * dp_rows, 16), dp_rows)

        def backward_step(i, carry):
            at(i, 0, BACKWARD)
            backward_in(i)
            at(i, 1, BACKWARD)

            @pl.when(i == images - 1)
            def _():
                for d in order:
                    s = lax.rem(j + d, n_dp)
                    pair[s, :, 0:256] = acc_q[mate, chunk(s), :].astype(BF16)
                    pair[s, :, 256:384] = acc_o[mate, chunk(s), :].astype(BF16)
                    pair_copy(s).start()

            backward_out(i)
            at(i, 2, BACKWARD)
            return carry

        lax.fori_loop(0, images, backward_step, 0)

        for src in range(n_t):
            packed = gmod[HD * src : HD * src + 8, :]
            for g in range(1, groups):
                rows = slice(HD * src + 8 * g, HD * src + 8 * (g + 1))
                packed = packed + pltpu.roll(gmod[rows, :], 12 * g, 1)
            gm_send[src] = packed
        for d in range(1, n_t):
            gm_copy(d).start()
        gm_in[t] = gm_send[t]
        for d in order:
            s = lax.rem(j + d, n_dp)
            pair_copy(s).wait_recv()
            sums_q = acc_q[core, chunk(s), :] + pair_in[s, :, 0:256].astype(F32)
            sums_o = acc_o[core, chunk(s), :] + pair_in[s, :, 256:384].astype(F32)
            moved = pltpu.roll(sums_o, 128 - FREE, 1)
            lane = iota((dp_rows, 128), 1)
            dp_sum[s, :, 0:128] = sums_q[:, :128].astype(BF16)
            dp_sum[s, :, 128:256] = (
                sums_q[:, 128:] + jnp.where(lane >= 128 - FREE, moved, 0.0)
            ).astype(BF16)
            rest = jnp.where(lane < HD - FREE, moved, 0.0)
            dp_ex[s] = (
                rest[:third]
                + pltpu.roll(rest[third : 2 * third], 32, 1)
                + pltpu.roll(rest[2 * third :], 64, 1)
            ).astype(BF16)
            if d in early:
                for copy in dp_copies(d):
                    copy.start()
        for d in range(1, n_t):
            gm_copy(d).wait_recv()
        for kk in range(2):
            total = gm_in[kk]
            for c in range(1, chips):
                total = total + gm_in[2 * c + kk]
            gm_sum[kk] = total
        for d in range(1, n_dp):
            gd_copy(d).start()
        for d in range(1, n_dp):
            if d not in early:
                for copy in dp_copies(d):
                    copy.start()
        gm_all[j] = gm_sum[...]
        for d in range(1, n_dp):
            act_copy(d).wait_recv()
        rows_act = act_g[0].astype(F32)
        for s in range(1, n_dp):
            rows_act = rows_act + pltpu.roll(act_g[s].astype(F32), samples * s, 1)

        total = dp_sum[j].astype(F32)
        rest = dp_ex[j].astype(F32)
        for d in range(1, n_dp):
            for copy in dp_copies(d):
                copy.wait_recv()
        for d in range(1, n_dp):
            src = lax.rem(j + d, n_dp)
            total = total + dp_in[src].astype(F32)
            rest = rest + dp_ex_in[src].astype(F32)
        gq_out[...] = total[:, :HW]
        lane = iota((dp_rows, 128), 1)
        spread = jnp.concatenate(
            [rest, pltpu.roll(rest, 128 - 32, 1), pltpu.roll(rest, 128 - 64, 1)], axis=0
        )
        total_o = jnp.where(lane >= 128 - FREE, total[:, 128:], 0.0) + jnp.where(
            lane < HD - FREE, spread, 0.0
        )
        go_out[...] = jnp.transpose(pltpu.roll(total_o, FREE, 1))[:HD]

        for d in range(1, n_dp):
            gd_copy(d).wait_recv()
        lane = iota((8, 128), 1)
        for k in range(3):
            pieces = []
            for g in range(groups):
                value = jnp.zeros((8, 128), F32)
                for s in range(n_dp):
                    for kk in range(2):
                        at = samples * s + images * kk
                        shift = (at - 12 * g - 4 * k) % 128
                        moved = gm_all[s, kk]
                        if shift:
                            moved = pltpu.roll(moved, shift, 1)
                        value = jnp.where((lane >= at) & (lane < at + images), moved, value)
                pieces.append(value)
            ga_out[k] = lax.dot_general(
                rows_act, jnp.concatenate(pieces, axis=0), (((1,), (1,)), ((), ())),
                precision=lax.Precision.HIGHEST, preferred_element_type=F32,
            )

        for copy in mate_noisy + w_copies:
            copy.wait_send()
        for s in range(n_dp):
            pair_copy(s).wait_send()
        for d in range(1, n_t):
            mod_copy(d).wait_send()
            gm_copy(d).wait_send()
        for d in range(1, n_dp):
            act_copy(d).wait_send()
            gd_copy(d).wait_send()
            for copy in dp_copies(d):
                copy.wait_send()
        for i in range(images):
            of_noisy = gather_z if NOISY[i] else gather_x
            of_cot = gather_z if COT[i] else gather_x
            for copy in (
                sum(of_noisy(noisy_g, i, s_ag, r_ag)[:2], [])
                + sum(of_cot(cot, i, s_c, r_c)[:2], [])
                + sum(sum_z(i), [])
            ):
                copy.wait_send()

    vm = pltpu.VMEM
    dma = pltpu.SemaphoreType.DMA
    scratch = [
        vm((images, HD, seq), BF16),
        vm((samples, HD, seq), BF16),
        vm((images, chips, block, seq), BF16),
        vm((1001, width), BF16),
        vm((1000, width), BF16),
        vm((32, width), BF16),
        vm((2, 3, HD, width), BF16),
        vm((2, SPLIT, 128), BF16),
        vm((n_t, SPLIT, 128), BF16),
        vm((images, width, 128), F32),
        vm((width, 128), BF16),
        vm((n_dp, dp_rows, 128), BF16),
        vm((2, 2, HW, width), BF16),
        vm((2, 2, HD, width), BF16),
        vm((2, 2 * HW, width), BF16),
        vm((width, 2 * HW), BF16),
        vm((2 * HD, width), BF16),
        vm((2, width, 2 * HD), BF16),
        vm((images, width, seq), BF16),
        vm((images, width, seq), BF16),
        vm((2, width, seq), BF16),
        vm((3, 2 * HD, seq), BF16),
        vm((images, 2, HD, seq), BF16),
        vm((images, width, seq), BF16),
        vm((images, 2, seq, seq), F32),
        vm((images, 2, 3, HP, seq), BF16),
        vm((images, chips, block, seq), BF16),
        vm((images, 2 * n_x, block, seq), BF16),
        vm((images, chips, block, seq), BF16),
        vm((width, seq), BF16),
        vm((2 * HW, seq), BF16),
        vm((2, width, 256), F32),
        vm((2, width, 128), F32),
        vm((width, 128), F32),
        vm((n_t, 8, 128), F32),
        vm((n_t, 8, 128), F32),
        vm((2, 8, 128), F32),
        vm((n_dp, 2, 8, 128), F32),
        vm((n_dp, dp_rows, 384), BF16),
        vm((n_dp, dp_rows, 384), BF16),
        vm((n_dp, dp_rows, 256), BF16),
        vm((n_dp, dp_rows, 256), BF16),
        vm((n_dp, dp_rows // 3, 128), BF16),
        vm((n_dp, dp_rows // 3, 128), BF16),
        dma((10,)),
        dma((images,)),
        dma((images,)),
        dma((4,)),
        dma((4,)),
        dma((n_t,)),
        dma((n_t,)),
        dma((n_dp,)),
        dma((n_dp,)),
        dma((images, 2 * n_x)),
        dma((images, 2 * n_x)),
        dma((images, 2 * n_x)),
        dma((images, 2 * n_x)),
        dma((images, 2 * n_x)),
        dma((images, 2 * n_x)),
        dma((n_t,)),
        dma((n_t,)),
        dma((n_dp,)),
        dma((n_dp,)),
        dma((n_dp,)),
        dma((n_dp,)),
        dma((n_dp,)),
        dma((n_dp,)),
        dma((n_dp,)),
        dma((n_dp,)),
    ]
    any_spec = pl.BlockSpec(memory_space=pl.ANY)
    smem_spec = pl.BlockSpec(memory_space=pltpu.SMEM)
    vmem_spec = pl.BlockSpec(memory_space=pltpu.VMEM)
    return pl.pallas_call(
        kernel,
        out_shape=(
            jax.ShapeDtypeStruct((dp_rows, HW), F32),
            jax.ShapeDtypeStruct((HD, dp_rows), F32),
            jax.ShapeDtypeStruct((3, dp_rows, HD), F32),
        ),
        in_specs=[smem_spec] * 4 + [any_spec] * 10,
        out_specs=(vmem_spec,) * 3,
        scratch_shapes=scratch,
        compiler_params=pltpu.CompilerParams(
            collective_id=0, has_side_effects=True, vmem_limit_bytes=60 * 1024 * 1024
        ),
        name="step",
    )


def pass_on(*refs):
    half = len(refs) // 2
    for src, dst in zip(refs[:half], refs[half:]):
        dst[...] = src[...]


def local(
    noisy,
    labels,
    tsteps,
    guide_index,
    class_table,
    time_table,
    guide_table,
    guide_weights,
    teacher_qkv,
    teacher_out,
    teacher_ada,
    student_qkv,
    student_out,
    student_ada,
):
    samples, seq_len, _ = noisy.shape
    n_t = lax.axis_size("tensor")
    n_dp = lax.axis_size("dp")
    norm_scale = 1.0 / math.sqrt(samples * n_dp * seq_len)
    step = make_kernel(n_t, n_dp, samples, seq_len, norm_scale)
    grads = step(
        labels, tsteps, guide_index, guide_weights,
        jnp.swapaxes(noisy, 1, 2), class_table, time_table, guide_table,
        teacher_qkv.T, student_qkv.T, teacher_out, student_out,
        jnp.swapaxes(teacher_ada, 1, 2), jnp.swapaxes(student_ada, 1, 2),
    )
    return pl.pallas_call(
        pass_on,
        out_shape=tuple(jax.ShapeDtypeStruct(g.shape, g.dtype) for g in grads),
        name="pass_on",
    )(*grads)


def solution(mesh):
    return jax.shard_map(
        local,
        mesh=mesh,
        in_specs=(
            P("dp", None, "tensor"),
            P("dp"),
            P("dp"),
            P("dp"),
            P(),
            P(),
            P(),
            P(),
            P(None, "tensor"),
            P("tensor", None),
            P(None, None, "tensor"),
            P(None, "tensor"),
            P("tensor", None),
            P(None, None, "tensor"),
        ),
        out_specs=(P("dp", "tensor"), P("tensor", "dp"), P(None, "dp", "tensor")),
        check_vma=False,
    )
```
